128 devices in a mesh: rep: 1, r: 4 (over x), s: 32 (over y, z, core).
Axes of the slice: x: 4, y: 4, z: 4, core: 2. Of those that a mesh axis runs over, the one named last changes fastest.
Arguments:
- x: bfloat16 [128, 2048, 1024], P(('rep', 'r', 's'))
- dy: bfloat16 [128, 2048, 1024], P(('rep', 'r', 's'))
- w_gate: bfloat16 [2, 1024, 3328], P(None, 's')
- w_up: bfloat16 [2, 1024, 3328], P(None, 's')
- w_down: bfloat16 [2, 3328, 1024], P(None, 's')
- m_w_gate: float32 [2, 1024, 3328], P(None, 's')
- m_w_up: float32 [2, 1024, 3328], P(None, 's')
- m_w_down: float32 [2, 3328, 1024], P(None, 's')
- v_w_gate: float32 [2, 1024, 3328], P(None, 's')
- v_w_up: float32 [2, 1024, 3328], P(None, 's')
- v_w_down: float32 [2, 3328, 1024], P(None, 's')
Outputs:
- output 1: bfloat16 [2, 1024, 3328], P('rep', 's')
- output 2: bfloat16 [2, 1024, 3328], P('rep', 's')
- output 3: bfloat16 [2, 3328, 1024], P('rep', 's')
- output 4: float32 [2, 1024, 3328], P('rep', 's')
- output 5: float32 [2, 1024, 3328], P('rep', 's')
- output 6: float32 [2, 3328, 1024], P('rep', 's')
- output 7: float32 [2, 1024, 3328], P('rep', 's')
- output 8: float32 [2, 1024, 3328], P('rep', 's')
- output 9: float32 [2, 3328, 1024], P('rep', 's')
All inputs are finite; a program needn't handle non-finite values.
Results may differ from the reference program's by a relative error of at most 0.022.
Values are sent between devices in bfloat16 or wider.
A program may use at most 1.5 GiB of HBM per device.

```python
import jax
import jax.numpy as jnp
from jax import lax

SEQUENCES = 128
TOKENS = 2048
D = 1024
FF = 3328
LAYERS = 2
NAMES = ("w_gate", "w_up", "w_down")
SHAPES = {"w_gate": (LAYERS, D, FF), "w_up": (LAYERS, D, FF), "w_down": (LAYERS, FF, D)}


def bump(key, n, height):
    away = (jnp.arange(n, dtype=jnp.int32) - jax.random.randint(key, (), 0, n, jnp.int32)) % n
    return jnp.where(away < n // 8, height, 1.0)


def together(key, own, strength):
    shared = jax.random.normal(key, own.shape[1:], jnp.float32)
    return (own + strength * shared) * lax.rsqrt(1 + strength * strength)


def setup_inputs(seed: int = 0, part: int = 0) -> dict:
    kx, kdy, ka, kb, kz, kf, kh, kl, *keys = jax.random.split(jax.random.key(seed), 8 + 3 * len(NAMES))
    kx, kdy, ka, kb = (jax.random.fold_in(k, part) for k in (kx, kdy, ka, kb))
    kw, km, kv = (keys[i::3] for i in range(3))
    shape = (SEQUENCES, TOKENS, D)
    much_x, much_dy = jax.random.uniform(kz, (2,), jnp.float32, 0.0, 1.0)
    loud = 2.0 ** jax.random.uniform(jax.random.fold_in(kz, 1), (), jnp.float32, -1.0, 2.0)
    layers = 2.0 ** jax.random.uniform(kl, (LAYERS, 1, 1), jnp.float32, -1.0, 1.0)
    x = together(ka, jax.random.normal(kx, shape, jnp.float32), much_x) * bump(kf, D, 4.0)
    dy = together(kb, jax.random.normal(kdy, shape, jnp.float32), much_dy)
    drawn = {"x": x.astype(jnp.bfloat16), "dy": (loud * dy * (SEQUENCES * TOKENS) ** -0.5).astype(jnp.bfloat16)}
    for key, name in zip(kw, NAMES, strict=True):
        w = jax.random.normal(key, SHAPES[name], jnp.float32) * SHAPES[name][1] ** -0.5
        drawn[name] = (w * {"w_gate": 1.0, "w_up": bump(kh, FF, 4.0), "w_down": layers}[name]).astype(jnp.bfloat16)
    for key, name in zip(km, NAMES, strict=True):
        drawn[f"m_{name}"] = 0.1 * jax.random.normal(key, SHAPES[name], jnp.float32)
    for key, name in zip(kv, NAMES, strict=True):
        drawn[f"v_{name}"] = loud * loud * jax.random.uniform(key, SHAPES[name], jnp.float32, 0.05, 0.15)
    return drawn


def matmul(a, w):
    return jnp.dot(a, w, preferred_element_type=jnp.float32).astype(jnp.bfloat16)


def normed(h):
    wide = h.astype(jnp.float32)
    scale = lax.rsqrt(jnp.mean(wide**2, -1, keepdims=True) + 1e-6)
    return (wide * scale).astype(jnp.bfloat16)


def layer(h, w):
    a = normed(h)
    gate = jnp.dot(a, w["w_gate"], preferred_element_type=jnp.float32)
    up = jnp.dot(a, w["w_up"], preferred_element_type=jnp.float32)
    return h + matmul((jax.nn.silu(gate) * up).astype(jnp.bfloat16), w["w_down"])


def adamw(w, m, v, g):
    m = 0.9 * m + 0.1 * g
    v = 0.95 * v + 0.05 * g * g
    step = m * lax.rsqrt(v + 1e-8) + 0.1 * w
    return (w - 0.02 * step).astype(jnp.bfloat16), m, v


def stack(weights, h):
    return lax.scan(lambda h, w: (layer(h, w), None), h, weights)[0]


def reference(x, dy, w_gate, w_up, w_down, m_w_gate, m_w_up, m_w_down, v_w_gate, v_w_up, v_w_down):
    weights = dict(zip(NAMES, (w_gate, w_up, w_down), strict=True))

    def take(so_far, sequence):
        h, by_y = sequence
        _, back = jax.vjp(lambda w: stack(w, h), weights)
        return jax.tree.map(lambda total, term: total + term.astype(jnp.float32), so_far, back(by_y)[0]), None

    none_yet = {name: jnp.zeros(w.shape, jnp.float32) for name, w in weights.items()}
    by_weights, _ = lax.scan(take, none_yet, (x, dy))
    gradients = [by_weights[name].astype(jnp.bfloat16).astype(jnp.float32) for name in NAMES]
    new = [
        adamw(w.astype(jnp.float32), m, v, g)
        for w, m, v, g in zip((w_gate, w_up, w_down), (m_w_gate, m_w_up, m_w_down), (v_w_gate, v_w_up, v_w_down), gradients, strict=True)
    ]
    return tuple(one[which] for which in range(3) for one in new)
```

```python
import functools

import jax
import jax.numpy as jnp
from jax import lax
from jax.experimental import pallas as pl
from jax.experimental.pallas import tpu as pltpu
from jax.sharding import PartitionSpec as P

NAMES = ("w_gate", "w_up", "w_down")
MESH = pl.DeviceIdType.MESH
F32, BF16 = jnp.float32, jnp.bfloat16
HOPS = 6


def matmul(a, w):
    return jnp.dot(a, w, preferred_element_type=jnp.float32).astype(jnp.bfloat16)


def normed(h):
    wide = h.astype(jnp.float32)
    scale = lax.rsqrt(jnp.mean(wide**2, -1, keepdims=True) + 1e-6)
    return (wide * scale).astype(jnp.bfloat16)


def layer(h, w):
    a = normed(h)
    gate = jnp.dot(a, w["w_gate"], preferred_element_type=jnp.float32)
    up = jnp.dot(a, w["w_up"], preferred_element_type=jnp.float32)
    return h + matmul((jax.nn.silu(gate) * up).astype(jnp.bfloat16), w["w_down"])


def adamw(w, m, v, g):
    m = 0.9 * m + 0.1 * g
    v = 0.95 * v + 0.05 * g * g
    step = m * lax.rsqrt(v + 1e-8) + 0.1 * w
    return (w - 0.02 * step).astype(jnp.bfloat16), m, v


class Place:
    def __init__(self):
        self.s, self.x = lax.axis_index("s"), lax.axis_index("r")
        self.core = self.s % 2
        y, z = self.s // 8, (self.s // 2) % 4
        self.a = y * (1 - self.core) + z * self.core
        self.b = z * (1 - self.core) + y * self.core
        self.step_a, self.step_b = 8 - 6 * self.core, 2 + 6 * self.core

    def chip(self, a, b):
        return (a % 4) * (self.step_a // 2) + (b % 4) * (self.step_b // 2)

    def at(self, a, b):
        return {"s": 2 * self.chip(a, b) + self.core}

    def partner(self):
        return {"s": self.s + 1 - 2 * self.core}

    def along_x(self, d):
        return {"r": (self.x + d) % 4}

    def neighbours(self):
        a, b = self.a, self.b
        plane = [self.partner()] + [self.at(a + d, b) for d in (1, 3)] + [self.at(a, b + d) for d in (1, 3)]
        return plane + [self.along_x(d) for d in (1, 2, 3)]


def meet(places):
    barrier = pltpu.get_barrier_semaphore()
    for place in places:
        pl.semaphore_signal(barrier, inc=1, device_id=place, device_id_type=MESH)
    pl.semaphore_wait(barrier, len(places))


def send(src, dst, send_sem, recv_sem, place):
    return pltpu.make_async_remote_copy(src_ref=src, dst_ref=dst, send_sem=send_sem, recv_sem=recv_sem, device_id=place, device_id_type=MESH)


def gather_kernel(layers, *refs):
    n = 3 * layers
    shards, full = refs[:3], refs[3 : 3 + n]
    here = refs[3 + n : 6 + n]
    sems_out, sems_in, sems_here = refs[6 + n :]
    p = Place()
    meet(p.neighbours()[:5])
    loads = [pltpu.make_async_copy(shards[i], here[i], sems_here.at[i]) for i in range(3)]
    for load in loads:
        load.start()
    for load in loads:
        load.wait()

    def run(core):
        def group(m, b, columns=None):
            whole = full[m].at[:, b % 4, core] if core == 0 else full[m].at[b % 4, :, core]
            return whole if columns is None else whole.at[:, :, pl.ds(*columns)]

        def piece(m, a, b, columns=None):
            whole = full[m].at[a % 4, b % 4, core] if core == 0 else full[m].at[b % 4, a % 4, core]
            return whole if columns is None else whole.at[:, pl.ds(*columns)]

        a, b = p.a, p.b
        started = []

        def go(m, i, src, dst, place):
            copy = send(src, dst, sems_out.at[m, i], sems_in.at[m, i], place)
            copy.start()
            started.append(copy)

        def came(m, i, ref):
            pltpu.make_async_copy(ref, ref, sems_in.at[m, i]).wait()

        halves = []
        for m in range(n):
            columns = full[m].shape[-1]
            halves.append(((0, columns // 2), (columns // 2, columns // 2)))
        order = range(n)
        for m in order:
            own = here[m % 3].at[m // 3]
            go(m, 0, own, piece(m, a, b), p.at(a + 1, b))
            go(m, 1, own, piece(m, a, b), p.at(a - 1, b))
            go(m, 8, own, piece(m, a, b), p.partner())
            local = pltpu.make_async_copy(own, piece(m, a, b), sems_here.at[3 + m])
            local.start()
        for m in order:
            pltpu.make_async_copy(here[m % 3].at[m // 3], piece(m, a, b), sems_here.at[3 + m]).wait()
            came(m, 0, piece(m, a - 1, b))
            go(m, 2, piece(m, a - 1, b, halves[m][0]), piece(m, a - 1, b, halves[m][0]), p.at(a + 1, b))
            go(m, 9, piece(m, a - 1, b), piece(m, a - 1, b), p.partner())
            came(m, 1, piece(m, a + 1, b))
            go(m, 3, piece(m, a + 1, b, halves[m][1]), piece(m, a + 1, b, halves[m][1]), p.at(a - 1, b))
            go(m, 10, piece(m, a + 1, b), piece(m, a + 1, b), p.partner())
        for m in order:
            came(m, 2, piece(m, a + 2, b, halves[m][0]))
            came(m, 3, piece(m, a + 2, b, halves[m][1]))
            go(m, 4, group(m, b), group(m, b), p.at(a, b + 1))
            go(m, 5, group(m, b), group(m, b), p.at(a, b - 1))
            go(m, 11, piece(m, a + 2, b), piece(m, a + 2, b), p.partner())
        for m in order:
            came(m, 4, group(m, b - 1))
            go(m, 6, group(m, b - 1, halves[m][0]), group(m, b - 1, halves[m][0]), p.at(a, b + 1))
            go(m, 12, group(m, b - 1), group(m, b - 1), p.partner())
            came(m, 5, group(m, b + 1))
            go(m, 7, group(m, b + 1, halves[m][1]), group(m, b + 1, halves[m][1]), p.at(a, b - 1))
            go(m, 13, group(m, b + 1), group(m, b + 1), p.partner())
        for m in order:
            came(m, 6, group(m, b + 2, halves[m][0]))
            came(m, 7, group(m, b + 2, halves[m][1]))
            go(m, 14, group(m, b + 2), group(m, b + 2), p.partner())
        for copy in started:
            copy.wait_send()
        for m in order:
            for i in (8, 9, 10, 11):
                came(m, i, piece(m, a, b))
            for i in (12, 13, 14):
                came(m, i, group(m, b))

    for core in range(2):
        pl.when(p.core == core)(functools.partial(run, core))


def gathered(weights):
    layers = weights[0].shape[0]
    shapes = [(4, 4, 2) + w.shape[1:] for _ in range(layers) for w in weights]
    any_space = pl.BlockSpec(memory_space=pl.ANY)
    out = pl.pallas_call(
        functools.partial(gather_kernel, layers),
        out_shape=[jax.ShapeDtypeStruct(shape, BF16) for shape in shapes],
        in_specs=[any_space] * 3,
        out_specs=[any_space] * len(shapes),
        scratch_shapes=[pltpu.VMEM(w.shape, BF16) for w in weights]
        + [
            pltpu.SemaphoreType.DMA((len(shapes), 15)),
            pltpu.SemaphoreType.DMA((len(shapes), 15)),
            pltpu.SemaphoreType.DMA((3 + len(shapes),)),
        ],
        compiler_params=pltpu.CompilerParams(collective_id=0, has_side_effects=True),
        name="gather",
    )(*weights)
    whole = [w.reshape(-1, w.shape[-1]) for w in out]
    return [dict(zip(NAMES, whole[3 * i : 3 * i + 3], strict=True)) for i in range(layers)]


class Sum:
    SCRATCH = 22

    @staticmethod
    def scratch(rows, columns):
        half = columns // 2

        def wide(*lead):
            return pltpu.VMEM((2, *lead, rows, columns), F32)

        def sent(*lead):
            return pltpu.VMEM((2, *lead, rows, columns), BF16)

        def part(*lead):
            return pltpu.VMEM((2, *lead, rows, half), BF16)

        return [
            sent(16, 2),
            sent(16),
            wide(4),
            wide(4),
            wide(4),
            sent(4),
            part(4),
            part(4),
            sent(4),
            sent(4),
            sent(4),
            sent(4),
            wide(),
            wide(),
            wide(),
            sent(),
            part(),
            part(),
            sent(),
            sent(),
            sent(),
            sent(),
            sent(4),
            pltpu.SemaphoreType.DMA((2, 12)),
            pltpu.SemaphoreType.DMA((2, 12)),
        ]

    def __init__(self, p, refs, total, emit):
        self.p, self.total, self.emit = p, total, emit
        (self.term, self.swapped, self.ca, self.cp, self.cm, self.x1, self.r1a, self.r1b, self.x2p, self.x2m, self.r2p, self.r2m) = refs[:12]
        (self.db, self.dp, self.dm, self.y1, self.r3a, self.r3b, self.y2p, self.y2m, self.r4p, self.r4m, self.rx) = refs[12:23]
        self.out_sem, self.in_sem = refs[23:25]
        self.half = self.term.shape[-1] // 2

    def copies(self, hop, k):
        p, h = self.p, self.half

        def one(i, src, dst, place):
            return send(src, dst, self.out_sem.at[k, i], self.in_sem.at[k, i], place)

        low, high = pl.ds(0, h), pl.ds(h, h)
        if hop == 0:
            return [one(0, self.term.at[k, :, 1 - p.core], self.swapped.at[k], p.partner())]
        if hop == 1:
            return [
                one(1, self.x1.at[k, :, :, low], self.r1a.at[k], p.at(p.a + 1, p.b)),
                one(2, self.x1.at[k, :, :, high], self.r1b.at[k], p.at(p.a - 1, p.b)),
            ]
        if hop == 2:
            return [
                one(3, self.x2p.at[k], self.r2p.at[k], p.at(p.a + 1, p.b)),
                one(4, self.x2m.at[k], self.r2m.at[k], p.at(p.a - 1, p.b)),
            ]
        if hop == 3:
            return [
                one(5, self.y1.at[k, :, low], self.r3a.at[k], p.at(p.a, p.b + 1)),
                one(6, self.y1.at[k, :, high], self.r3b.at[k], p.at(p.a, p.b - 1)),
            ]
        if hop == 4:
            return [
                one(7, self.y2p.at[k], self.r4p.at[k], p.at(p.a, p.b + 1)),
                one(8, self.y2m.at[k], self.r4m.at[k], p.at(p.a, p.b - 1)),
            ]
        return [one(8 + d, self.rx.at[k, p.x], self.rx.at[k, p.x], p.along_x(d)) for d in (1, 2, 3)]

    def add(self, hop, k, u):
        p, h = self.p, self.half

        def f(ref, *index):
            return ref[index].astype(F32)

        low, high = slice(0, h), slice(h, None)
        if hop == 1:
            for quarter, ref in ((p.a, self.ca), (p.a + 1, self.cp), (p.a - 1, self.cm), (p.a + 2, self.x1)):
                for b in range(4):
                    chip = p.chip(quarter, b)
                    ref[k, b] = (f(self.term, k, chip, p.core) + f(self.swapped, k, chip)).astype(ref.dtype)
        if hop == 2:
            for b in range(4):
                self.x2p[k, b, :, low] = (self.cp[k, b, :, low] + f(self.r1a, k, b)).astype(BF16)
                self.x2p[k, b, :, high] = self.cp[k, b, :, high].astype(BF16)
                self.x2m[k, b, :, low] = self.cm[k, b, :, low].astype(BF16)
                self.x2m[k, b, :, high] = (self.cm[k, b, :, high] + f(self.r1b, k, b)).astype(BF16)
        if hop == 3:
            for place, ref in ((p.b, self.db), (p.b + 1, self.dp), (p.b - 1, self.dm), (p.b + 2, self.y1)):
                b = place % 4
                ref[k] = (self.ca[k, b] + f(self.r2p, k, b) + f(self.r2m, k, b)).astype(ref.dtype)
        if hop == 4:
            self.y2p[k, :, low] = (self.dp[k, :, low] + f(self.r3a, k)).astype(BF16)
            self.y2p[k, :, high] = self.dp[k, :, high].astype(BF16)
            self.y2m[k, :, low] = self.dm[k, :, low].astype(BF16)
            self.y2m[k, :, high] = (self.dm[k, :, high] + f(self.r3b, k)).astype(BF16)
        if hop == 5:
            self.rx[k, p.x] = (self.db[k] + f(self.r4p, k) + f(self.r4m, k)).astype(BF16)
        if hop == 6:
            self.emit(u, ((f(self.rx, k, 0) + f(self.rx, k, 1)) + (f(self.rx, k, 2) + f(self.rx, k, 3))).astype(BF16))

    def hop(self, hop, u):
        k = u % 2
        if hop:
            for copy in self.copies(hop - 1, k):
                copy.wait()
        self.add(hop, k, u)
        if hop < HOPS:
            for copy in self.copies(hop, k):
                copy.start()

    def step(self, t, first=1):
        for hop in range(HOPS, first - 1, -1):
            u = t - hop
            pl.when((u >= 0) & (u < self.total))(functools.partial(self.hop, hop, u))


ROWS, COLUMNS = 64, 256


def sum_kernel(layers, ff_units, d_units, *refs):
    n = 3 * layers
    terms, out, scratch, load_sem = refs[:n], refs[n], refs[n + 1 : -1], refs[-1]
    p = Place()
    meet(p.neighbours())
    per = ff_units + d_units
    total = layers * per

    def emit(u, value):
        out[u] = value

    sums = Sum(p, scratch, total, emit)

    def loads(u, k):
        which = []
        for number in range(layers):
            gate, up, down = terms[3 * number : 3 * number + 3]

            def both(j, gate=gate, up=up):
                at = pl.ds(pl.multiple_of(j * COLUMNS, COLUMNS), COLUMNS)
                return [
                    pltpu.make_async_copy(ref.at[:, :, :, at], sums.term.at[k, :, :, pl.ds(32 * i, 32)], load_sem.at[i])
                    for i, ref in enumerate((gate, up))
                ]

            def rows(q, down=down):
                at = pl.ds(pl.multiple_of(16 * q - 8 * (q // (d_units - 1)), 8), 16)
                return [
                    pltpu.make_async_copy(down.at[:, :, at, pl.ds(256 * i, 256)], sums.term.at[k, :, :, pl.ds(16 * i, 16)], load_sem.at[i])
                    for i in range(4)
                ]

            which += [(number * per, ff_units, both), (number * per + ff_units, d_units, rows)]
        return which

    def body(t, _):
        sums.step(t)
        k = t % 2
        for start, count, made in loads(t, k):

            @pl.when((t >= start) & (t < start + count))
            def _(start=start, made=made):
                copies = made(t - start)
                for copy in copies:
                    copy.start()
                for copy in copies:
                    copy.wait()

        pl.when(t < total)(functools.partial(sums.hop, 0, t))

    lax.fori_loop(0, total + HOPS, lambda t, c: (body(t, c), c)[1], 0)


def summed(terms):
    layers = len(terms)
    flat = [t.reshape(16, 2, t.shape[0] // 32, t.shape[1]) for one in terms for t in one]
    d_rows = terms[0][2].shape[0] // 32
    ff_units, d_units = terms[0][0].shape[1] // COLUMNS, -(-d_rows // 16)
    per = ff_units + d_units
    out = pl.pallas_call(
        functools.partial(sum_kernel, layers, ff_units, d_units),
        out_shape=jax.ShapeDtypeStruct((layers * per, ROWS, COLUMNS), BF16),
        in_specs=[pl.BlockSpec(memory_space=pl.ANY)] * len(flat),
        out_specs=pl.BlockSpec(memory_space=pltpu.VMEM),
        scratch_shapes=Sum.scratch(ROWS, COLUMNS) + [pltpu.SemaphoreType.DMA((4,))],
        compiler_params=pltpu.CompilerParams(collective_id=1, has_side_effects=True, vmem_limit_bytes=48 * 2**20),
        name="sum",
    )(*flat)
    blocks = []
    for number in range(layers):
        one = out[number * per : (number + 1) * per]
        both = one[:ff_units].reshape(ff_units, 2, 32, COLUMNS).transpose(1, 2, 0, 3).reshape(2, 32, -1)
        down = one[ff_units:].reshape(d_units, 4, 16, COLUMNS).transpose(0, 2, 1, 3).reshape(d_units * 16, -1)
        kept = 16 * (d_units - 1)
        down = jnp.concatenate([down[: kept - (16 * d_units - d_rows)], down[kept:]]) if 16 * d_units != d_rows else down
        blocks.append([both[0], both[1], down])
    return blocks


def solution(mesh):
    def step(x, dy, *arrays):
        weights, m, v = (arrays[i : i + 3] for i in (0, 3, 6))
        layers = weights[0].shape[0]
        whole = gathered(weights)
        h, kept = x[0], []
        for number in range(layers):
            kept.append(h)
            h = layer(h, whole[number])
        by_h, terms = dy[0], [None] * layers
        for number in reversed(range(layers)):
            _, back = jax.vjp(lambda w, h: layer(h, w), whole[number], kept[number])
            by_w, by_h = back(by_h)
            terms[number] = [by_w[name] for name in NAMES]
        mine = summed(terms)
        gradients = [jnp.stack([mine[number][i] for number in range(layers)]).astype(jnp.float32) for i in range(3)]
        new = [adamw(w.astype(jnp.float32), m, v, g) for w, m, v, g in zip(weights, m, v, gradients, strict=True)]
        return tuple(one[which] for which in range(3) for one in new)

    states, cut = P(("rep", "r", "s"), None, None), P(None, "s", None)
    return jax.shard_map(
        step,
        mesh=mesh,
        in_specs=(states, states) + (cut,) * 9,
        out_specs=(P("rep", "s", None),) * 9,
        check_vma=False,
    )
```

```python
import functools

import jax
import jax.numpy as jnp
from jax import lax
from jax.experimental import pallas as pl
from jax.experimental.pallas import tpu as pltpu
from jax.sharding import PartitionSpec as P

NAMES = ("w_gate", "w_up", "w_down")
MESH = pl.DeviceIdType.MESH
F32, BF16 = jnp.float32, jnp.bfloat16
HOPS = 6
VMEM_LIMIT = 67043328
PLAIN, BY_COLUMNS, BY_ROWS = (((1,), (0,)), ((), ())), (((1,), (1,)), ((), ())), (((0,), (0,)), ((), ()))
HERE, NEXT, FAR, LAST = range(4)
TILE = 256


def adamw(w, m, v, g):
    m = 0.9 * m + 0.1 * g
    v = 0.95 * v + 0.05 * g * g
    step = m * lax.rsqrt(v + 1e-8) + 0.1 * w
    return (w - 0.02 * step).astype(jnp.bfloat16), m, v


def dot(a, b, dims=PLAIN):
    return lax.dot_general(a, b, dims, preferred_element_type=F32)


def block(n, size=TILE):
    return pl.ds(pl.multiple_of(n * size, size), size)


def added(values):
    total = None
    for value in values:
        total = value if total is None else total + value
    return total


RING, OTHERS = ((NEXT, HERE), (LAST, HERE), (HERE, NEXT), (HERE, LAST)), (NEXT, FAR, LAST)


class Place:
    def __init__(self):
        self.s, self.x = lax.axis_index("s"), lax.axis_index("r")
        self.core = lax.rem(self.s, 2)
        y, z = lax.div(self.s, 8), lax.rem(lax.div(self.s, 2), 4)
        a = y * (1 - self.core) + z * self.core
        b = z * (1 - self.core) + y * self.core
        step_a, step_b = 4 - 3 * self.core, 1 + 3 * self.core
        self.a, self.b = [[lax.rem(at + d, 4) for d in range(4)] for at in (a, b)]
        self.chips = [[self.a[d] * step_a + self.b[e] * step_b for e in range(4)] for d in range(4)]
        self.devices = {(d, e): 2 * self.chips[d][e] + self.core for d in range(4) for e in range(4)}
        self.across = self.s + 1 - 2 * self.core
        self.xs = [lax.rem(self.x + d, 4) for d in range(4)]

    def at(self, d, e):
        return {"s": self.devices[d, e]}

    def partner(self):
        return {"s": self.across}

    def along_x(self, d):
        return {"r": self.xs[d]}

    def neighbours(self):
        return [self.partner()] + [self.at(*there) for there in RING] + [self.along_x(d) for d in OTHERS]


def meet(places):
    barrier = pltpu.get_barrier_semaphore()
    for place in places:
        pl.semaphore_signal(barrier, inc=1, device_id=place, device_id_type=MESH)
    pl.semaphore_wait(barrier, len(places))


def send(src, dst, send_sem, recv_sem, place):
    return pltpu.make_async_remote_copy(src_ref=src, dst_ref=dst, send_sem=send_sem, recv_sem=recv_sem, device_id=place, device_id_type=MESH)


class Gather:
    SLOTS = 12

    def __init__(self, p, n, m, here, full, sems):
        self.p, self.n, self.m, self.here, self.full = p, n, m, here, full
        self.out_sem, self.in_sem, self.here_sem, self.own_sem = sems
        self.total = 2 * (n + m)

    def hop(self, core, kind, hop, u, later):
        p, k = self.p, lax.rem(u, self.SLOTS)
        at = u - self.m * later if kind == 0 else u - self.n * (1 + later)
        here = self.here[kind].at[at]
        rows = here.shape[0]
        f = self.full[kind].at[at]
        cut = (rows // 2 + 7) // 8 * 8
        low, high = (0, cut), (cut, rows - cut)

        def piece(d, e, half=(0, rows)):
            if kind:
                return f.at[pl.ds(pl.multiple_of(rows * p.devices[d, e], 8) + half[0], half[1])]
            whole = f.at[p.a[d], p.b[e], core] if core == 0 else f.at[p.b[e], p.a[d], core]
            return whole.at[pl.ds(*half)]

        def group(e, half=(0, rows)):
            if kind:
                return [piece(d, e, half) for d in range(4)]
            whole = f.at[:, p.b[e], core] if core == 0 else f.at[p.b[e], :, core]
            return [whole.at[:, pl.ds(*half)]]

        def of_size(lines, columns, half=(0, rows)):
            if kind:
                return f.at[pl.ds(0, lines * columns * half[1])]
            return f.at[pl.ds(0, lines), pl.ds(0, columns), 0, pl.ds(*half)]

        def go(i, ref, place, left=0, src=None):
            send(ref if src is None else src, ref, self.out_sem.at[k, left], self.in_sem.at[k, i], place).start()

        def over(ref, src=None):
            go(8, ref, p.partner(), FAR, src)

        def came(sem, ref):
            pltpu.make_async_copy(ref, ref, sem).wait()

        def all_came(i, columns, half=(0, rows)):
            came(self.in_sem.at[k, i], of_size(1, columns, half))

        if hop == 0:
            came(self.here_sem.at[u], here)
            own = piece(HERE, HERE)
            go(0, own, p.at(NEXT, HERE), src=here)
            go(1, own, p.at(LAST, HERE), src=here)
            over(own, src=here)
            pltpu.make_async_copy(here, own, self.own_sem.at[k]).start()
        if hop == 1:
            all_came(0, 1)
            go(2, piece(LAST, HERE, low), p.at(NEXT, HERE))
            over(piece(LAST, HERE))
            all_came(1, 1)
            go(3, piece(NEXT, HERE, high), p.at(LAST, HERE))
            over(piece(NEXT, HERE))
        if hop == 2:
            came(self.own_sem.at[k], piece(HERE, HERE))
            all_came(2, 1, low)
            all_came(3, 1, high)
            for one in group(HERE):
                go(4, one, p.at(HERE, NEXT), 1)
                go(5, one, p.at(HERE, LAST), 1)
            over(piece(FAR, HERE))
        if hop == 3:
            all_came(4, 4)
            for one in group(LAST, low):
                go(6, one, p.at(HERE, NEXT), 1)
            for one in group(LAST):
                over(one)
            all_came(5, 4)
            for one in group(NEXT, high):
                go(7, one, p.at(HERE, LAST), 1)
            for one in group(NEXT):
                over(one)
        if hop == 4:
            all_came(6, 4, low)
            all_came(7, 4, high)
            for one in group(FAR):
                over(one)
        if hop == 5:
            came(self.in_sem.at[k, 8], of_size(4, 4))
            for i, (lines, columns) in enumerate(((1, 3), (3, 4), (4, 4))):
                came(self.out_sem.at[k, i], of_size(lines, columns))

    def step(self, t):
        def both(core, hop, u):
            later = lax.div(u, self.n + self.m)
            is_down = u - (self.n + self.m) * later >= self.n
            pl.when(~is_down)(lambda: self.hop(core, 0, hop, u, later))
            pl.when(is_down)(lambda: self.hop(core, 1, hop, u, later))

        def run(core):
            for hop in range(5, -1, -1):
                u = t - 2 * hop
                pl.when((u >= 0) & (u < self.total))(functools.partial(both, core, hop, u))

        for core in (0, 1):
            pl.when(self.p.core == core)(functools.partial(run, core))

    def steps(self, first, count):
        lax.fori_loop(0, count, lambda i, c: (self.step(first + i), c)[1], 0)


def normed(wide):
    return (wide * lax.rsqrt(jnp.mean(wide * wide, -1, keepdims=True) + 1e-6)).astype(BF16)


def forward_kernel(x, dy, w_gate, w_up, w_down, gu, d, pq, act_out, at_out, h_out, dw_out,
                   a, dyv, act, wt, wdt, pqs, h, ats, xs, dws, here_gu, here_d, out_sem, in_sem, here_sem, own_sem,
                   x_sem, dy_sem, act_sem, h_sem, w_sem, wd_sem, pq_sem, at_sem, xs_sem, dw_sem):
    tokens, width = a.shape
    n, m = act.shape[0], h.shape[0]
    p = Place()
    gather = Gather(p, n, m, (here_gu, here_d), (gu, d), (out_sem, in_sem, here_sem, own_sem))
    copy = pltpu.make_async_copy
    copy(x, a, x_sem).start()
    for layer in range(2):

        def bring(j, c, layer=layer):
            u = j + layer * (n + m)
            copy(w_gate.at[layer, :, block(j)], here_gu.at[layer * n + j, pl.ds(0, 32)], here_sem.at[u]).start()
            copy(w_up.at[layer, :, block(j)], here_gu.at[layer * n + j, pl.ds(32, 32)], here_sem.at[u]).start()
            return c

        lax.fori_loop(0, n, bring, 0)
        for i in range(m):
            u = n + i + layer * (n + m)
            copy(w_down.at[layer, :, pl.ds(i * TILE, TILE)], here_d.at[layer * m + i], here_sem.at[u]).start()
    copy(dy, dyv, dy_sem).start()
    meet(p.neighbours()[:5])

    def transposed(layer, i):
        return copy(ats.at[lax.rem(i, 2)], at_out.at[layer, :, block(i)], at_sem.at[lax.rem(i, 2)])

    def norm(layer, i, wide):
        value = normed(wide)
        a[block(i)] = value
        pl.when(i >= 2)(lambda: transposed(layer, i - 2).wait())
        ats[lax.rem(i, 2)] = value.T
        transposed(layer, i).start()

    def norm_done(layer):
        for i in (tokens // TILE - 2, tokens // TILE - 1):
            transposed(layer, i).wait()

    def start(t, c):
        gather.step(t)

        @pl.when(t == 2)
        def _():
            copy(x, a, x_sem).wait()

        @pl.when((t >= 2) & (t < 2 + tokens // TILE))
        def _():
            norm(0, t - 2, a[block(t - 2)].astype(F32))

        return c

    lax.fori_loop(0, 11, start, 0)
    norm_done(0)

    def w_tile(unit, k):
        return copy(gu.at[unit], wt.at[k], w_sem.at[k])

    def wd_tile(i, k):
        return copy(d.at[i], wdt.at[k], wd_sem.at[k])

    def x_tile(i, k):
        return copy(x.at[:, block(i)], xs.at[k], xs_sem.at[k])

    def pq_tile(layer, j, k):
        return copy(pqs.at[k], pq.at[layer * n + j], pq_sem.at[k])

    def dw_tile(j, k):
        return copy(dws.at[k], dw_out.at[block(j)], dw_sem.at[k])

    def act_tile(j):
        return copy(act.at[j], act_out.at[j], act_sem)

    base = 12 + n + m - 1

    def hidden(layer):
        def body(j, c):
            k = lax.rem(j, 2)
            if layer:

                def more(i, c):
                    pl.when((i == 0) | (lax.rem(j, 3) == 2))(lambda: gather.step(base + j + lax.div(j, 3) + i))
                    return c

                lax.fori_loop(0, 2, more, 0)
            else:
                gather.step(11 + j)

            @pl.when(j < n - 1)
            def _():
                w_tile(layer * n + j + 1, 1 - k).start()

            if layer == 0:

                @pl.when(j == n - 1)
                def _():
                    wd_tile(0, 0).start()
                    x_tile(0, 0).start()

            w_tile(layer * n + j, k).wait()
            pl.when(j >= 2)(lambda: pq_tile(layer, j - 2, k).wait())
            if layer:
                pl.when(j >= 2)(lambda: dw_tile(j - 2, k).wait())
            gate_w, up_w = (wt[k, :, :, :, 32 * i : 32 * i + 32, :].reshape(width, TILE) for i in (0, 1))
            for i in range(tokens // 512):
                rows = pl.ds(512 * i, 512)
                gate, up = dot(a[rows], gate_w), dot(a[rows], up_w)
                s = 0.5 * jnp.tanh(0.5 * gate) + 0.5
                silu = gate * s
                pqs[k, 0, rows] = silu
                pqs[k, 1, rows] = up * (s + silu * (1 - s))
                act[j, rows] = (silu * up).astype(BF16)
            if layer:
                dws[k] = dot(act[j], dyv[...], BY_ROWS).astype(BF16)
                dw_tile(j, k).start()
            else:
                act_tile(j).start()
            pq_tile(layer, j, k).start()
            return c

        lax.fori_loop(0, n, body, 0)
        for j in (n - 2, n - 1):
            pq_tile(layer, j, j % 2).wait()
            if layer:
                dw_tile(j, j % 2).wait()

    w_tile(0, 0).start()
    hidden(0)

    def h_tile(i):
        return copy(h.at[i], h_out.at[:, block(i)], h_sem)

    def down(i, c):
        k = lax.rem(i, 2)
        gather.step(11 + n + i)

        @pl.when(i < m - 1)
        def _():
            wd_tile(i + 1, 1 - k).start()
            x_tile(i + 1, 1 - k).start()

        @pl.when(i == m - 1)
        def _():
            w_tile(n, 0).start()

        wd_tile(i, k).wait()
        x_tile(i, k).wait()
        for r in range(tokens // 512):
            rows = pl.ds(512 * r, 512)
            out = added(dot(act[j, rows], wdt[k, pl.ds(TILE * j, TILE)]) for j in range(n))
            h[i, rows] = xs[k, rows] + out.astype(BF16)
        h_tile(i).start()
        return c

    lax.fori_loop(0, m, down, 0)

    def norm_later(i, c):
        norm(1, i, jnp.concatenate([h[q, block(i)] for q in range(m)], -1).astype(F32))
        return c

    lax.fori_loop(0, tokens // TILE, norm_later, 0)
    norm_done(1)
    copy(act, act_out, act_sem).wait()
    copy(dy, dyv, dy_sem).wait()
    hidden(1)
    gather.steps(base + n + n // 3, max(0, 2 * (n + m) + 10 - (base + n + n // 3)))
    copy(h, h, h_sem).wait()


def forward(x, dy, weights):
    tokens, width = x.shape
    w_gate, w_up, w_down = weights
    hidden, rows = w_gate.shape[-1], w_down.shape[1]
    n, m = hidden // TILE, width // TILE
    layers, pieces = 2, (4, 4, 2, 64, TILE)
    shapes = [
        ((layers * n, *pieces), BF16),
        ((layers * m, hidden, TILE), BF16),
        ((layers * n, 2, tokens, TILE), F32),
        ((n, tokens, TILE), BF16),
        ((layers, width, tokens), BF16),
        ((tokens, width), BF16),
        ((hidden, width), BF16),
    ]

    def twice(*shape, dtype=BF16):
        return pltpu.VMEM((2, *shape), dtype)

    def sems(*shape):
        return pltpu.SemaphoreType.DMA(shape)

    scratch = [
        pltpu.VMEM((tokens, width), BF16),
        pltpu.VMEM((tokens, width), BF16),
        pltpu.VMEM((n, tokens, TILE), BF16),
        twice(*pieces),
        twice(hidden, TILE),
        twice(2, tokens, TILE, dtype=F32),
        pltpu.VMEM((m, tokens, TILE), BF16),
        twice(width, TILE),
        twice(tokens, TILE),
        twice(TILE, width),
        pltpu.VMEM((layers * n, *pieces[3:]), BF16),
        pltpu.VMEM((layers * m, rows, TILE), BF16),
        sems(Gather.SLOTS, 3),
        sems(Gather.SLOTS, 9),
        sems(layers * (n + m)),
        sems(Gather.SLOTS),
    ]
    scratch += [sems() for _ in range(4)] + [sems(2) for _ in range(6)]
    return pl.pallas_call(
        forward_kernel,
        out_shape=[jax.ShapeDtypeStruct(*shape) for shape in shapes],
        in_specs=[pl.BlockSpec(memory_space=pl.ANY)] * 5,
        out_specs=[pl.BlockSpec(memory_space=pl.ANY)] * len(shapes),
        scratch_shapes=scratch,
        compiler_params=pltpu.CompilerParams(collective_id=0, has_side_effects=True, vmem_limit_bytes=VMEM_LIMIT),
        name="forward",
    )(x, dy, w_gate, w_up, w_down)


class Sum:
    @staticmethod
    def scratch(rows, columns):
        half = columns // 2

        def wide(*lead):
            return pltpu.VMEM((2, *lead, rows, columns), F32)

        def sent(*lead):
            return pltpu.VMEM((2, *lead, rows, columns), BF16)

        def part(*lead):
            return pltpu.VMEM((2, *lead, rows, half), BF16)

        return [
            sent(16, 2),
            sent(16),
            wide(4),
            wide(4),
            wide(4),
            sent(4),
            part(4),
            part(4),
            sent(4),
            sent(4),
            sent(4),
            sent(4),
            wide(),
            wide(),
            wide(),
            sent(),
            part(),
            part(),
            sent(),
            sent(),
            sent(),
            sent(),
            sent(4),
            pltpu.SemaphoreType.DMA((2, 12)),
            pltpu.SemaphoreType.DMA((2, 12)),
        ]

    def __init__(self, p, refs, emit):
        self.p, self.emit = p, emit
        (self.term, self.swapped, self.ca, self.cp, self.cm, self.x1, self.r1a, self.r1b, self.x2p, self.x2m, self.r2p, self.r2m) = refs[:12]
        (self.db, self.dp, self.dm, self.y1, self.r3a, self.r3b, self.y2p, self.y2m, self.r4p, self.r4m, self.rx) = refs[12:23]
        self.out_sem, self.in_sem = refs[23:25]
        self.half = self.term.shape[-1] // 2

    def copies(self, hop, k):
        p, h = self.p, self.half

        def one(i, src, dst, place):
            return send(src, dst, self.out_sem.at[k, i], self.in_sem.at[k, i], place)

        low, high = pl.ds(0, h), pl.ds(h, h)
        if hop == 0:
            return [one(0, self.term.at[k, :, 1 - p.core], self.swapped.at[k], p.partner())]
        if hop == 1:
            return [
                one(1, self.x1.at[k, :, :, low], self.r1a.at[k], p.at(NEXT, HERE)),
                one(2, self.x1.at[k, :, :, high], self.r1b.at[k], p.at(LAST, HERE)),
            ]
        if hop == 2:
            return [
                one(3, self.x2p.at[k], self.r2p.at[k], p.at(NEXT, HERE)),
                one(4, self.x2m.at[k], self.r2m.at[k], p.at(LAST, HERE)),
            ]
        if hop == 3:
            return [
                one(5, self.y1.at[k, :, low], self.r3a.at[k], p.at(HERE, NEXT)),
                one(6, self.y1.at[k, :, high], self.r3b.at[k], p.at(HERE, LAST)),
            ]
        if hop == 4:
            return [
                one(7, self.y2p.at[k], self.r4p.at[k], p.at(HERE, NEXT)),
                one(8, self.y2m.at[k], self.r4m.at[k], p.at(HERE, LAST)),
            ]
        return [one(8 + d, self.rx.at[k, p.x], self.rx.at[k, p.x], p.along_x(d)) for d in OTHERS]

    def add(self, hop, k, u):
        p, h = self.p, self.half

        def f(ref, *index):
            return ref[index].astype(F32)

        low, high = slice(0, h), slice(h, None)
        if hop == 1:
            for d, ref in enumerate((self.ca, self.cp, self.x1, self.cm)):
                for e in range(4):
                    chip = p.chips[d][e]
                    ref[k, e] = (f(self.term, k, chip, p.core) + f(self.swapped, k, chip)).astype(ref.dtype)
        if hop == 2:
            for b in range(4):
                self.x2p[k, b, :, low] = (self.cp[k, b, :, low] + f(self.r1a, k, b)).astype(BF16)
                self.x2p[k, b, :, high] = self.cp[k, b, :, high].astype(BF16)
                self.x2m[k, b, :, low] = self.cm[k, b, :, low].astype(BF16)
                self.x2m[k, b, :, high] = (self.cm[k, b, :, high] + f(self.r1b, k, b)).astype(BF16)
        if hop == 3:
            for e, ref in enumerate((self.db, self.dp, self.y1, self.dm)):
                ref[k] = (self.ca[k, e] + f(self.r2p, k, e) + f(self.r2m, k, e)).astype(ref.dtype)
        if hop == 4:
            self.y2p[k, :, low] = (self.dp[k, :, low] + f(self.r3a, k)).astype(BF16)
            self.y2p[k, :, high] = self.dp[k, :, high].astype(BF16)
            self.y2m[k, :, low] = self.dm[k, :, low].astype(BF16)
            self.y2m[k, :, high] = (self.dm[k, :, high] + f(self.r3b, k)).astype(BF16)
        if hop == 5:
            self.rx[k, p.x] = (self.db[k] + f(self.r4p, k) + f(self.r4m, k)).astype(BF16)
        if hop == 6:
            self.emit(u, ((f(self.rx, k, 0) + f(self.rx, k, 1)) + (f(self.rx, k, 2) + f(self.rx, k, 3))).astype(BF16))

    def hop(self, hop, u):
        k = lax.rem(u, 2)
        if hop:
            for copy in self.copies(hop - 1, k):
                copy.wait()
        self.add(hop, k, u)
        if hop < HOPS:
            for copy in self.copies(hop, k):
                copy.start()

    def step(self, t, first, last):
        for hop in range(HOPS, 0, -1):
            u = t - hop
            pl.when((u >= first) & (u < last))(functools.partial(self.hop, hop, u))


def backward_kernel(dy, gu, d, pq, act, at, h, dw1, g_gu, g_d, dgu_out, dw0, dh, av, dwt, load_sem, dh_sem, at_sem, gu_sem, wd_sem, pq_sem, act_sem, dgu_sem, dw_sem, dgc_sem, h_sem, *scratch):
    tokens, width = dh.shape
    n, q = g_gu.shape[0] // 2, g_d.shape[0] // 2
    half = len(scratch) // 2
    copy = pltpu.make_async_copy
    p = Place()
    overlap = 16 * q - dw1.shape[0] // 32

    def keep(out):
        def emit(u, value):
            out[u] = value

        return emit

    sum_gu, sum_d = Sum(p, scratch[:half], keep(g_gu)), Sum(p, scratch[half:], keep(g_d))
    copy(dy, dh, dh_sem).start()
    copy(at.at[1], av, at_sem).start()

    d_rows = dw1.shape[0] // 32

    def d_start(term, s, u):
        def one(i, c):
            rows = pl.ds(pl.multiple_of(d_rows * i + 16 * s - overlap * lax.div(s, q - 1), 8), 16)
            copy(term.at[rows], sum_d.term.at[lax.rem(u, 2), lax.div(i, 2), lax.rem(i, 2)], load_sem).start()
            return c

        lax.fori_loop(0, 32, one, 0)

    def d_step(term, s, first):
        sum_d.step(first + s, first, first + q)

        @pl.when(s < q)
        def _():
            whole = sum_d.term.at[lax.rem(first + s, 2)]
            copy(whole, whole, load_sem).wait()
            sum_d.hop(0, first + s)

        pl.when(s + 1 < q)(lambda: d_start(term, s + 1, first + s + 1))

    def gradients(layer, term, first, d_first):
        def phase(wdt, pqt, dgu):
            m = width // TILE

            def tiles(j, k):
                return [
                    copy(d.at[pl.ds(layer * m, m), block(j)], wdt.at[k], wd_sem.at[k]),
                    copy(pq.at[layer * n + j], pqt.at[k], pq_sem.at[k]),
                ]

            def dgu_tile(j, k):
                return copy(dgu.at[k], dgu_out.at[j], dgu_sem.at[k])

            def body(j, c):
                k = lax.rem(j, 2)
                sum_gu.step(first + j, first, first + n)
                pl.when(k == 0)(lambda: d_step(term, lax.div(j, 2), d_first))

                @pl.when(j < n - 1)
                def _():
                    for one in tiles(j + 1, 1 - k):
                        one.start()

                for one in tiles(j, k):
                    one.wait()
                if layer:
                    pl.when(j >= 2)(lambda: dgu_tile(j - 2, k).wait())
                for i in range(tokens // 512):
                    rows = pl.ds(512 * i, 512)
                    by_act = added(dot(dh[rows, TILE * e : TILE * e + TILE], wdt[k, e], BY_COLUMNS) for e in range(m))
                    by_act = by_act.astype(BF16).astype(F32)
                    dgu[k, 0, rows] = (by_act * pqt[k, 1, rows]).astype(BF16)
                    dgu[k, 1, rows] = (by_act * pqt[k, 0, rows]).astype(BF16)
                slot = lax.rem(first + j, 2)
                for i in range(m):
                    for e in (0, 1):
                        value = dot(av[TILE * i : TILE * i + TILE], dgu[k, e]).astype(BF16)
                        sum_gu.term[slot, 4 * i : 4 * i + 4, :, 32 * e : 32 * e + 32, :] = value.reshape(4, 2, 32, TILE)
                if layer:
                    dgu_tile(j, k).start()
                sum_gu.hop(0, first + j)
                return c

            for one in tiles(0, 0):
                one.start()
            lax.fori_loop(0, n, body, 0)
            if layer:
                for j in (n - 2, n - 1):
                    dgu_tile(j, j % 2).wait()

        pl.run_scoped(
            phase,
            pltpu.VMEM((2, width // TILE, TILE, TILE), BF16),
            pltpu.VMEM((2, 2, tokens, TILE), F32),
            pltpu.VMEM((2, 2, tokens, TILE), BF16),
        )

    def to_states(wv, dgc, hv):
        def rows_in(i, k):
            return [
                copy(dgu_out.at[:, :, block(i)], dgc.at[k], dgc_sem.at[k]),
                copy(h.at[block(i)], hv.at[k], h_sem.at[k]),
            ]

        def body(i, c):
            k = lax.rem(i, 2)
            sum_gu.step(n + i, 0, n)
            d_step(dw1, (n + 1) // 2 + i, 0)

            @pl.when(i < tokens // TILE - 1)
            def _():
                for one in rows_in(i + 1, 1 - k):
                    one.start()

            for one in rows_in(i, k):
                one.wait()
            parts = []
            for e in range(width // TILE):
                two = [
                    added(dot(dgc[k, j, o], wv[j, e, :, :, 32 * o : 32 * o + 32, :].reshape(TILE, TILE), BY_COLUMNS) for j in range(n))
                    for o in (0, 1)
                ]
                parts.append((two[0].astype(BF16) + two[1].astype(BF16)).astype(F32))
            by_a = jnp.concatenate(parts, -1)
            wide = hv[k].astype(F32)
            scale = lax.rsqrt(jnp.mean(wide * wide, -1, keepdims=True) + 1e-6)
            along = jnp.mean(by_a * wide, -1, keepdims=True)
            by_h = by_a * scale - wide * (scale * scale * scale * along)
            dh[block(i)] = dh[block(i)] + by_h.astype(BF16)
            return c

        for one in rows_in(0, 0):
            one.start()
        copy(gu.at[pl.ds(n, n)], wv, gu_sem).start()
        copy(gu.at[pl.ds(n, n)], wv, gu_sem).wait()
        lax.fori_loop(0, tokens // TILE, body, 0)

    def down(acts):
        def tile(j, k):
            return copy(act.at[j], acts.at[k], act_sem.at[k])

        def out(j, k):
            return copy(dwt.at[k], dw0.at[block(j)], dw_sem.at[k])

        def body(j, c):
            k = lax.rem(j, 2)
            pl.when(j < n - 1)(lambda: tile(j + 1, 1 - k).start())
            tile(j, k).wait()
            pl.when(j >= 2)(lambda: out(j - 2, k).wait())
            dwt[k] = dot(acts[k], dh[...], BY_ROWS).astype(BF16)
            out(j, k).start()
            return c

        tile(0, 0).start()
        lax.fori_loop(0, n, body, 0)
        for j in (n - 2, n - 1):
            out(j, j % 2).wait()

    d_start(dw1, 0, 0)
    meet(p.neighbours())
    copy(dy, dh, dh_sem).wait()
    copy(at.at[1], av, at_sem).wait()
    gradients(1, dw1, 0, 0)
    copy(at.at[0], av, at_sem).start()
    pl.run_scoped(
        to_states,
        pltpu.VMEM((n, 4, 4, 2, 64, TILE), BF16),
        pltpu.VMEM((2, n, 2, TILE, TILE), BF16),
        pltpu.VMEM((2, TILE, width), BF16),
    )
    pl.run_scoped(down, pltpu.VMEM((2, tokens, TILE), BF16))
    d_start(dw0, 0, q)
    copy(at.at[0], av, at_sem).wait()
    gradients(0, dw0, n, q)

    def rest(i, c):
        sum_gu.step(2 * n + i, n, 2 * n)
        d_step(dw0, (n + 1) // 2 + i, q)
        return c

    lax.fori_loop(0, HOPS, rest, 0)


def backward(dy, gu, d, pq, act, at, h, dw1):
    tokens, width = dy.shape
    n, hidden = gu.shape[0] // 2, dw1.shape[0]
    q = -(-(hidden // 32) // 16)
    assert q == (n + 1) // 2 and tokens // TILE >= HOPS
    any_space, vmem = pl.BlockSpec(memory_space=pl.ANY), pl.BlockSpec(memory_space=pltpu.VMEM)
    out = pl.pallas_call(
        backward_kernel,
        out_shape=[
            jax.ShapeDtypeStruct((2 * n, 64, TILE), BF16),
            jax.ShapeDtypeStruct((2 * q, 16, width), BF16),
            jax.ShapeDtypeStruct((n, 2, tokens, TILE), BF16),
            jax.ShapeDtypeStruct((hidden, width), BF16),
        ],
        in_specs=[any_space] * 8,
        out_specs=[vmem, vmem, any_space, any_space],
        scratch_shapes=[
            pltpu.VMEM((tokens, width), BF16),
            pltpu.VMEM((width, tokens), BF16),
            pltpu.VMEM((2, TILE, width), BF16),
        ]
        + [pltpu.SemaphoreType.DMA(()) for _ in range(4)]
        + [pltpu.SemaphoreType.DMA((2,)) for _ in range(7)]
        + Sum.scratch(64, TILE)
        + Sum.scratch(16, width),
        compiler_params=pltpu.CompilerParams(collective_id=1, has_side_effects=True, vmem_limit_bytes=VMEM_LIMIT),
        name="backward",
    )(dy, gu, d, pq, act, at, h, dw1)
    g_gu, g_d = out[:2]
    both = g_gu.reshape(2, n, 2, 32, TILE).transpose(0, 2, 3, 1, 4).reshape(2, 2, 32, hidden)
    down = g_d.reshape(2, q * 16, width)
    rows, kept = hidden // 32, 16 * (q - 1)
    down = jnp.concatenate([down[:, : rows - 16], down[:, kept:]], 1)
    return [one[::-1] for one in (both[:, 0], both[:, 1], down)]


def solution(mesh):
    def step(x, dy, *arrays):
        weights, m, v = (arrays[i : i + 3] for i in (0, 3, 6))
        gradients = [g.astype(F32) for g in backward(dy[0], *forward(x[0], dy[0], weights))]
        new = [adamw(w.astype(jnp.float32), m, v, g) for w, m, v, g in zip(weights, m, v, gradients, strict=True)]
        return tuple(one[which] for which in range(3) for one in new)

    states, cut = P(("rep", "r", "s"), None, None), P(None, "s", None)
    return jax.shard_map(
        step,
        mesh=mesh,
        in_specs=(states, states) + (cut,) * 9,
        out_specs=(P("rep", "s", None),) * 9,
        check_vma=False,
    )
```

```python
import functools

import jax
import jax.numpy as jnp
from jax import lax
from jax.experimental import pallas as pl
from jax.experimental.pallas import tpu as pltpu
from jax.sharding import PartitionSpec as P

NAMES = ("w_gate", "w_up", "w_down")
MESH = pl.DeviceIdType.MESH
F32, BF16 = jnp.float32, jnp.bfloat16
HOPS = 6
VMEM_LIMIT = 67043328
PLAIN, BY_COLUMNS, BY_ROWS = (((1,), (0,)), ((), ())), (((1,), (1,)), ((), ())), (((0,), (0,)), ((), ()))
HERE, NEXT, FAR, LAST = range(4)
DOWN = 2
TILE = 256


def adamw(w, m, v, g):
    m = 0.9 * m + 0.1 * g
    v = 0.95 * v + 0.05 * g * g
    step = m * lax.rsqrt(v + 1e-8) + 0.1 * w
    return (w - 0.02 * step).astype(jnp.bfloat16), m, v


def dot(a, b, dims=PLAIN):
    return lax.dot_general(a, b, dims, preferred_element_type=F32)


def scoped(name):
    def wrap(f):
        @functools.wraps(f)
        def inner(*args, **kwargs):
            with jax.named_scope(name):
                return f(*args, **kwargs)

        return inner

    return wrap


def block(n, size=TILE):
    return pl.ds(pl.multiple_of(n * size, size), size)


def added(values):
    total = None
    for value in values:
        total = value if total is None else total + value
    return total


OTHERS = (NEXT, FAR, LAST)


class Place:
    def __init__(self):
        self.s, self.x = lax.axis_index("s"), lax.axis_index("r")
        self.core = lax.rem(self.s, 2)
        y, z = self.yz = lax.div(self.s, 8), lax.rem(lax.div(self.s, 2), 4)
        a = y * (1 - self.core) + z * self.core
        b = z * (1 - self.core) + y * self.core
        step_a, step_b = 4 - 3 * self.core, 1 + 3 * self.core
        self.a, self.b = [[lax.rem(at + d, 4) for d in range(4)] for at in (a, b)]
        self.chips = [[self.a[d] * step_a + self.b[e] * step_b for e in range(4)] for d in range(4)]
        self.devices = {(d, e): 2 * self.chips[d][e] + self.core for d in range(4) for e in range(4)}
        self.across = self.s + 1 - 2 * self.core

    def at(self, d, e):
        return {"s": self.devices[d, e]}

    def partner(self):
        return {"s": self.across}

    def pair(self, second):
        return {"r": 3 - self.x if second else self.x + 1 - 2 * lax.rem(self.x, 2)}

    def neighbours(self, far):
        around = [self.at(*there) for there in ((NEXT, HERE), (LAST, HERE), (HERE, NEXT), (HERE, LAST), *far)]
        return [self.partner()] + around


def meet(places):
    barrier = pltpu.get_barrier_semaphore()
    for place in places:
        pl.semaphore_signal(barrier, inc=1, device_id=place, device_id_type=MESH)
    pl.semaphore_wait(barrier, len(places))


def send(src, dst, send_sem, recv_sem, place):
    return pltpu.make_async_remote_copy(src_ref=src, dst_ref=dst, send_sem=send_sem, recv_sem=recv_sem, device_id=place, device_id_type=MESH)


class Gather:
    SLOTS = 12

    def __init__(self, p, n, m, here, full, sems):
        self.p, self.n, self.m, self.here, self.full = p, n, m, here, full
        self.out_sem, self.in_sem, self.here_sem, self.own_sem = sems
        self.total = 2 * (n + m)

    def hop(self, core, kind, hop, u, later):
        p, k = self.p, lax.rem(u, self.SLOTS)
        at = u - self.n * (1 + later) if kind == DOWN else u - (self.n + self.m) * later
        f = self.full[kind].at[at]
        here = self.here[kind].at[at] if kind else f.at[(*p.yz, core)]
        rows = here.shape[0]
        cut = (rows // 2 + 7) // 8 * 8
        low, high = (0, cut), (cut, rows - cut)

        def piece(d, e, half=(0, rows)):
            if kind == DOWN:
                return f.at[pl.ds(pl.multiple_of(rows * p.devices[d, e], 8) + half[0], half[1])]
            whole = f.at[p.a[d], p.b[e], core] if core == 0 else f.at[p.b[e], p.a[d], core]
            return whole.at[pl.ds(*half)]

        def group(e, half=(0, rows)):
            if kind == DOWN:
                return [piece(d, e, half) for d in range(4)]
            whole = f.at[:, p.b[e], core] if core == 0 else f.at[p.b[e], :, core]
            return [whole.at[:, pl.ds(*half)]]

        def of_size(lines, columns, half=(0, rows)):
            if kind == DOWN:
                return f.at[pl.ds(0, lines * columns * half[1])]
            return f.at[pl.ds(0, lines), pl.ds(0, columns), 0, pl.ds(*half)]

        def go(i, ref, place, left=0, src=None):
            send(ref if src is None else src, ref, self.out_sem.at[k, left], self.in_sem.at[k, i], place).start()

        def over(e):
            for one in group(e):
                go(8, one, p.partner(), FAR)

        def came(sem, ref):
            pltpu.make_async_copy(ref, ref, sem).wait()

        def all_came(i, columns, half=(0, rows)):
            came(self.in_sem.at[k, i], of_size(1, columns, half))

        sides = ((NEXT, LAST, low), (LAST, NEXT, high))
        if hop == 0:
            came(self.here_sem.at[u], here)
            own = piece(HERE, HERE)
            for side, (ahead, _, _) in enumerate(sides):
                go(side, own, p.at(ahead, HERE), src=here)
            if kind:
                pltpu.make_async_copy(here, own, self.own_sem.at[k]).start()
        if hop == 1:
            for side, (ahead, back, half) in enumerate(sides):
                all_came(side, 1)
                go(2 + side, piece(back, HERE, half), p.at(ahead, HERE))
        if hop == 2:
            if kind:
                came(self.own_sem.at[k], piece(HERE, HERE))
            for side, (_, _, half) in enumerate(sides):
                all_came(2 + side, 1, half)
            for one in group(HERE):
                for side, (ahead, _, _) in enumerate(sides):
                    go(4 + side, one, p.at(HERE, ahead), 1)
            over(HERE)
        if hop == 3:
            for side, (ahead, back, half) in enumerate(sides):
                all_came(4 + side, 4)
                for one in group(back, half):
                    go(6 + side, one, p.at(HERE, ahead), 1)
                over(back)
        if hop == 4:
            for side, (_, _, half) in enumerate(sides):
                all_came(6 + side, 4, half)
            over(FAR)
        if hop == 5:
            came(self.in_sem.at[k, 8], of_size(4, 4))
            for i, (lines, columns) in enumerate(((1, 3), (3, 4), (4, 4))):
                came(self.out_sem.at[k, i], of_size(lines, columns))

    EARLY, LATER = 2, 4

    def done(self, u):
        return u + 10 + (self.LATER if u >= self.EARLY else 0)

    @scoped("gather")
    def step(self, t):
        def both(core, hop, u):
            later = lax.div(u, self.n + self.m)
            is_down = u - (self.n + self.m) * later >= self.n
            for layer in range(2):
                pl.when(~is_down & (later == layer))(lambda layer=layer: self.hop(core, layer, hop, u, later))
            pl.when(is_down)(lambda: self.hop(core, DOWN, hop, u, later))

        def run(core):
            for hop in range(5, -1, -1):
                at = t - 2 * hop
                early = at < self.EARLY
                u = jnp.where(early, at, at - self.LATER)
                there = (at >= 0) & (u < self.total) & (early | (u >= self.EARLY))
                pl.when(there)(functools.partial(both, core, hop, u))

        for core in (0, 1):
            pl.when(self.p.core == core)(functools.partial(run, core))

    def steps(self, first, count):
        lax.fori_loop(0, count, lambda i, c: (self.step(first + i), c)[1], 0)


def normed(wide):
    return (wide * lax.rsqrt(jnp.mean(wide * wide, -1, keepdims=True) + 1e-6)).astype(BF16)


def forward_kernel(x, dy, w_gate, w_up, w_down, gu, d, pq, act_out, at_out, h_out, dw_out,
                   a, dyv, act, near, wt, wdt, pqs, h, ats, xs, dws, here, here_d, out_sem, in_sem, here_sem, own_sem,
                   x_sem, dy_sem, act_sem, h_sem, w_sem, wd_sem, pq_sem, at_sem, xs_sem, dw_sem):
    tokens, width = a.shape
    n, m = act.shape[0], h.shape[0]
    p = Place()
    gather = Gather(p, n, m, (None, here, here_d), (near, gu, d), (out_sem, in_sem, here_sem, own_sem))
    copy = pltpu.make_async_copy
    copy(x, a, x_sem).start()
    for layer in range(2):

        def bring(j, c, layer=layer):
            u = j + layer * (n + m)
            own = here.at[j] if layer else near.at[(j, *p.yz, p.core)]
            copy(w_gate.at[layer, :, block(j)], own.at[pl.ds(0, 32)], here_sem.at[u]).start()
            copy(w_up.at[layer, :, block(j)], own.at[pl.ds(32, 32)], here_sem.at[u]).start()
            return c

        lax.fori_loop(0, n, bring, 0)
        for i in range(m):
            u = n + i + layer * (n + m)
            copy(w_down.at[layer, :, pl.ds(i * TILE, TILE)], here_d.at[layer * m + i], here_sem.at[u]).start()
    copy(dy, dyv, dy_sem).start()
    meet(p.neighbours(()))

    def transposed(layer, i):
        return copy(ats.at[lax.rem(i, 2)], at_out.at[layer, :, block(i)], at_sem.at[lax.rem(i, 2)])

    @scoped("norm")
    def norm(layer, i, wide):
        value = normed(wide)
        a[block(i)] = value
        pl.when(i >= 2)(lambda: transposed(layer, i - 2).wait())
        ats[lax.rem(i, 2)] = value.T
        transposed(layer, i).start()

    def norm_done(layer):
        for i in (tokens // TILE - 2, tokens // TILE - 1):
            transposed(layer, i).wait()

    def start(t, c):
        gather.step(t)
        pl.when(t == 1)(lambda: copy(x, a, x_sem).wait())

        @pl.when((t >= 1) & (t <= tokens // TILE))
        def _():
            norm(0, t - 1, a[block(t - 1)].astype(F32))

        return c

    assert gather.done(0) >= tokens // TILE and gather.LATER == 4
    lax.fori_loop(0, gather.done(0) + 1, start, 0)
    norm_done(0)

    def w_tile(j, k):
        return copy(gu.at[j], wt.at[k], w_sem.at[k])

    def wd_tile(i, k):
        return copy(d.at[i], wdt.at[k], wd_sem.at[k])

    def x_tile(i, k):
        return copy(x.at[:, block(i)], xs.at[k], xs_sem.at[k])

    def pq_tile(layer, j, k):
        return copy(pqs.at[k], pq.at[layer * n + j], pq_sem.at[k])

    def dw_tile(j, k):
        return copy(dws.at[k], dw_out.at[block(j)], dw_sem.at[k])

    def act_tile(j):
        return copy(act.at[j], act_out.at[j], act_sem)

    base = gather.done(n + 1) + 2 * m

    def hidden(layer):
        def body(j, c):
            k = lax.rem(j, 2)
            if layer:
                gather.step(base + j)
            else:
                first = jnp.where(j < 3, gather.done(0) + 1 + 3 * (j - 1), gather.done(2) + j - 2)

                def more(i, c):
                    pl.when((j > 0) & ((i == 0) | (j < 3)))(lambda: gather.step(first + i))
                    return c

                lax.fori_loop(0, 3, more, 0)
            if layer:
                pl.when(j < n - 1)(lambda: w_tile(j + 1, 1 - k).start())
                w_tile(j, k).wait()
            else:

                @pl.when(j == n - 1)
                def _():
                    gather.step(gather.done(n))
                    wd_tile(0, 0).start()
                    x_tile(0, 0).start()

            pl.when(j >= 2 - 2 * layer)(lambda: pq_tile(layer, j, k).wait())
            if layer:
                pl.when(j >= 2)(lambda: dw_tile(j - 2, k).wait())
            with jax.named_scope("hidden"):
                w = wt.at[k] if layer else near.at[j]
                gate_w, up_w = (w[:, :, :, 32 * i : 32 * i + 32, :].reshape(width, TILE) for i in range(2))
                for i in range(tokens // 512):
                    rows = pl.ds(512 * i, 512)
                    gate, up = dot(a[rows], gate_w), dot(a[rows], up_w)
                    s = 0.5 * jnp.tanh(0.5 * gate) + 0.5
                    silu = gate * s
                    pqs[k, 0, rows] = silu
                    pqs[k, 1, rows] = up * (s + silu * (1 - s))
                    act[j, rows] = (silu * up).astype(BF16)
            if layer:

                @pl.when(j < n)
                @scoped("down_terms")
                def _():
                    dws[k] = dot(act[j], dyv[...], BY_ROWS).astype(BF16)

                dw_tile(j, k).start()
            else:
                act_tile(j).start()
            pq_tile(layer, j, k).start()
            return c

        lax.fori_loop(0, n, body, 0)
        if layer:
            for j in (n - 2, n - 1):
                pq_tile(layer, j, j % 2).wait()
                dw_tile(j, j % 2).wait()

    hidden(0)

    def h_tile(i):
        return copy(h.at[i], h_out.at[:, block(i)], h_sem)

    def down(i, c):
        k = lax.rem(i, 2)
        for more in range(2):
            gather.step(gather.done(n + 1) + 2 * i + more)

        @pl.when(i < m - 1)
        def _():
            wd_tile(i + 1, 1 - k).start()
            x_tile(i + 1, 1 - k).start()

        @pl.when(i == m - 1)
        def _():
            w_tile(0, 0).start()

        with jax.named_scope("tiles"):
            wd_tile(i, k).wait()
            x_tile(i, k).wait()
        with jax.named_scope("down"):
            for r in range(tokens // 512):
                rows = pl.ds(512 * r, 512)
                out = added(dot(act[j, rows], wdt[k, pl.ds(TILE * j, TILE)]) for j in range(n))
                h[i, rows] = xs[k, rows] + out.astype(BF16)
        h_tile(i).start()
        return c

    lax.fori_loop(0, m, down, 0)

    def norm_later(i, c):
        norm(1, i, jnp.concatenate([h[q, block(i)] for q in range(m)], -1).astype(F32))
        return c

    lax.fori_loop(0, tokens // TILE, norm_later, 0)
    norm_done(1)
    with jax.named_scope("between"):
        copy(act, act_out, act_sem).wait()
        copy(dy, dyv, dy_sem).wait()
    hidden(1)
    gather.steps(base + n, max(0, gather.done(gather.total - 1) + 1 - base - n))
    copy(h, h, h_sem).wait()


def forward(x, dy, weights):
    tokens, width = x.shape
    w_gate, w_up, w_down = weights
    hidden, rows = w_gate.shape[-1], w_down.shape[1]
    n, m = hidden // TILE, width // TILE
    layers, pieces = 2, (4, 4, 2, 64, TILE)
    shapes = [
        ((n, *pieces), BF16),
        ((layers * m, hidden, TILE), BF16),
        ((layers * n, 2, tokens, TILE), F32),
        ((n, tokens, TILE), BF16),
        ((layers, width, tokens), BF16),
        ((tokens, width), BF16),
        ((hidden, width), BF16),
    ]

    def twice(*shape, dtype=BF16):
        return pltpu.VMEM((2, *shape), dtype)

    def sems(*shape):
        return pltpu.SemaphoreType.DMA(shape)

    scratch = [
        pltpu.VMEM((tokens, width), BF16),
        pltpu.VMEM((tokens, width), BF16),
        pltpu.VMEM((n, tokens, TILE), BF16),
        pltpu.VMEM((n, *pieces), BF16),
        twice(*pieces),
        twice(hidden, TILE),
        twice(2, tokens, TILE, dtype=F32),
        pltpu.VMEM((m, tokens, TILE), BF16),
        twice(width, TILE),
        twice(tokens, TILE),
        twice(TILE, width),
        pltpu.VMEM((n, *pieces[3:]), BF16),
        pltpu.VMEM((layers * m, rows, TILE), BF16),
        sems(Gather.SLOTS, 3),
        sems(Gather.SLOTS, 9),
        sems(layers * (n + m)),
        sems(Gather.SLOTS),
    ]
    scratch += [sems() for _ in range(4)] + [sems(2) for _ in range(6)]
    return pl.pallas_call(
        forward_kernel,
        out_shape=[jax.ShapeDtypeStruct(*shape) for shape in shapes],
        in_specs=[pl.BlockSpec(memory_space=pl.ANY)] * 5,
        out_specs=[pl.BlockSpec(memory_space=pl.ANY)] * len(shapes),
        scratch_shapes=scratch,
        compiler_params=pltpu.CompilerParams(collective_id=0, has_side_effects=True, vmem_limit_bytes=VMEM_LIMIT),
        name="forward",
    )(x, dy, w_gate, w_up, w_down)


class Sum:
    @staticmethod
    def scratch(terms, slots, rows, columns):
        def many(slots, *lead, columns=columns, dtype=BF16, count=1):
            return [pltpu.VMEM((slots, *lead, rows, columns), dtype)] * count

        half, near = columns // 2, 2
        return (
            many(terms, 16, 2)
            + many(slots, 16)
            + many(slots, 4, dtype=F32)
            + many(near, 4, dtype=F32, count=2)
            + many(near, 4, count=3)
            + many(slots, 4, columns=half, count=2)
            + many(slots, 4, count=2)
            + many(slots, dtype=F32)
            + many(near, 3)
            + many(slots, 3)
            + many(near, count=2)
            + many(slots, count=2)
            + [pltpu.SemaphoreType.DMA((slots, 10))] * 2
        )

    def __init__(self, p, refs, emit, lag, delay):
        self.p, self.emit, self.lag, self.delay = p, emit, lag, delay
        self.term, self.swapped, self.ca, self.cp, self.cm, self.x1, self.x2p, self.x2m, self.r1a, self.r1b, self.r2p, self.r2m = refs[:12]
        self.db, self.y, self.ry, self.z, self.w, self.rz, self.rw = refs[12:19]
        self.out_sem, self.in_sem = refs[19:]
        self.half = self.term.shape[-1] // 2

    def slot(self, ref, u):
        return ref.at[lax.rem(u, ref.shape[0])]

    def copies(self, hop, u):
        p, h = self.p, self.half
        out_sem, in_sem = self.slot(self.out_sem, u), self.slot(self.in_sem, u)

        def one(i, src, dst, place):
            return send(src, dst, out_sem.at[i], in_sem.at[i], place)

        if hop == 0:
            return [one(0, self.slot(self.term, u).at[:, 1 - p.core], self.slot(self.swapped, u), p.partner())]
        if hop == 3:
            y, ry = self.slot(self.y, u), self.slot(self.ry, u)
            return [one(5 + i, y.at[i], ry.at[i], p.at(HERE, ahead)) for i, ahead in enumerate(OTHERS)]
        if hop > 3:
            second = hop == 5
            src, dst = (self.w, self.rw) if second else (self.z, self.rz)
            return [one(4 + hop, self.slot(src, u), self.slot(dst, u), p.pair(second))]
        sources, landings = ((self.x1, self.x1), (self.r1a, self.r1b)) if hop == 1 else ((self.x2p, self.x2m), (self.r2p, self.r2m))
        made = []
        for side, (src, dst, ahead) in enumerate(zip(sources, landings, (NEXT, LAST), strict=True)):
            src = self.slot(src, u)
            if hop == 1:
                src = src.at[:, :, pl.ds(side * h, h)]
            made.append(one(2 * hop - 1 + side, src, self.slot(dst, u), p.at(ahead, HERE)))
        return made

    def add(self, hop, u):
        p, h = self.p, self.half
        low, high = slice(0, h), slice(h, None)

        def of(ref, *index):
            return ref[(lax.rem(u, ref.shape[0]), *index)].astype(F32)

        def put(ref, value, *index):
            ref[(lax.rem(u, ref.shape[0]), *index)] = value.astype(ref.dtype)

        rows = slice(None)
        if hop == 1:
            for d, ref in enumerate((self.ca, self.cp, self.x1, self.cm)):
                for e in range(4):
                    chip = p.chips[d][e]
                    put(ref, of(self.term, chip, p.core) + of(self.swapped, chip), e)
        if hop == 2:
            for e in range(4):
                put(self.x2p, of(self.cp, e, rows, low) + of(self.r1a, e), e, rows, low)
                put(self.x2p, of(self.cp, e, rows, high), e, rows, high)
                put(self.x2m, of(self.cm, e, rows, low), e, rows, low)
                put(self.x2m, of(self.cm, e, rows, high) + of(self.r1b, e), e, rows, high)
        if hop == 3:
            for e in range(4):
                value = of(self.ca, e) + of(self.r2p, e) + of(self.r2m, e)
                put(self.y, value, e - 1) if e else put(self.db, value)
        if hop == 4:
            put(self.z, (of(self.db) + of(self.ry, 0)) + (of(self.ry, 1) + of(self.ry, 2)))
        if hop == 5:
            put(self.w, of(self.z) + of(self.rz))
        if hop == 6:
            self.emit(u, (of(self.w) + of(self.rw)).astype(BF16))

    def hop(self, hop, u):
        with jax.named_scope(f"hop{hop}"):
            self.do(hop, u)

    def do(self, hop, u):
        if hop:
            for copy in self.copies(hop - 1, u):
                copy.wait()
        self.add(hop, u)
        if hop < HOPS:
            for copy in self.copies(hop, u):
                copy.start()

    def step(self, t, first, last):
        for hop in range(HOPS, -self.delay, -1):
            u = t - self.delay - self.lag * hop
            pl.when((u >= first) & (u < last))(functools.partial(self.hop, hop, u))


def backward_kernel(dy, gu, d, pq, act, at, h, dw1, g_gate, g_up, g_down, dgu_out, dw0, dh, av, big, load_sem, dh_sem, at_sem, big_sem, wd_sem, pq_sem, dgu_sem, dw_sem, dgc_sem, h_sem, *scratch):
    tokens, width = dh.shape
    n, m, d_rows = act.shape[0], width // TILE, g_down.shape[1]
    half = len(scratch) // 2
    copy = pltpu.make_async_copy
    p = Place()

    def emit_gu(u, value):
        later = lax.div(u, n)
        for i, out in enumerate((g_gate, g_up)):
            out[1 - later, :, block(u - n * later)] = value[32 * i : 32 * i + 32]

    def emit_d(u, value):
        later = lax.div(u, m)
        g_down[1 - later, :, block(u - m * later)] = value

    sum_gu, sum_d = Sum(p, scratch[:half], emit_gu, 2, 1), Sum(p, scratch[half:], emit_d, 1, 0)
    copy(dy, dh, dh_sem).start()
    copy(at.at[1], av, at_sem).start()

    def d_start(term, s, first):
        def one(i, c):
            rows = pl.ds(pl.multiple_of(d_rows * i, 8), d_rows)
            copy(term.at[rows, block(s)], sum_d.term.at[lax.rem(first + s, 2), lax.div(i, 2), lax.rem(i, 2)], load_sem).start()
            return c

        lax.fori_loop(0, 32, one, 0)

    def d_step(term, s, first, ready=None):
        sum_d.step(first + s, first, first + m)

        @pl.when(s < m)
        def _():
            whole = sum_d.term.at[lax.rem(first + s, 2)]
            copy(whole, whole, load_sem).wait()
            sum_d.hop(0, first + s)

        @pl.when(s + 1 < m)
        def _():
            if ready is not None:
                ready(s + 1)
            d_start(term, s + 1, first)

    def gradients(layer, first, begin, d_turn):
        def phase(wdt, pqt, dgu):
            def tiles(j, k):
                return [
                    copy(d.at[pl.ds(layer * m, m), block(j)], wdt.at[k], wd_sem.at[k]),
                    copy(pq.at[layer * n + j], pqt.at[k], pq_sem.at[k]),
                ]

            def dgu_tile(j, k):
                return copy(dgu.at[k], dgu_out.at[j], dgu_sem.at[k])

            def body(j, c):
                k = lax.rem(j, 2)
                sum_gu.step(first + j, first, first + n)
                d_turn(j)
                if layer:
                    copy(gu.at[j], big.at[j], big_sem.at[0]).start()

                @pl.when(j < n - 1)
                def _():
                    for one in tiles(j + 1, 1 - k):
                        one.start()

                with jax.named_scope("tiles"):
                    for one in tiles(j, k):
                        one.wait()
                    if layer:
                        pl.when(j >= 2)(lambda: dgu_tile(j - 2, k).wait())
                with jax.named_scope("terms"):
                    for i in range(tokens // 512):
                        rows = pl.ds(512 * i, 512)
                        by_act = added(dot(dh[rows, TILE * e : TILE * e + TILE], wdt[k, e], BY_COLUMNS) for e in range(m))
                        by_act = by_act.astype(BF16).astype(F32)
                        dgu[k, 0, rows] = (by_act * pqt[k, 1, rows]).astype(BF16)
                        dgu[k, 1, rows] = (by_act * pqt[k, 0, rows]).astype(BF16)
                    slot = lax.rem(first + j, sum_gu.term.shape[0])
                    for i in range(m):
                        for e in (0, 1):
                            value = dot(av[TILE * i : TILE * i + TILE], dgu[k, e]).astype(BF16)
                            sum_gu.term[slot, 4 * i : 4 * i + 4, :, 32 * e : 32 * e + 32, :] = value.reshape(4, 2, 32, TILE)
                if layer:
                    dgu_tile(j, k).start()
                return c

            for one in tiles(0, 0):
                one.start()
            begin()
            lax.fori_loop(0, n, body, 0)
            if layer:
                for j in (n - 2, n - 1):
                    dgu_tile(j, j % 2).wait()

        pl.run_scoped(
            phase,
            pltpu.VMEM((2, m, TILE, TILE), BF16),
            pltpu.VMEM((2, 2, tokens, TILE), F32),
            pltpu.VMEM((2, 2, tokens, TILE), BF16),
        )

    def to_states(dgc, hv):
        def rows_in(i, k):
            return [
                copy(dgu_out.at[:, :, block(i)], dgc.at[k], dgc_sem.at[k]),
                copy(h.at[block(i)], hv.at[k], h_sem.at[k]),
            ]

        def body(i, c):
            k = lax.rem(i, 2)
            sum_gu.step(n + i, 0, n)
            pl.when(k == 0)(lambda: d_step(dw1, (n + 1) // 2 + lax.div(i, 2), 0))

            @pl.when(i < tokens // TILE - 1)
            def _():
                for one in rows_in(i + 1, 1 - k):
                    one.start()

            with jax.named_scope("tiles"):
                for one in rows_in(i, k):
                    one.wait()
            with jax.named_scope("states"):
                parts = []
                for e in range(m):
                    weights = [big[j, 2 * TILE * e : 2 * TILE * (e + 1)].reshape(8, 64, TILE) for j in range(n)]
                    two = [
                        added(dot(dgc[k, j, o], weights[j][:, 32 * o : 32 * o + 32].reshape(TILE, TILE), BY_COLUMNS) for j in range(n))
                        for o in (0, 1)
                    ]
                    parts.append((two[0].astype(BF16) + two[1].astype(BF16)).astype(F32))
                by_a = jnp.concatenate(parts, -1)
                wide = hv[k].astype(F32)
                scale = lax.rsqrt(jnp.mean(wide * wide, -1, keepdims=True) + 1e-6)
                along = jnp.mean(by_a * wide, -1, keepdims=True)
                by_h = by_a * scale - wide * (scale * scale * scale * along)
                dh[block(i)] = dh[block(i)] + by_h.astype(BF16)
            return c

        for one in rows_in(0, 0):
            one.start()
        with jax.named_scope("weights"):
            copy(gu, big, big_sem.at[0]).wait()
        lax.fori_loop(0, tokens // TILE, body, 0)

    def down(turned, made):
        def out(e):
            return copy(made.at[lax.rem(e, 2)], dw0.at[:, block(e)], dw_sem.at[lax.rem(e, 2)])

        def body(e, c):
            k = lax.rem(e, 2)
            for i in (0, 1):
                sum_gu.step(n + tokens // TILE + 2 * e + i, 0, n)

            @pl.when(e == 1)
            def _():
                out(0).wait()
                d_start(dw0, 0, m)

            pl.when(e >= 2)(lambda: d_step(dw0, e - 2, m, lambda s: out(s).wait()))
            with jax.named_scope("turn"):
                turned[...] = dh[:, block(e)].T

            pl.when(e == 0)(lambda: copy(act, big, big_sem.at[0]).wait())
            with jax.named_scope("down_terms"):
                for j in range(n):
                    made[k, TILE * j : TILE * (j + 1)] = dot(turned[...], big[j]).astype(BF16).T
            out(e).start()
            return c

        copy(act, big, big_sem.at[0]).start()
        lax.fori_loop(0, m, body, 0)

        def last_turn(j):
            pl.when(lax.rem(j, 2) == 0)(lambda: d_step(dw0, 2 + lax.div(j, 2), m, lambda s: out(s).wait()))

        copy(at.at[0], av, at_sem).wait()
        gradients(0, n, lambda: None, last_turn)

    @scoped("meet")
    def begin():
        meet(p.neighbours(((HERE, FAR),)) + [p.pair(False), p.pair(True)])
        copy(dy, dh, dh_sem).wait()
        copy(at.at[1], av, at_sem).wait()

    def turn(j):
        pl.when(lax.rem(j, 2) == 0)(lambda: d_step(dw1, lax.div(j, 2), 0))

    d_start(dw1, 0, 0)
    gradients(1, 0, begin, turn)
    copy(at.at[0], av, at_sem).start()
    pl.run_scoped(
        to_states,
        pltpu.VMEM((2, n, 2, TILE, TILE), BF16),
        pltpu.VMEM((2, TILE, width), BF16),
    )
    pl.run_scoped(down, pltpu.VMEM((TILE, tokens), BF16), pltpu.VMEM((2, 32 * d_rows, TILE), BF16))

    def rest(i, c):
        sum_gu.step(2 * n + i, n, 2 * n)
        pl.when(i == 1)(lambda: d_step(dw0, (n + 1) // 2 + 2, m, lambda s: None))
        return c

    lax.fori_loop(0, 2 * HOPS + 1, rest, 0)


def backward(dy, gu, d, pq, act, at, h, dw1):
    tokens, width = dy.shape
    n, hidden = gu.shape[0], dw1.shape[0]
    rows, m = hidden // 32, width // TILE
    gu = gu.reshape(n, tokens, TILE)
    assert 32 * 64 == tokens and n + 2 == 3 * m + 3 and 2 * HOPS + 1 <= tokens // TILE + 2 * m
    any_space, vmem = pl.BlockSpec(memory_space=pl.ANY), pl.BlockSpec(memory_space=pltpu.VMEM)
    shapes = [((2, 32, hidden), BF16)] * 2 + [((2, rows, width), BF16), ((n, 2, tokens, TILE), BF16), ((hidden, width), BF16)]
    out = pl.pallas_call(
        backward_kernel,
        out_shape=[jax.ShapeDtypeStruct(*shape) for shape in shapes],
        in_specs=[any_space] * 8,
        out_specs=[vmem] * 3 + [any_space] * 2,
        scratch_shapes=[pltpu.VMEM(shape, BF16) for shape in ((tokens, width), (width, tokens), (n, tokens, TILE))]
        + [pltpu.SemaphoreType.DMA(())] * 3
        + [pltpu.SemaphoreType.DMA((2,))] * 7
        + Sum.scratch(3, 4, 64, TILE)
        + Sum.scratch(2, 2, rows, TILE),
        compiler_params=pltpu.CompilerParams(collective_id=1, has_side_effects=True, vmem_limit_bytes=VMEM_LIMIT),
        name="backward",
    )(dy, gu, d, pq, act, at, h, dw1)
    return out[:3]


def solution(mesh):
    def step(x, dy, *arrays):
        weights, m, v = (arrays[i : i + 3] for i in (0, 3, 6))
        gradients = backward(dy[0], *forward(x[0], dy[0], weights))
        new = [adamw(w.astype(F32), m, v, g.astype(F32)) for w, m, v, g in zip(weights, m, v, gradients, strict=True)]
        return tuple(one[which] for which in range(3) for one in new)

    states, cut = P(("rep", "r", "s"), None, None), P(None, "s", None)
    return jax.shard_map(
        step,
        mesh=mesh,
        in_specs=(states, states) + (cut,) * 9,
        out_specs=(P("rep", "s", None),) * 9,
        check_vma=False,
    )
```

```python
import functools

import jax
import jax.numpy as jnp
from jax import lax
from jax.experimental import pallas as pl
from jax.experimental.pallas import tpu as pltpu
from jax.sharding import PartitionSpec as P

NAMES = ("w_gate", "w_up", "w_down")
MESH = pl.DeviceIdType.MESH
F32, BF16 = jnp.float32, jnp.bfloat16
HOPS = 6
VMEM_LIMIT = 67043328
PLAIN, BY_COLUMNS, BY_ROWS = (((1,), (0,)), ((), ())), (((1,), (1,)), ((), ())), (((0,), (0,)), ((), ()))
HERE, NEXT, FAR, LAST = range(4)
DOWN = 2
TILE = 256


def adamw(w, m, v, g):
    m = 0.9 * m + 0.1 * g
    v = 0.95 * v + 0.05 * g * g
    step = m * lax.rsqrt(v + 1e-8) + 0.1 * w
    return (w - 0.02 * step).astype(jnp.bfloat16), m, v


def dot(a, b, dims=PLAIN):
    return lax.dot_general(a, b, dims, preferred_element_type=F32)


def scoped(name):
    def wrap(f):
        @functools.wraps(f)
        def inner(*args, **kwargs):
            with jax.named_scope(name):
                return f(*args, **kwargs)

        return inner

    return wrap


def block(n, size=TILE):
    return pl.ds(pl.multiple_of(n * size, size), size)


def added(values):
    total = None
    for value in values:
        total = value if total is None else total + value
    return total


OTHERS = (NEXT, FAR, LAST)


class Place:
    def __init__(self):
        self.s, self.x = lax.axis_index("s"), lax.axis_index("r")
        self.core = lax.rem(self.s, 2)
        y, z = self.yz = lax.div(self.s, 8), lax.rem(lax.div(self.s, 2), 4)
        a = y * (1 - self.core) + z * self.core
        b = z * (1 - self.core) + y * self.core
        step_a, step_b = 4 - 3 * self.core, 1 + 3 * self.core
        self.a, self.b = [[lax.rem(at + d, 4) for d in range(4)] for at in (a, b)]
        self.chips = [[self.a[d] * step_a + self.b[e] * step_b for e in range(4)] for d in range(4)]
        self.devices = {(d, e): 2 * self.chips[d][e] + self.core for d in range(4) for e in range(4)}
        self.across = self.s + 1 - 2 * self.core

    def at(self, d, e):
        return {"s": self.devices[d, e]}

    def partner(self):
        return {"s": self.across}

    def pair(self, second):
        return {"r": 3 - self.x if second else self.x + 1 - 2 * lax.rem(self.x, 2)}

    def neighbours(self, far):
        around = [self.at(*there) for there in ((NEXT, HERE), (LAST, HERE), (HERE, NEXT), (HERE, LAST), *far)]
        return [self.partner()] + around


def meet(places):
    barrier = pltpu.get_barrier_semaphore()
    for place in places:
        pl.semaphore_signal(barrier, inc=1, device_id=place, device_id_type=MESH)
    pl.semaphore_wait(barrier, len(places))


def send(src, dst, send_sem, recv_sem, place):
    return pltpu.make_async_remote_copy(src_ref=src, dst_ref=dst, send_sem=send_sem, recv_sem=recv_sem, device_id=place, device_id_type=MESH)


class Gather:
    SLOTS = 12

    def __init__(self, p, n, m, here, full, sems):
        self.p, self.n, self.m, self.here, self.full = p, n, m, here, full
        self.out_sem, self.in_sem, self.here_sem, self.own_sem = sems
        self.total = 2 * (n + m)

    def hop(self, core, kind, hop, u, later):
        p, k = self.p, lax.rem(u, self.SLOTS)
        at = u - self.n * (1 + later) if kind == DOWN else u - (self.n + self.m) * later
        f = self.full[kind].at[at]
        here = self.here[kind].at[at] if kind else f.at[(*p.yz, core)]
        rows = here.shape[0]
        cut = (rows // 2 + 7) // 8 * 8
        low, high = (0, cut), (cut, rows - cut)

        def piece(d, e, half=(0, rows)):
            if kind == DOWN:
                return f.at[pl.ds(pl.multiple_of(rows * p.devices[d, e], 8) + half[0], half[1])]
            whole = f.at[p.a[d], p.b[e], core] if core == 0 else f.at[p.b[e], p.a[d], core]
            return whole.at[pl.ds(*half)]

        def group(e, half=(0, rows)):
            if kind == DOWN:
                return [piece(d, e, half) for d in range(4)]
            whole = f.at[:, p.b[e], core] if core == 0 else f.at[p.b[e], :, core]
            return [whole.at[:, pl.ds(*half)]]

        def of_size(lines, columns, half=(0, rows)):
            if kind == DOWN:
                return f.at[pl.ds(0, lines * columns * half[1])]
            return f.at[pl.ds(0, lines), pl.ds(0, columns), 0, pl.ds(*half)]

        def go(i, ref, place, left=0, src=None):
            send(ref if src is None else src, ref, self.out_sem.at[k, left], self.in_sem.at[k, i], place).start()

        def over(e):
            for one in group(e):
                go(8, one, p.partner(), FAR)

        def came(sem, ref):
            pltpu.make_async_copy(ref, ref, sem).wait()

        def all_came(i, columns, half=(0, rows)):
            came(self.in_sem.at[k, i], of_size(1, columns, half))

        sides = ((NEXT, LAST, low), (LAST, NEXT, high))
        if hop == 0:
            came(self.here_sem.at[u], here)
            own = piece(HERE, HERE)
            for side, (ahead, _, _) in enumerate(sides):
                go(side, own, p.at(ahead, HERE), src=here)
            if kind:
                pltpu.make_async_copy(here, own, self.own_sem.at[k]).start()
        if hop == 1:
            for side, (ahead, back, half) in enumerate(sides):
                all_came(side, 1)
                go(2 + side, piece(back, HERE, half), p.at(ahead, HERE))
        if hop == 2:
            if kind:
                came(self.own_sem.at[k], piece(HERE, HERE))
            for side, (_, _, half) in enumerate(sides):
                all_came(2 + side, 1, half)
            for one in group(HERE):
                for side, (ahead, _, _) in enumerate(sides):
                    go(4 + side, one, p.at(HERE, ahead), 1)
            over(HERE)
        if hop == 3:
            for side, (ahead, back, half) in enumerate(sides):
                all_came(4 + side, 4)
                for one in group(back, half):
                    go(6 + side, one, p.at(HERE, ahead), 1)
                over(back)
        if hop == 4:
            for side, (_, _, half) in enumerate(sides):
                all_came(6 + side, 4, half)
            over(FAR)
        if hop == 5:
            came(self.in_sem.at[k, 8], of_size(4, 4))
            for i, (lines, columns) in enumerate(((1, 3), (3, 4), (4, 4))):
                came(self.out_sem.at[k, i], of_size(lines, columns))

    def done(self, u):
        return u + 10

    @scoped("gather")
    def step(self, t):
        def both(core, hop, u):
            later = lax.div(u, self.n + self.m)
            is_down = u - (self.n + self.m) * later >= self.n
            for layer in range(2):
                pl.when(~is_down & (later == layer))(lambda layer=layer: self.hop(core, layer, hop, u, later))
            pl.when(is_down)(lambda: self.hop(core, DOWN, hop, u, later))

        def run(core):
            for hop in range(5, -1, -1):
                u = t - 2 * hop
                pl.when((u >= 0) & (u < self.total))(functools.partial(both, core, hop, u))

        for core in (0, 1):
            pl.when(self.p.core == core)(functools.partial(run, core))

    def steps(self, first, count):
        lax.fori_loop(0, count, lambda i, c: (self.step(first + i), c)[1], 0)


def normed(wide):
    return (wide * lax.rsqrt(jnp.mean(wide * wide, -1, keepdims=True) + 1e-6)).astype(BF16)


def forward_kernel(x, dy, w_gate, w_up, w_down, gu, d, pq, act_out, at_out, h_out, dw_out,
                   a, dyv, act, near, wt, wdt, pqs, h, ats, xs, dws, here, here_d, out_sem, in_sem, here_sem, own_sem,
                   x_sem, dy_sem, act_sem, h_sem, w_sem, wd_sem, pq_sem, at_sem, xs_sem, dw_sem):
    tokens, width = a.shape
    n, m = act.shape[0], h.shape[0]
    p = Place()
    gather = Gather(p, n, m, (None, here, here_d), (near, gu, d), (out_sem, in_sem, here_sem, own_sem))
    copy = pltpu.make_async_copy
    copy(x, a, x_sem).start()
    for layer in range(2):

        def bring(j, c, layer=layer):
            u = j + layer * (n + m)
            own = here.at[j] if layer else near.at[(j, *p.yz, p.core)]
            copy(w_gate.at[layer, :, block(j)], own.at[pl.ds(0, 32)], here_sem.at[u]).start()
            copy(w_up.at[layer, :, block(j)], own.at[pl.ds(32, 32)], here_sem.at[u]).start()
            return c

        lax.fori_loop(0, n, bring, 0)
        for i in range(m):
            u = n + i + layer * (n + m)
            copy(w_down.at[layer, :, pl.ds(i * TILE, TILE)], here_d.at[layer * m + i], here_sem.at[u]).start()
    copy(dy, dyv, dy_sem).start()
    meet(p.neighbours(()))

    def transposed(layer, i):
        return copy(ats.at[lax.rem(i, 2)], at_out.at[layer, :, block(i)], at_sem.at[lax.rem(i, 2)])

    @scoped("norm")
    def norm(layer, i, wide):
        value = normed(wide)
        a[block(i)] = value
        pl.when(i >= 2)(lambda: transposed(layer, i - 2).wait())
        ats[lax.rem(i, 2)] = value.T
        transposed(layer, i).start()

    def norm_done(layer):
        for i in (tokens // TILE - 2, tokens // TILE - 1):
            transposed(layer, i).wait()

    def start(t, c):
        gather.step(t)
        pl.when(t == 1)(lambda: copy(x, a, x_sem).wait())

        @pl.when((t >= 1) & (t <= tokens // TILE))
        def _():
            norm(0, t - 1, a[block(t - 1)].astype(F32))

        return c

    assert gather.done(0) >= tokens // TILE
    lax.fori_loop(0, gather.done(0), start, 0)
    norm_done(0)

    def w_tile(j, k):
        return copy(gu.at[j], wt.at[k], w_sem.at[k])

    def wd_tile(i, k):
        return copy(d.at[i], wdt.at[k], wd_sem.at[k])

    def x_tile(i, k):
        return copy(x.at[:, block(i)], xs.at[k], xs_sem.at[k])

    def pq_tile(layer, j, k):
        return copy(pqs.at[k], pq.at[layer * n + j], pq_sem.at[k])

    def dw_tile(j, k):
        return copy(dws.at[k], dw_out.at[block(j)], dw_sem.at[k])

    def act_tile(j):
        return copy(act.at[j], act_out.at[j], act_sem)

    base = gather.done(n + 1) + 2 * m

    def hidden(layer):
        def body(j, c):
            k = lax.rem(j, 2)
            gather.step(base + j if layer else gather.done(0) + j)
            if layer:
                pl.when(j < n - 1)(lambda: w_tile(j + 1, 1 - k).start())
                w_tile(j, k).wait()
            else:

                @pl.when(j == n - 1)
                def _():
                    gather.step(gather.done(n))
                    wd_tile(0, 0).start()
                    x_tile(0, 0).start()

            pl.when(j >= 2 - 2 * layer)(lambda: pq_tile(layer, j, k).wait())
            if layer:
                pl.when(j >= 2)(lambda: dw_tile(j - 2, k).wait())
            with jax.named_scope("hidden"):
                w = wt.at[k] if layer else near.at[j]
                gate_w, up_w = (w[:, :, :, 32 * i : 32 * i + 32, :].reshape(width, TILE) for i in range(2))
                for i in range(tokens // 512):
                    rows = pl.ds(512 * i, 512)
                    gate, up = dot(a[rows], gate_w), dot(a[rows], up_w)
                    s = 0.5 * jnp.tanh(0.5 * gate) + 0.5
                    silu = gate * s
                    pqs[k, 0, rows] = silu
                    pqs[k, 1, rows] = up * (s + silu * (1 - s))
                    act[j, rows] = (silu * up).astype(BF16)
            if layer:

                @pl.when(j < n)
                @scoped("down_terms")
                def _():
                    dws[k] = dot(act[j], dyv[...], BY_ROWS).astype(BF16)

                dw_tile(j, k).start()
            else:
                act_tile(j).start()
            pq_tile(layer, j, k).start()
            return c

        lax.fori_loop(0, n, body, 0)
        if layer:
            for j in (n - 2, n - 1):
                pq_tile(layer, j, j % 2).wait()
                dw_tile(j, j % 2).wait()

    hidden(0)

    def h_tile(i):
        return copy(h.at[i], h_out.at[:, block(i)], h_sem)

    def down(i, c):
        k = lax.rem(i, 2)
        for more in range(2):
            gather.step(gather.done(n + 1) + 2 * i + more)

        @pl.when(i < m - 1)
        def _():
            wd_tile(i + 1, 1 - k).start()
            x_tile(i + 1, 1 - k).start()

        @pl.when(i == m - 1)
        def _():
            w_tile(0, 0).start()

        with jax.named_scope("tiles"):
            wd_tile(i, k).wait()
            x_tile(i, k).wait()
        with jax.named_scope("down"):
            for r in range(tokens // 512):
                rows = pl.ds(512 * r, 512)
                out = added(dot(act[j, rows], wdt[k, pl.ds(TILE * j, TILE)]) for j in range(n))
                h[i, rows] = xs[k, rows] + out.astype(BF16)
        h_tile(i).start()
        return c

    lax.fori_loop(0, m, down, 0)

    def norm_later(i, c):
        norm(1, i, jnp.concatenate([h[q, block(i)] for q in range(m)], -1).astype(F32))
        return c

    lax.fori_loop(0, tokens // TILE, norm_later, 0)
    norm_done(1)
    with jax.named_scope("between"):
        copy(act, act_out, act_sem).wait()
        copy(dy, dyv, dy_sem).wait()
    hidden(1)
    gather.steps(base + n, max(0, gather.done(gather.total - 1) + 1 - base - n))
    copy(h, h, h_sem).wait()


def forward(x, dy, weights):
    tokens, width = x.shape
    w_gate, w_up, w_down = weights
    hidden, rows = w_gate.shape[-1], w_down.shape[1]
    n, m = hidden // TILE, width // TILE
    layers, pieces = 2, (4, 4, 2, 64, TILE)
    shapes = [
        ((n, *pieces), BF16),
        ((layers * m, hidden, TILE), BF16),
        ((layers * n, 2, tokens, TILE), F32),
        ((n, tokens, TILE), BF16),
        ((layers, width, tokens), BF16),
        ((tokens, width), BF16),
        ((hidden, width), BF16),
    ]

    def twice(*shape, dtype=BF16):
        return pltpu.VMEM((2, *shape), dtype)

    def sems(*shape):
        return pltpu.SemaphoreType.DMA(shape)

    scratch = [
        pltpu.VMEM((tokens, width), BF16),
        pltpu.VMEM((tokens, width), BF16),
        pltpu.VMEM((n, tokens, TILE), BF16),
        pltpu.VMEM((n, *pieces), BF16),
        twice(*pieces),
        twice(hidden, TILE),
        twice(2, tokens, TILE, dtype=F32),
        pltpu.VMEM((m, tokens, TILE), BF16),
        twice(width, TILE),
        twice(tokens, TILE),
        twice(TILE, width),
        pltpu.VMEM((n, *pieces[3:]), BF16),
        pltpu.VMEM((layers * m, rows, TILE), BF16),
        sems(Gather.SLOTS, 3),
        sems(Gather.SLOTS, 9),
        sems(layers * (n + m)),
        sems(Gather.SLOTS),
    ]
    scratch += [sems() for _ in range(4)] + [sems(2) for _ in range(6)]
    return pl.pallas_call(
        forward_kernel,
        out_shape=[jax.ShapeDtypeStruct(*shape) for shape in shapes],
        in_specs=[pl.BlockSpec(memory_space=pl.ANY)] * 5,
        out_specs=[pl.BlockSpec(memory_space=pl.ANY)] * len(shapes),
        scratch_shapes=scratch,
        compiler_params=pltpu.CompilerParams(collective_id=0, has_side_effects=True, vmem_limit_bytes=VMEM_LIMIT),
        name="forward",
    )(x, dy, w_gate, w_up, w_down)


class Sum:
    @staticmethod
    def scratch(terms, slots, rows, columns):
        def many(slots, *lead, columns=columns, dtype=BF16, count=1):
            return [pltpu.VMEM((slots, *lead, rows, columns), dtype)] * count

        half, near = columns // 2, 2
        return (
            many(terms, 16, 2)
            + many(slots, 16)
            + many(slots, 4, dtype=F32)
            + many(near, 4, dtype=F32, count=2)
            + many(near, 4, count=3)
            + many(slots, 4, columns=half, count=2)
            + many(slots, 4, count=2)
            + many(slots, dtype=F32)
            + many(near, 3)
            + many(slots, 3)
            + many(near, count=2)
            + many(slots, count=2)
            + [pltpu.SemaphoreType.DMA((slots, 10))] * 2
        )

    def __init__(self, p, refs, emit, lag, delay):
        self.p, self.emit, self.lag, self.delay = p, emit, lag, delay
        self.term, self.swapped, self.ca, self.cp, self.cm, self.x1, self.x2p, self.x2m, self.r1a, self.r1b, self.r2p, self.r2m = refs[:12]
        self.db, self.y, self.ry, self.z, self.w, self.rz, self.rw = refs[12:19]
        self.out_sem, self.in_sem = refs[19:]
        self.half = self.term.shape[-1] // 2

    def slot(self, ref, u):
        return ref.at[lax.rem(u, ref.shape[0])]

    def copies(self, hop, u):
        p, h = self.p, self.half
        out_sem, in_sem = self.slot(self.out_sem, u), self.slot(self.in_sem, u)

        def one(i, src, dst, place):
            return send(src, dst, out_sem.at[i], in_sem.at[i], place)

        if hop == 0:
            return [one(0, self.slot(self.term, u).at[:, 1 - p.core], self.slot(self.swapped, u), p.partner())]
        if hop == 3:
            y, ry = self.slot(self.y, u), self.slot(self.ry, u)
            return [one(5 + i, y.at[i], ry.at[i], p.at(HERE, ahead)) for i, ahead in enumerate(OTHERS)]
        if hop > 3:
            second = hop == 5
            src, dst = (self.w, self.rw) if second else (self.z, self.rz)
            return [one(4 + hop, self.slot(src, u), self.slot(dst, u), p.pair(second))]
        sources, landings = ((self.x1, self.x1), (self.r1a, self.r1b)) if hop == 1 else ((self.x2p, self.x2m), (self.r2p, self.r2m))
        made = []
        for side, (src, dst, ahead) in enumerate(zip(sources, landings, (NEXT, LAST), strict=True)):
            src = self.slot(src, u)
            if hop == 1:
                src = src.at[:, :, pl.ds(side * h, h)]
            made.append(one(2 * hop - 1 + side, src, self.slot(dst, u), p.at(ahead, HERE)))
        return made

    def add(self, hop, u):
        p, h = self.p, self.half
        low, high = slice(0, h), slice(h, None)

        def of(ref, *index):
            return ref[(lax.rem(u, ref.shape[0]), *index)].astype(F32)

        def put(ref, value, *index):
            ref[(lax.rem(u, ref.shape[0]), *index)] = value.astype(ref.dtype)

        rows = slice(None)
        if hop == 1:
            for d, ref in enumerate((self.ca, self.cp, self.x1, self.cm)):
                for e in range(4):
                    chip = p.chips[d][e]
                    put(ref, of(self.term, chip, p.core) + of(self.swapped, chip), e)
        if hop == 2:
            for e in range(4):
                put(self.x2p, of(self.cp, e, rows, low) + of(self.r1a, e), e, rows, low)
                put(self.x2p, of(self.cp, e, rows, high), e, rows, high)
                put(self.x2m, of(self.cm, e, rows, low), e, rows, low)
                put(self.x2m, of(self.cm, e, rows, high) + of(self.r1b, e), e, rows, high)
        if hop == 3:
            for e in range(4):
                value = of(self.ca, e) + of(self.r2p, e) + of(self.r2m, e)
                put(self.y, value, e - 1) if e else put(self.db, value)
        if hop == 4:
            put(self.z, (of(self.db) + of(self.ry, 0)) + (of(self.ry, 1) + of(self.ry, 2)))
        if hop == 5:
            put(self.w, of(self.z) + of(self.rz))
        if hop == 6:
            self.emit(u, (of(self.w) + of(self.rw)).astype(BF16))

    def hop(self, hop, u):
        with jax.named_scope(f"hop{hop}"):
            self.do(hop, u)

    def do(self, hop, u):
        if hop:
            for copy in self.copies(hop - 1, u):
                copy.wait()
        self.add(hop, u)
        if hop < HOPS:
            for copy in self.copies(hop, u):
                copy.start()

    def step(self, t, first, last):
        for hop in range(HOPS, -self.delay, -1):
            u = t - self.delay - self.lag * hop
            pl.when((u >= first) & (u < last))(functools.partial(self.hop, hop, u))


def backward_kernel(dy, gu, d, pq, act, at, h, dw1, g_gate, g_up, g_down, dgu_out, dw0, dh, av, big, load_sem, dh_sem, at_sem, big_sem, wd_sem, pq_sem, dgu_sem, dw_sem, dgc_sem, h_sem, *scratch):
    tokens, width = dh.shape
    n, m, d_rows = act.shape[0], width // TILE, g_down.shape[1]
    half = len(scratch) // 2
    copy = pltpu.make_async_copy
    p = Place()

    def emit_gu(u, value):
        later = lax.div(u, n)
        for i, out in enumerate((g_gate, g_up)):
            out[1 - later, :, block(u - n * later)] = value[32 * i : 32 * i + 32]

    def emit_d(u, value):
        later = lax.div(u, m)
        g_down[1 - later, :, block(u - m * later)] = value

    sum_gu, sum_d = Sum(p, scratch[:half], emit_gu, 2, 1), Sum(p, scratch[half:], emit_d, 1, 0)
    copy(dy, dh, dh_sem).start()
    copy(at.at[1], av, at_sem).start()

    def d_start(term, s, first):
        def one(i, c):
            rows = pl.ds(pl.multiple_of(d_rows * i, 8), d_rows)
            copy(term.at[rows, block(s)], sum_d.term.at[lax.rem(first + s, 2), lax.div(i, 2), lax.rem(i, 2)], load_sem).start()
            return c

        lax.fori_loop(0, 32, one, 0)

    def d_step(term, s, first, ready=None):
        sum_d.step(first + s, first, first + m)

        @pl.when(s < m)
        def _():
            whole = sum_d.term.at[lax.rem(first + s, 2)]
            copy(whole, whole, load_sem).wait()
            sum_d.hop(0, first + s)

        @pl.when(s + 1 < m)
        def _():
            if ready is not None:
                ready(s + 1)
            d_start(term, s + 1, first)

    def gradients(layer, first, begin, d_turn):
        def phase(wdt, pqt, dgu):
            def tiles(j, k):
                return [
                    copy(d.at[pl.ds(layer * m, m), block(j)], wdt.at[k], wd_sem.at[k]),
                    copy(pq.at[layer * n + j], pqt.at[k], pq_sem.at[k]),
                ]

            def dgu_tile(j, k):
                return copy(dgu.at[k], dgu_out.at[j], dgu_sem.at[k])

            def body(j, c):
                k = lax.rem(j, 2)
                sum_gu.step(first + j, first, first + n)
                d_turn(j)
                if layer:
                    copy(gu.at[j], big.at[j], big_sem.at[0]).start()

                @pl.when(j < n - 1)
                def _():
                    for one in tiles(j + 1, 1 - k):
                        one.start()

                with jax.named_scope("tiles"):
                    for one in tiles(j, k):
                        one.wait()
                    if layer:
                        pl.when(j >= 2)(lambda: dgu_tile(j - 2, k).wait())
                with jax.named_scope("terms"):
                    for i in range(tokens // 512):
                        rows = pl.ds(512 * i, 512)
                        by_act = added(dot(dh[rows, TILE * e : TILE * e + TILE], wdt[k, e], BY_COLUMNS) for e in range(m))
                        by_act = by_act.astype(BF16).astype(F32)
                        dgu[k, 0, rows] = (by_act * pqt[k, 1, rows]).astype(BF16)
                        dgu[k, 1, rows] = (by_act * pqt[k, 0, rows]).astype(BF16)
                    slot = lax.rem(first + j, sum_gu.term.shape[0])
                    for i in range(m):
                        for e in (0, 1):
                            value = dot(av[TILE * i : TILE * i + TILE], dgu[k, e]).astype(BF16)
                            sum_gu.term[slot, 4 * i : 4 * i + 4, :, 32 * e : 32 * e + 32, :] = value.reshape(4, 2, 32, TILE)
                if layer:
                    dgu_tile(j, k).start()
                return c

            for one in tiles(0, 0):
                one.start()
            begin()
            lax.fori_loop(0, n, body, 0)
            if layer:
                for j in (n - 2, n - 1):
                    dgu_tile(j, j % 2).wait()

        pl.run_scoped(
            phase,
            pltpu.VMEM((2, m, TILE, TILE), BF16),
            pltpu.VMEM((2, 2, tokens, TILE), F32),
            pltpu.VMEM((2, 2, tokens, TILE), BF16),
        )

    def to_states(dgc, hv):
        def rows_in(i, k):
            return [
                copy(dgu_out.at[:, :, block(i)], dgc.at[k], dgc_sem.at[k]),
                copy(h.at[block(i)], hv.at[k], h_sem.at[k]),
            ]

        def body(i, c):
            k = lax.rem(i, 2)
            sum_gu.step(n + i, 0, n)
            pl.when(k == 0)(lambda: d_step(dw1, (n + 1) // 2 + lax.div(i, 2), 0))

            @pl.when(i < tokens // TILE - 1)
            def _():
                for one in rows_in(i + 1, 1 - k):
                    one.start()

            with jax.named_scope("tiles"):
                for one in rows_in(i, k):
                    one.wait()
            with jax.named_scope("states"):
                parts = []
                for e in range(m):
                    weights = [big[j, 2 * TILE * e : 2 * TILE * (e + 1)].reshape(8, 64, TILE) for j in range(n)]
                    two = [
                        added(dot(dgc[k, j, o], weights[j][:, 32 * o : 32 * o + 32].reshape(TILE, TILE), BY_COLUMNS) for j in range(n))
                        for o in (0, 1)
                    ]
                    parts.append((two[0].astype(BF16) + two[1].astype(BF16)).astype(F32))
                by_a = jnp.concatenate(parts, -1)
                wide = hv[k].astype(F32)
                scale = lax.rsqrt(jnp.mean(wide * wide, -1, keepdims=True) + 1e-6)
                along = jnp.mean(by_a * wide, -1, keepdims=True)
                by_h = by_a * scale - wide * (scale * scale * scale * along)
                dh[block(i)] = dh[block(i)] + by_h.astype(BF16)
            return c

        for one in rows_in(0, 0):
            one.start()
        with jax.named_scope("weights"):
            copy(gu, big, big_sem.at[0]).wait()
        lax.fori_loop(0, tokens // TILE, body, 0)

    def down(turned, made, load_sems):
        def out(e):
            return copy(made.at[lax.rem(e, 2)], dw0.at[:, block(e)], dw_sem.at[lax.rem(e, 2)])

        def body(e, c):
            k = lax.rem(e, 2)
            for i in (0, 1):
                sum_gu.step(n + tokens // TILE + 2 * e + i, 0, n)

            @pl.when(e == 1)
            def _():
                out(0).wait()
                d_start(dw0, 0, m)

            pl.when(e >= 2)(lambda: d_step(dw0, e - 2, m, lambda s: out(s).wait()))
            with jax.named_scope("turn"):
                turned[...] = dh[:, block(e)].T

            with jax.named_scope("down_terms"):

                @pl.when(e == 0)
                def _():
                    def one(j, c):
                        copy(act.at[j], big.at[j], load_sems.at[j]).wait()
                        made[k, block(j)] = dot(turned[...], big[j]).astype(BF16).T
                        return c

                    lax.fori_loop(0, n, one, 0)

                @pl.when(e > 0)
                def _():
                    for j in range(n):
                        made[k, TILE * j : TILE * (j + 1)] = dot(turned[...], big[j]).astype(BF16).T

            out(e).start()
            return c

        for j in range(n):
            copy(act.at[j], big.at[j], load_sems.at[j]).start()
        lax.fori_loop(0, m, body, 0)

        def last_turn(j):
            pl.when(lax.rem(j, 2) == 0)(lambda: d_step(dw0, 2 + lax.div(j, 2), m, lambda s: out(s).wait()))

        copy(at.at[0], av, at_sem).wait()
        gradients(0, n, lambda: None, last_turn)

    @scoped("meet")
    def begin():
        meet(p.neighbours(((HERE, FAR),)) + [p.pair(False), p.pair(True)])
        copy(dy, dh, dh_sem).wait()
        copy(at.at[1], av, at_sem).wait()

    def turn(j):
        pl.when(lax.rem(j, 2) == 0)(lambda: d_step(dw1, lax.div(j, 2), 0))

    d_start(dw1, 0, 0)
    gradients(1, 0, begin, turn)
    copy(at.at[0], av, at_sem).start()
    pl.run_scoped(
        to_states,
        pltpu.VMEM((2, n, 2, TILE, TILE), BF16),
        pltpu.VMEM((2, TILE, width), BF16),
    )
    pl.run_scoped(down, pltpu.VMEM((TILE, tokens), BF16), pltpu.VMEM((2, 32 * d_rows, TILE), BF16), pltpu.SemaphoreType.DMA((n,)))

    def rest(i, c):
        sum_gu.step(2 * n + i, n, 2 * n)
        pl.when(i == 1)(lambda: d_step(dw0, (n + 1) // 2 + 2, m, lambda s: None))
        return c

    lax.fori_loop(0, 2 * HOPS + 1, rest, 0)


def backward(dy, gu, d, pq, act, at, h, dw1):
    tokens, width = dy.shape
    n, hidden = gu.shape[0], dw1.shape[0]
    rows, m = hidden // 32, width // TILE
    gu = gu.reshape(n, tokens, TILE)
    assert 32 * 64 == tokens and n + 2 == 3 * m + 3 and 2 * HOPS + 1 <= tokens // TILE + 2 * m
    any_space, vmem = pl.BlockSpec(memory_space=pl.ANY), pl.BlockSpec(memory_space=pltpu.VMEM)
    shapes = [((2, 32, hidden), BF16)] * 2 + [((2, rows, width), BF16), ((n, 2, tokens, TILE), BF16), ((hidden, width), BF16)]
    out = pl.pallas_call(
        backward_kernel,
        out_shape=[jax.ShapeDtypeStruct(*shape) for shape in shapes],
        in_specs=[any_space] * 8,
        out_specs=[vmem] * 3 + [any_space] * 2,
        scratch_shapes=[pltpu.VMEM(shape, BF16) for shape in ((tokens, width), (width, tokens), (n, tokens, TILE))]
        + [pltpu.SemaphoreType.DMA(())] * 3
        + [pltpu.SemaphoreType.DMA((2,))] * 7
        + Sum.scratch(3, 4, 64, TILE)
        + Sum.scratch(2, 2, rows, TILE),
        compiler_params=pltpu.CompilerParams(collective_id=1, has_side_effects=True, vmem_limit_bytes=VMEM_LIMIT),
        name="backward",
    )(dy, gu, d, pq, act, at, h, dw1)
    return out[:3]


def solution(mesh):
    def step(x, dy, *arrays):
        weights, m, v = (arrays[i : i + 3] for i in (0, 3, 6))
        gradients = backward(dy[0], *forward(x[0], dy[0], weights))
        new = [adamw(w.astype(F32), m, v, g.astype(F32)) for w, m, v, g in zip(weights, m, v, gradients, strict=True)]
        return tuple(one[which] for which in range(3) for one in new)

    states, cut = P(("rep", "r", "s"), None, None), P(None, "s", None)
    return jax.shard_map(
        step,
        mesh=mesh,
        in_specs=(states, states) + (cut,) * 9,
        out_specs=(P("rep", "s", None),) * 9,
        check_vma=False,
    )
```

```python
import functools

import jax
import jax.numpy as jnp
from jax import lax
from jax.experimental import pallas as pl
from jax.experimental.pallas import tpu as pltpu
from jax.sharding import PartitionSpec as P

NAMES = ("w_gate", "w_up", "w_down")
MESH = pl.DeviceIdType.MESH
F32, BF16 = jnp.float32, jnp.bfloat16
HOPS = 5
VMEM_LIMIT = 67043328
PLAIN, BY_COLUMNS, BY_ROWS = (((1,), (0,)), ((), ())), (((1,), (1,)), ((), ())), (((0,), (0,)), ((), ()))
HERE, NEXT, FAR, LAST = range(4)
TILE = 256


def adamw(w, m, v, g):
    m = 0.9 * m + 0.1 * g
    v = 0.95 * v + 0.05 * g * g
    step = m * lax.rsqrt(v + 1e-8) + 0.1 * w
    return (w - 0.02 * step).astype(jnp.bfloat16), m, v


def dot(a, b, dims=PLAIN):
    return lax.dot_general(a, b, dims, preferred_element_type=F32)


def scoped(name):
    def wrap(f):
        @functools.wraps(f)
        def inner(*args, **kwargs):
            with jax.named_scope(name):
                return f(*args, **kwargs)

        return inner

    return wrap


def block(n, size=TILE):
    return pl.ds(pl.multiple_of(n * size, size), size)


def added(values):
    total = None
    for value in values:
        total = value if total is None else total + value
    return total


OTHERS = (NEXT, FAR, LAST)


class Place:
    def __init__(self):
        self.s, self.x = lax.axis_index("s"), lax.axis_index("r")
        self.core = lax.rem(self.s, 2)
        y, z = lax.div(self.s, 8), lax.rem(lax.div(self.s, 2), 4)
        a = y * (1 - self.core) + z * self.core
        b = z * (1 - self.core) + y * self.core
        step_a, step_b = 4 - 3 * self.core, 1 + 3 * self.core
        self.a, self.b = [[lax.rem(at + d, 4) for d in range(4)] for at in (a, b)]
        self.chips = [[self.a[d] * step_a + self.b[e] * step_b for e in range(4)] for d in range(4)]
        self.devices = {(d, e): 2 * self.chips[d][e] + self.core for d in range(4) for e in range(4)}
        self.across = self.s + 1 - 2 * self.core

    def at(self, d, e):
        return {"s": self.devices[d, e]}

    def partner(self):
        return {"s": self.across}

    def along_x(self, d):
        return {"r": lax.rem(self.x + d, 4)}

    def neighbours(self, far):
        around = [self.at(*there) for there in ((NEXT, HERE), (LAST, HERE), (HERE, NEXT), (HERE, LAST), far)]
        return [self.partner()] + around


def meet(places):
    barrier = pltpu.get_barrier_semaphore()
    for place in places:
        pl.semaphore_signal(barrier, inc=1, device_id=place, device_id_type=MESH)
    pl.semaphore_wait(barrier, len(places))


def send(src, dst, send_sem, recv_sem, place):
    return pltpu.make_async_remote_copy(src_ref=src, dst_ref=dst, send_sem=send_sem, recv_sem=recv_sem, device_id=place, device_id_type=MESH)


class Gather:
    SLOTS = 10

    def __init__(self, p, n, m, here, full, sems):
        self.p, self.n, self.m, self.here, self.full = p, n, m, here, full
        self.out_sem, self.in_sem, self.here_sem, self.own_sem = sems
        self.total = 2 * (n + m)

    def hop(self, core, kind, hop, u, later):
        p, k = self.p, lax.rem(u, self.SLOTS)
        at = u - self.m * later if kind == 0 else u - self.n * (1 + later)
        here = self.here[kind].at[at]
        rows = here.shape[0]
        f = self.full[kind].at[at]
        cut = (rows // 2 + 7) // 8 * 8
        low, high = (0, cut), (cut, rows - cut)

        def piece(d, e, half=(0, rows)):
            if kind:
                return f.at[pl.ds(pl.multiple_of(rows * p.devices[d, e], 8) + half[0], half[1])]
            whole = f.at[p.a[d], p.b[e], core] if core == 0 else f.at[p.b[e], p.a[d], core]
            return whole.at[pl.ds(*half)]

        def group(e, half=(0, rows)):
            if kind:
                return [piece(d, e, half) for d in range(4)]
            whole = f.at[:, p.b[e], core] if core == 0 else f.at[p.b[e], :, core]
            return [whole.at[:, pl.ds(*half)]]

        def of_size(lines, columns, half=(0, rows)):
            if kind:
                return f.at[pl.ds(0, lines * columns * half[1])]
            return f.at[pl.ds(0, lines), pl.ds(0, columns), 0, pl.ds(*half)]

        def go(i, ref, place, left=0, src=None):
            send(ref if src is None else src, ref, self.out_sem.at[k, left], self.in_sem.at[k, i], place).start()

        def over(e):
            for one in group(e):
                go(7, one, p.partner(), FAR)

        def came(sem, ref):
            pltpu.make_async_copy(ref, ref, sem).wait()

        def all_came(i, columns, half=(0, rows)):
            came(self.in_sem.at[k, i], of_size(1, columns, half))

        sides = ((NEXT, LAST, low), (LAST, NEXT, high))
        if hop == 0:
            came(self.here_sem.at[u], here)
            own = piece(HERE, HERE)
            for i, ahead in enumerate(OTHERS):
                go(i, own, p.at(ahead, HERE), src=here)
            pltpu.make_async_copy(here, own, self.own_sem.at[k]).start()
        if hop == 1:
            came(self.own_sem.at[k], piece(HERE, HERE))
            for i, _ in enumerate(OTHERS):
                all_came(i, 1)
            for one in group(HERE):
                for side, (ahead, _, _) in enumerate(sides):
                    go(3 + side, one, p.at(HERE, ahead), 1)
            over(HERE)
        if hop == 2:
            for side, (ahead, back, half) in enumerate(sides):
                all_came(3 + side, 4)
                for one in group(back, half):
                    go(5 + side, one, p.at(HERE, ahead), 1)
                over(back)
        if hop == 3:
            for side, (_, _, half) in enumerate(sides):
                all_came(5 + side, 4, half)
            over(FAR)
        if hop == 4:
            came(self.in_sem.at[k, 7], of_size(4, 4))
            for i, (lines, columns) in enumerate(((1, 3), (3, 4), (4, 4))):
                came(self.out_sem.at[k, i], of_size(lines, columns))

    def done(self, u):
        return u + 8

    @scoped("gather")
    def step(self, t):
        def both(core, hop, u):
            later = lax.div(u, self.n + self.m)
            is_down = u - (self.n + self.m) * later >= self.n
            pl.when(~is_down)(lambda: self.hop(core, 0, hop, u, later))
            pl.when(is_down)(lambda: self.hop(core, 1, hop, u, later))

        def run(core):
            for hop in range(4, -1, -1):
                u = t - 2 * hop
                pl.when((u >= 0) & (u < self.total))(functools.partial(both, core, hop, u))

        for core in (0, 1):
            pl.when(self.p.core == core)(functools.partial(run, core))

    def steps(self, first, count):
        lax.fori_loop(0, count, lambda i, c: (self.step(first + i), c)[1], 0)


def normed(wide):
    return (wide * lax.rsqrt(jnp.mean(wide * wide, -1, keepdims=True) + 1e-6)).astype(BF16)


def forward_kernel(x, dy, w_gate, w_up, w_down, gu, d, pq, act_out, at_out, h_out, dw_out,
                   a, dyv, act, wt, wdt, pqs, h, turned, xs, dws, here_gu, here_d, out_sem, in_sem, here_sem, own_sem,
                   x_sem, dy_sem, act_sem, h_sem, at_sem, w_sem, wd_sem, pq_sem, xs_sem, dw_sem):
    tokens, width = a.shape
    n, m = act.shape[0], h.shape[0]
    p = Place()
    gather = Gather(p, n, m, (here_gu, here_d), (gu, d), (out_sem, in_sem, here_sem, own_sem))
    copy = pltpu.make_async_copy
    copy(x, a, x_sem).start()
    for layer in range(2):

        def bring(j, c, layer=layer):
            u = j + layer * (n + m)
            copy(w_gate.at[layer, :, block(j)], here_gu.at[layer * n + j, pl.ds(0, 32)], here_sem.at[u]).start()
            copy(w_up.at[layer, :, block(j)], here_gu.at[layer * n + j, pl.ds(32, 32)], here_sem.at[u]).start()
            return c

        lax.fori_loop(0, n, bring, 0)
        for i in range(m):
            u = n + i + layer * (n + m)
            copy(w_down.at[layer, :, pl.ds(i * TILE, TILE)], here_d.at[layer * m + i], here_sem.at[u]).start()
    copy(dy, dyv, dy_sem).start()
    meet(p.neighbours((FAR, HERE)))

    @scoped("norm")
    def norm(rows, wide):
        value = normed(wide)
        a[rows] = value
        turned[:, rows] = value.T

    def turned_out(layer):
        return copy(turned, at_out.at[layer], at_sem)

    def start(t, c):
        gather.step(t)
        pl.when(t == 1)(lambda: copy(x, a, x_sem).wait())

        @pl.when(t >= 1)
        def _():
            norm(block(t - 1), a[block(t - 1)].astype(F32))

        return c

    assert gather.done(0) == tokens // TILE
    lax.fori_loop(0, gather.done(1), start, 0)
    turned_out(0).start()

    def w_tile(unit, k):
        return copy(gu.at[unit], wt.at[k], w_sem.at[k])

    def wd_tile(i, k):
        return copy(d.at[i], wdt.at[k], wd_sem.at[k])

    def x_tile(i, k):
        return copy(x.at[:, block(i)], xs.at[k], xs_sem.at[k])

    def pq_tile(layer, j, k):
        return copy(pqs.at[k], pq.at[layer * n + j], pq_sem.at[k])

    def dw_tile(j, k):
        return copy(dws.at[k], dw_out.at[block(j)], dw_sem.at[k])

    def act_tile(j):
        return copy(act.at[j], act_out.at[j], act_sem)

    base = gather.done(n + m) + 1

    def hidden(layer):
        def body(j, c):
            k = lax.rem(j, 2)
            if layer:

                def more(i, c):
                    pl.when((i == 0) | (lax.rem(j, 3) == 2))(lambda: gather.step(base + j + lax.div(j, 3) + i))
                    return c

                lax.fori_loop(0, 2, more, 0)
            else:
                gather.step(gather.done(1) + j)

            @pl.when(j < n - 1)
            def _():
                w_tile(layer * n + j + 1, 1 - k).start()

            if layer == 0:

                @pl.when(j == n - 1)
                def _():
                    wd_tile(0, 0).start()
                    x_tile(0, 0).start()

            w_tile(layer * n + j, k).wait()
            pl.when(j >= 2 - 2 * layer)(lambda: pq_tile(layer, j, k).wait())
            if layer:
                pl.when(j >= 2)(lambda: dw_tile(j - 2, k).wait())
            gate_w, up_w = (wt[k, :, :, :, 32 * i : 32 * i + 32, :].reshape(width, TILE) for i in range(2))

            @scoped("hidden")
            def make(fresh):
                for i in range(tokens // 512):
                    rows = pl.ds(512 * i, 512)
                    if fresh:
                        norm(rows, jnp.concatenate([h[q, rows] for q in range(m)], -1).astype(F32))
                    gate, up = dot(a[rows], gate_w), dot(a[rows], up_w)
                    s = 0.5 * jnp.tanh(0.5 * gate) + 0.5
                    silu = gate * s
                    pqs[k, 0, rows] = silu
                    pqs[k, 1, rows] = up * (s + silu * (1 - s))
                    act[j, rows] = (silu * up).astype(BF16)

            if layer:
                pl.when(j == 0)(lambda: make(True))
                pl.when(j > 0)(lambda: make(False))
                pl.when(j == 0)(lambda: turned_out(1).start())
            else:
                make(False)
            pq_tile(layer, j, k).start()
            if layer:

                @pl.when(j < n)
                @scoped("down_terms")
                def _():
                    dws[k] = dot(act[j], dyv[...], BY_ROWS).astype(BF16)

                dw_tile(j, k).start()
            else:
                act_tile(j).start()
            return c

        lax.fori_loop(0, n, body, 0)
        if layer:
            for j in (n - 2, n - 1):
                pq_tile(layer, j, j % 2).wait()
                dw_tile(j, j % 2).wait()
            turned_out(1).wait()

    w_tile(0, 0).start()
    hidden(0)

    def h_tile(i):
        return copy(h.at[i], h_out.at[:, block(i)], h_sem)

    def down(i, c):
        k = lax.rem(i, 2)
        gather.step(gather.done(n + 1) + i)

        @pl.when(i < m - 1)
        def _():
            wd_tile(i + 1, 1 - k).start()
            x_tile(i + 1, 1 - k).start()

        @pl.when(i == m - 1)
        def _():
            w_tile(n, 0).start()

        with jax.named_scope("tiles"):
            wd_tile(i, k).wait()
            x_tile(i, k).wait()
        with jax.named_scope("down"):
            for r in range(tokens // 512):
                rows = pl.ds(512 * r, 512)
                out = added(dot(act[j, rows], wdt[k, pl.ds(TILE * j, TILE)]) for j in range(n))
                h[i, rows] = xs[k, rows] + out.astype(BF16)
        h_tile(i).start()
        return c

    lax.fori_loop(0, m, down, 0)

    turned_out(0).wait()
    with jax.named_scope("between"):
        copy(act, act_out, act_sem).wait()
        copy(dy, dyv, dy_sem).wait()
    hidden(1)
    gather.steps(base + n + n // 3, max(0, gather.done(gather.total - 1) + 1 - (base + n + n // 3)))
    copy(h, h, h_sem).wait()


def forward(x, dy, weights):
    tokens, width = x.shape
    w_gate, w_up, w_down = weights
    hidden, rows = w_gate.shape[-1], w_down.shape[1]
    n, m = hidden // TILE, width // TILE
    layers, pieces = 2, (4, 4, 2, 64, TILE)
    shapes = [
        ((layers * n, *pieces), BF16),
        ((layers * m, hidden, TILE), BF16),
        ((layers * n, 2, tokens, TILE), F32),
        ((n, tokens, TILE), BF16),
        ((layers, width, tokens), BF16),
        ((tokens, width), BF16),
        ((hidden, width), BF16),
    ]

    def twice(*shape, dtype=BF16):
        return pltpu.VMEM((2, *shape), dtype)

    def sems(*shape):
        return pltpu.SemaphoreType.DMA(shape)

    scratch = [
        pltpu.VMEM((tokens, width), BF16),
        pltpu.VMEM((tokens, width), BF16),
        pltpu.VMEM((n, tokens, TILE), BF16),
        twice(*pieces),
        twice(hidden, TILE),
        twice(2, tokens, TILE, dtype=F32),
        pltpu.VMEM((m, tokens, TILE), BF16),
        pltpu.VMEM((width, tokens), BF16),
        twice(tokens, TILE),
        twice(TILE, width),
        pltpu.VMEM((layers * n, *pieces[3:]), BF16),
        pltpu.VMEM((layers * m, rows, TILE), BF16),
        sems(Gather.SLOTS, 3),
        sems(Gather.SLOTS, 8),
        sems(layers * (n + m)),
        sems(Gather.SLOTS),
    ]
    scratch += [sems() for _ in range(5)] + [sems(2) for _ in range(5)]
    return pl.pallas_call(
        forward_kernel,
        out_shape=[jax.ShapeDtypeStruct(*shape) for shape in shapes],
        in_specs=[pl.BlockSpec(memory_space=pl.ANY)] * 5,
        out_specs=[pl.BlockSpec(memory_space=pl.ANY)] * len(shapes),
        scratch_shapes=scratch,
        compiler_params=pltpu.CompilerParams(collective_id=0, has_side_effects=True, vmem_limit_bytes=VMEM_LIMIT),
        name="forward",
    )(x, dy, w_gate, w_up, w_down)


class Sum:
    @staticmethod
    def scratch(terms, slots, rows, columns):
        def many(slots, *lead, columns=columns, dtype=BF16, count=1):
            return [pltpu.VMEM((slots, *lead, rows, columns), dtype)] * count

        half, near = columns // 2, 2
        return (
            many(terms, 16, 2)
            + many(slots, 16)
            + many(slots, 4, dtype=F32)
            + many(near, 4, dtype=F32, count=2)
            + many(near, 4, count=3)
            + many(slots, 4, columns=half, count=2)
            + many(slots, 4, count=2)
            + many(slots, dtype=F32)
            + many(near, 3)
            + many(slots, 3)
            + many(slots, 4)
            + [pltpu.SemaphoreType.DMA((slots, 11))] * 2
        )

    def __init__(self, p, refs, emit, lag, delay):
        self.p, self.emit, self.lag, self.delay = p, emit, lag, delay
        self.term, self.swapped, self.ca, self.cp, self.cm, self.x1, self.x2p, self.x2m, self.r1a, self.r1b, self.r2p, self.r2m = refs[:12]
        self.db, self.y, self.ry, self.rx, self.out_sem, self.in_sem = refs[12:]
        self.half = self.term.shape[-1] // 2

    def slot(self, ref, u):
        return ref.at[lax.rem(u, ref.shape[0])]

    def copies(self, hop, u):
        p, h = self.p, self.half
        out_sem, in_sem = self.slot(self.out_sem, u), self.slot(self.in_sem, u)

        def one(i, src, dst, place):
            return send(src, dst, out_sem.at[i], in_sem.at[i], place)

        if hop == 0:
            return [one(0, self.slot(self.term, u).at[:, 1 - p.core], self.slot(self.swapped, u), p.partner())]
        if hop == 3:
            y, ry = self.slot(self.y, u), self.slot(self.ry, u)
            return [one(5 + i, y.at[i], ry.at[i], p.at(HERE, ahead)) for i, ahead in enumerate(OTHERS)]
        if hop > 3:
            mine = self.slot(self.rx, u).at[p.x]
            return [one(8 + i, mine, mine, p.along_x(d)) for i, d in enumerate(OTHERS)]
        sources, landings = ((self.x1, self.x1), (self.r1a, self.r1b)) if hop == 1 else ((self.x2p, self.x2m), (self.r2p, self.r2m))
        made = []
        for side, (src, dst, ahead) in enumerate(zip(sources, landings, (NEXT, LAST), strict=True)):
            src = self.slot(src, u)
            if hop == 1:
                src = src.at[:, :, pl.ds(side * h, h)]
            made.append(one(2 * hop - 1 + side, src, self.slot(dst, u), p.at(ahead, HERE)))
        return made

    def add(self, hop, u):
        p, h = self.p, self.half
        low, high = slice(0, h), slice(h, None)

        def of(ref, *index):
            return ref[(lax.rem(u, ref.shape[0]), *index)].astype(F32)

        def put(ref, value, *index):
            ref[(lax.rem(u, ref.shape[0]), *index)] = value.astype(ref.dtype)

        rows = slice(None)
        if hop == 1:
            for d, ref in enumerate((self.ca, self.cp, self.x1, self.cm)):
                for e in range(4):
                    chip = p.chips[d][e]
                    put(ref, of(self.term, chip, p.core) + of(self.swapped, chip), e)
        if hop == 2:
            for e in range(4):
                put(self.x2p, of(self.cp, e, rows, low) + of(self.r1a, e), e, rows, low)
                put(self.x2p, of(self.cp, e, rows, high), e, rows, high)
                put(self.x2m, of(self.cm, e, rows, low), e, rows, low)
                put(self.x2m, of(self.cm, e, rows, high) + of(self.r1b, e), e, rows, high)
        if hop == 3:
            for e in range(4):
                value = of(self.ca, e) + of(self.r2p, e) + of(self.r2m, e)
                put(self.y, value, e - 1) if e else put(self.db, value)
        if hop == 4:
            put(self.rx, (of(self.db) + of(self.ry, 0)) + (of(self.ry, 1) + of(self.ry, 2)), p.x)
        if hop == 5:
            self.emit(u, ((of(self.rx, 0) + of(self.rx, 1)) + (of(self.rx, 2) + of(self.rx, 3))).astype(BF16))

    def hop(self, hop, u):
        with jax.named_scope(f"hop{hop}"):
            self.do(hop, u)

    def do(self, hop, u):
        if hop:
            for copy in self.copies(hop - 1, u):
                copy.wait()
        self.add(hop, u)
        if hop < HOPS:
            for copy in self.copies(hop, u):
                copy.start()

    def step(self, t, first, last):
        for hop in range(HOPS, -self.delay, -1):
            u = t - self.delay - self.lag * hop
            pl.when((u >= first) & (u < last))(functools.partial(self.hop, hop, u))


def backward_kernel(dy, gu, d, pq, act, at, h, dw1, g_gate, g_up, g_down, dgu_out, dw0, dh, av, big, load_sem, dh_sem, at_sem, big_sem, wd_sem, pq_sem, dgu_sem, dw_sem, dgc_sem, h_sem, *scratch):
    tokens, width = dh.shape
    n, m, d_rows = act.shape[0], width // TILE, g_down.shape[1]
    half = len(scratch) // 2
    copy = pltpu.make_async_copy
    p = Place()

    def emit_gu(u, value):
        later = lax.div(u, n)
        for i, out in enumerate((g_gate, g_up)):
            out[1 - later, :, block(u - n * later)] = value[32 * i : 32 * i + 32]

    def emit_d(u, value):
        later = lax.div(u, m)
        g_down[1 - later, :, block(u - m * later)] = value

    sum_gu, sum_d = Sum(p, scratch[:half], emit_gu, 2, 1), Sum(p, scratch[half:], emit_d, 1, 0)
    copy(dy, dh, dh_sem).start()
    copy(at.at[1], av, at_sem).start()

    def d_start(term, s, first):
        def one(i, c):
            rows = pl.ds(pl.multiple_of(d_rows * i, 8), d_rows)
            copy(term.at[rows, block(s)], sum_d.term.at[lax.rem(first + s, 2), lax.div(i, 2), lax.rem(i, 2)], load_sem).start()
            return c

        lax.fori_loop(0, 32, one, 0)

    def d_step(term, s, first, ready=None):
        sum_d.step(first + s, first, first + m)

        @pl.when(s < m)
        def _():
            whole = sum_d.term.at[lax.rem(first + s, 2)]
            copy(whole, whole, load_sem).wait()
            sum_d.hop(0, first + s)

        @pl.when(s + 1 < m)
        def _():
            if ready is not None:
                ready(s + 1)
            d_start(term, s + 1, first)

    def gradients(layer, first, begin, d_turn):
        def phase(wdt, pqt, dgu):
            def tiles(j, k):
                return [
                    copy(d.at[pl.ds(layer * m, m), block(j)], wdt.at[k], wd_sem.at[k]),
                    copy(pq.at[layer * n + j], pqt.at[k], pq_sem.at[k]),
                ]

            def dgu_tile(j, k):
                return copy(dgu.at[k], dgu_out.at[j], dgu_sem.at[k])

            def body(j, c):
                k = lax.rem(j, 2)
                sum_gu.step(first + j, first, first + n)
                d_turn(j)
                if layer:
                    copy(gu.at[n + j], big.at[j], big_sem.at[0]).start()

                @pl.when(j < n - 1)
                def _():
                    for one in tiles(j + 1, 1 - k):
                        one.start()

                with jax.named_scope("tiles"):
                    for one in tiles(j, k):
                        one.wait()
                    if layer:
                        pl.when(j >= 2)(lambda: dgu_tile(j - 2, k).wait())
                with jax.named_scope("terms"):
                    for i in range(tokens // 512):
                        rows = pl.ds(512 * i, 512)
                        by_act = added(dot(dh[rows, TILE * e : TILE * e + TILE], wdt[k, e], BY_COLUMNS) for e in range(m))
                        by_act = by_act.astype(BF16).astype(F32)
                        dgu[k, 0, rows] = (by_act * pqt[k, 1, rows]).astype(BF16)
                        dgu[k, 1, rows] = (by_act * pqt[k, 0, rows]).astype(BF16)
                    slot = lax.rem(first + j, sum_gu.term.shape[0])
                    for i in range(m):
                        for e in (0, 1):
                            value = dot(av[TILE * i : TILE * i + TILE], dgu[k, e]).astype(BF16)
                            sum_gu.term[slot, 4 * i : 4 * i + 4, :, 32 * e : 32 * e + 32, :] = value.reshape(4, 2, 32, TILE)
                if layer:
                    dgu_tile(j, k).start()
                return c

            for one in tiles(0, 0):
                one.start()
            begin()
            lax.fori_loop(0, n, body, 0)
            if layer:
                for j in (n - 2, n - 1):
                    dgu_tile(j, j % 2).wait()

        pl.run_scoped(
            phase,
            pltpu.VMEM((2, m, TILE, TILE), BF16),
            pltpu.VMEM((2, 2, tokens, TILE), F32),
            pltpu.VMEM((2, 2, tokens, TILE), BF16),
        )

    def to_states(dgc, hv):
        def rows_in(i, k):
            return [
                copy(dgu_out.at[:, :, block(i)], dgc.at[k], dgc_sem.at[k]),
                copy(h.at[block(i)], hv.at[k], h_sem.at[k]),
            ]

        def body(i, c):
            k = lax.rem(i, 2)
            sum_gu.step(n + i, 0, n)
            pl.when(k == 0)(lambda: d_step(dw1, (n + 1) // 2 + lax.div(i, 2), 0))

            @pl.when(i < tokens // TILE - 1)
            def _():
                for one in rows_in(i + 1, 1 - k):
                    one.start()

            with jax.named_scope("tiles"):
                for one in rows_in(i, k):
                    one.wait()
            with jax.named_scope("states"):
                parts = []
                for e in range(m):
                    weights = [big[j, 2 * TILE * e : 2 * TILE * (e + 1)].reshape(8, 64, TILE) for j in range(n)]
                    two = [
                        added(dot(dgc[k, j, o], weights[j][:, 32 * o : 32 * o + 32].reshape(TILE, TILE), BY_COLUMNS) for j in range(n))
                        for o in (0, 1)
                    ]
                    parts.append((two[0].astype(BF16) + two[1].astype(BF16)).astype(F32))
                by_a = jnp.concatenate(parts, -1)
                wide = hv[k].astype(F32)
                scale = lax.rsqrt(jnp.mean(wide * wide, -1, keepdims=True) + 1e-6)
                along = jnp.mean(by_a * wide, -1, keepdims=True)
                by_h = by_a * scale - wide * (scale * scale * scale * along)
                dh[block(i)] = dh[block(i)] + by_h.astype(BF16)
            return c

        for one in rows_in(0, 0):
            one.start()
        with jax.named_scope("weights"):
            copy(gu.at[pl.ds(n, n)], big, big_sem.at[0]).wait()
        lax.fori_loop(0, tokens // TILE, body, 0)

    def down(turned, made):
        def out(e):
            return copy(made.at[lax.rem(e, 2)], dw0.at[:, block(e)], dw_sem.at[lax.rem(e, 2)])

        def body(e, c):
            k = lax.rem(e, 2)
            for i in (0, 1):
                sum_gu.step(n + tokens // TILE + 2 * e + i, 0, n)

            @pl.when(e == 1)
            def _():
                out(0).wait()
                d_start(dw0, 0, m)

            pl.when(e >= 2)(lambda: d_step(dw0, e - 2, m, lambda s: out(s).wait()))
            with jax.named_scope("turn"):
                turned[...] = dh[:, block(e)].T

            pl.when(e == 0)(lambda: copy(act, big, big_sem.at[0]).wait())
            with jax.named_scope("down_terms"):
                for j in range(n):
                    made[k, TILE * j : TILE * (j + 1)] = dot(turned[...], big[j]).astype(BF16).T
            out(e).start()
            return c

        copy(act, big, big_sem.at[0]).start()
        lax.fori_loop(0, m, body, 0)

        def last_turn(j):
            pl.when(lax.rem(j, 2) == 0)(lambda: d_step(dw0, 2 + lax.div(j, 2), m, lambda s: out(s).wait()))

        copy(at.at[0], av, at_sem).wait()
        gradients(0, n, lambda: None, last_turn)

    @scoped("meet")
    def begin():
        meet(p.neighbours((HERE, FAR)) + [p.along_x(d) for d in OTHERS])
        copy(dy, dh, dh_sem).wait()
        copy(at.at[1], av, at_sem).wait()

    def turn(j):
        pl.when(lax.rem(j, 2) == 0)(lambda: d_step(dw1, lax.div(j, 2), 0))

    d_start(dw1, 0, 0)
    gradients(1, 0, begin, turn)
    copy(at.at[0], av, at_sem).start()
    pl.run_scoped(
        to_states,
        pltpu.VMEM((2, n, 2, TILE, TILE), BF16),
        pltpu.VMEM((2, TILE, width), BF16),
    )
    pl.run_scoped(down, pltpu.VMEM((TILE, tokens), BF16), pltpu.VMEM((2, 32 * d_rows, TILE), BF16))

    def rest(i, c):
        sum_gu.step(2 * n + i, n, 2 * n)
        return c

    lax.fori_loop(0, 2 * HOPS + 1, rest, 0)


def backward(dy, gu, d, pq, act, at, h, dw1):
    tokens, width = dy.shape
    n, hidden = gu.shape[0] // 2, dw1.shape[0]
    rows, m = hidden // 32, width // TILE
    gu = gu.reshape(2 * n, tokens, TILE)
    assert 32 * 64 == tokens and n == 3 * m + 1 and HOPS + m == (n + 5) // 2 and 2 * HOPS + 1 <= tokens // TILE + 2 * m
    any_space, vmem = pl.BlockSpec(memory_space=pl.ANY), pl.BlockSpec(memory_space=pltpu.VMEM)
    shapes = [((2, 32, hidden), BF16)] * 2 + [((2, rows, width), BF16), ((n, 2, tokens, TILE), BF16), ((hidden, width), BF16)]
    out = pl.pallas_call(
        backward_kernel,
        out_shape=[jax.ShapeDtypeStruct(*shape) for shape in shapes],
        in_specs=[any_space] * 8,
        out_specs=[vmem] * 3 + [any_space] * 2,
        scratch_shapes=[pltpu.VMEM(shape, BF16) for shape in ((tokens, width), (width, tokens), (n, tokens, TILE))]
        + [pltpu.SemaphoreType.DMA(())] * 3
        + [pltpu.SemaphoreType.DMA((2,))] * 7
        + Sum.scratch(3, 4, 64, TILE)
        + Sum.scratch(2, 2, rows, TILE),
        compiler_params=pltpu.CompilerParams(collective_id=1, has_side_effects=True, vmem_limit_bytes=VMEM_LIMIT),
        name="backward",
    )(dy, gu, d, pq, act, at, h, dw1)
    return out[:3]


def solution(mesh):
    def step(x, dy, *arrays):
        weights, m, v = (arrays[i : i + 3] for i in (0, 3, 6))
        gradients = backward(dy[0], *forward(x[0], dy[0], weights))
        new = [adamw(w.astype(F32), m, v, g.astype(F32)) for w, m, v, g in zip(weights, m, v, gradients, strict=True)]
        return tuple(one[which] for which in range(3) for one in new)

    states, cut = P(("rep", "r", "s"), None, None), P(None, "s", None)
    return jax.shard_map(
        step,
        mesh=mesh,
        in_specs=(states, states) + (cut,) * 9,
        out_specs=(P("rep", "s", None),) * 9,
        check_vma=False,
    )
```

```python
import functools

import jax
import jax.numpy as jnp
from jax import lax
from jax.experimental import pallas as pl
from jax.experimental.pallas import tpu as pltpu
from jax.sharding import PartitionSpec as P

NAMES = ("w_gate", "w_up", "w_down")
MESH = pl.DeviceIdType.MESH
F32, BF16 = jnp.float32, jnp.bfloat16
HOPS = 5
VMEM_LIMIT = 67043328
PLAIN, BY_COLUMNS, BY_ROWS = (((1,), (0,)), ((), ())), (((1,), (1,)), ((), ())), (((0,), (0,)), ((), ()))
HERE, NEXT, FAR, LAST = range(4)
TILE = 256


def adamw(w, m, v, g):
    m = 0.9 * m + 0.1 * g
    v = 0.95 * v + 0.05 * g * g
    step = m * lax.rsqrt(v + 1e-8) + 0.1 * w
    return (w - 0.02 * step).astype(jnp.bfloat16), m, v


def update_kernel(*refs):
    given, out = refs[:12], refs[12:]
    for i in range(3):
        new = adamw(*(ref[...].astype(F32) for ref in given[i::3]))
        for ref, value in zip(out[i::3], new, strict=True):
            ref[...] = value


def update(weights, m, v, gradients):
    def spec(w):
        return pl.BlockSpec((1, w.shape[1], w.shape[2] // 2), lambda layer, half: (layer, 0, half))

    return pl.pallas_call(
        update_kernel,
        grid=(2, 2),
        out_shape=[jax.ShapeDtypeStruct(w.shape, w.dtype) for w in (*weights, *m, *v)],
        in_specs=[spec(w) for w in weights] * 4,
        out_specs=[spec(w) for w in weights] * 3,
        name="update",
    )(*weights, *m, *v, *gradients)


def dot(a, b, dims=PLAIN):
    return lax.dot_general(a, b, dims, preferred_element_type=F32)


def scoped(name):
    def wrap(f):
        @functools.wraps(f)
        def inner(*args, **kwargs):
            with jax.named_scope(name):
                return f(*args, **kwargs)

        return inner

    return wrap


def block(n, size=TILE):
    return pl.ds(pl.multiple_of(n * size, size), size)


def added(values):
    total = None
    for value in values:
        total = value if total is None else total + value
    return total


OTHERS = (NEXT, FAR, LAST)


class Place:
    def __init__(self):
        self.s, self.x = lax.axis_index("s"), lax.axis_index("r")
        self.core = lax.rem(self.s, 2)
        y, z = lax.div(self.s, 8), lax.rem(lax.div(self.s, 2), 4)
        a = y * (1 - self.core) + z * self.core
        b = z * (1 - self.core) + y * self.core
        step_a, step_b = 4 - 3 * self.core, 1 + 3 * self.core
        self.a, self.b = [[lax.rem(at + d, 4) for d in range(4)] for at in (a, b)]
        self.chips = [[self.a[d] * step_a + self.b[e] * step_b for e in range(4)] for d in range(4)]
        self.devices = {(d, e): 2 * self.chips[d][e] + self.core for d in range(4) for e in range(4)}
        self.across = self.s + 1 - 2 * self.core

    def at(self, d, e):
        return {"s": self.devices[d, e]}

    def partner(self):
        return {"s": self.across}

    def along_x(self, d):
        return {"r": lax.rem(self.x + d, 4)}

    def neighbours(self, far):
        around = [self.at(*there) for there in ((NEXT, HERE), (LAST, HERE), (HERE, NEXT), (HERE, LAST), far)]
        return [self.partner()] + around


def meet(places):
    barrier = pltpu.get_barrier_semaphore()
    for place in places:
        pl.semaphore_signal(barrier, inc=1, device_id=place, device_id_type=MESH)
    pl.semaphore_wait(barrier, len(places))


def send(src, dst, send_sem, recv_sem, place):
    return pltpu.make_async_remote_copy(src_ref=src, dst_ref=dst, send_sem=send_sem, recv_sem=recv_sem, device_id=place, device_id_type=MESH)


class Gather:
    SLOTS = 10

    def __init__(self, p, n, m, here, full, sems):
        self.p, self.n, self.m, self.here, self.full = p, n, m, here, full
        self.out_sem, self.in_sem, self.here_sem, self.own_sem = sems
        self.total = 2 * (n + m)

    def hop(self, core, kind, hop, u, later):
        p, k = self.p, lax.rem(u, self.SLOTS)
        at = u - self.m * later if kind == 0 else u - self.n * (1 + later)
        here = self.here[kind].at[at]
        rows = here.shape[0]
        f = self.full[kind].at[at]
        cut = (rows // 2 + 7) // 8 * 8
        low, high = (0, cut), (cut, rows - cut)

        def piece(d, e, half=(0, rows)):
            if kind:
                return f.at[pl.ds(pl.multiple_of(rows * p.devices[d, e], 8) + half[0], half[1])]
            whole = f.at[p.a[d], p.b[e], core] if core == 0 else f.at[p.b[e], p.a[d], core]
            return whole.at[pl.ds(*half)]

        def group(e, half=(0, rows)):
            if kind:
                return [piece(d, e, half) for d in range(4)]
            whole = f.at[:, p.b[e], core] if core == 0 else f.at[p.b[e], :, core]
            return [whole.at[:, pl.ds(*half)]]

        def of_size(lines, columns, half=(0, rows)):
            if kind:
                return f.at[pl.ds(0, lines * columns * half[1])]
            return f.at[pl.ds(0, lines), pl.ds(0, columns), 0, pl.ds(*half)]

        def go(i, ref, place, left=0, src=None):
            send(ref if src is None else src, ref, self.out_sem.at[k, left], self.in_sem.at[k, i], place).start()

        def over(e):
            for one in group(e):
                go(7, one, p.partner(), FAR)

        def came(sem, ref):
            pltpu.make_async_copy(ref, ref, sem).wait()

        def all_came(i, columns, half=(0, rows)):
            came(self.in_sem.at[k, i], of_size(1, columns, half))

        sides = ((NEXT, LAST, low), (LAST, NEXT, high))
        if hop == 0:
            came(self.here_sem.at[u], here)
            own = piece(HERE, HERE)
            for i, ahead in enumerate(OTHERS):
                go(i, own, p.at(ahead, HERE), src=here)
            pltpu.make_async_copy(here, own, self.own_sem.at[k]).start()
        if hop == 1:
            came(self.own_sem.at[k], piece(HERE, HERE))
            for i, _ in enumerate(OTHERS):
                all_came(i, 1)
            for one in group(HERE):
                for side, (ahead, _, _) in enumerate(sides):
                    go(3 + side, one, p.at(HERE, ahead), 1)
            over(HERE)
        if hop == 2:
            for side, (ahead, back, half) in enumerate(sides):
                all_came(3 + side, 4)
                for one in group(back, half):
                    go(5 + side, one, p.at(HERE, ahead), 1)
                over(back)
        if hop == 3:
            for side, (_, _, half) in enumerate(sides):
                all_came(5 + side, 4, half)
            over(FAR)
        if hop == 4:
            came(self.in_sem.at[k, 7], of_size(4, 4))
            for i, (lines, columns) in enumerate(((1, 3), (3, 4), (4, 4))):
                came(self.out_sem.at[k, i], of_size(lines, columns))

    def done(self, u):
        return u + 8

    @scoped("gather")
    def step(self, t):
        def both(core, hop, u):
            later = lax.div(u, self.n + self.m)
            is_down = u - (self.n + self.m) * later >= self.n
            pl.when(~is_down)(lambda: self.hop(core, 0, hop, u, later))
            pl.when(is_down)(lambda: self.hop(core, 1, hop, u, later))

        def run(core):
            for hop in range(4, -1, -1):
                u = t - 2 * hop
                pl.when((u >= 0) & (u < self.total))(functools.partial(both, core, hop, u))

        for core in (0, 1):
            pl.when(self.p.core == core)(functools.partial(run, core))

    def steps(self, first, count):
        lax.fori_loop(0, count, lambda i, c: (self.step(first + i), c)[1], 0)


def normed(wide):
    return (wide * lax.rsqrt(jnp.mean(wide * wide, -1, keepdims=True) + 1e-6)).astype(BF16)


def forward_kernel(x, dy, w_gate, w_up, w_down, gu, d, pq, act_out, at_out, h_out, dw_out,
                   a, dyv, act, wt, wdt, pqs, h, turned, xs, dws, here_gu, here_d, out_sem, in_sem, here_sem, own_sem,
                   x_sem, dy_sem, act_sem, h_sem, at_sem, w_sem, wd_sem, pq_sem, xs_sem, dw_sem):
    tokens, width = a.shape
    n, m = act.shape[0], h.shape[0]
    p = Place()
    gather = Gather(p, n, m, (here_gu, here_d), (gu, d), (out_sem, in_sem, here_sem, own_sem))
    copy = pltpu.make_async_copy
    copy(x, a, x_sem).start()
    for layer in range(2):

        def bring(j, c, layer=layer):
            u = j + layer * (n + m)
            copy(w_gate.at[layer, :, block(j)], here_gu.at[layer * n + j, pl.ds(0, 32)], here_sem.at[u]).start()
            copy(w_up.at[layer, :, block(j)], here_gu.at[layer * n + j, pl.ds(32, 32)], here_sem.at[u]).start()
            return c

        lax.fori_loop(0, n, bring, 0)
        for i in range(m):
            u = n + i + layer * (n + m)
            copy(w_down.at[layer, :, pl.ds(i * TILE, TILE)], here_d.at[layer * m + i], here_sem.at[u]).start()
    copy(dy, dyv, dy_sem).start()
    meet(p.neighbours((FAR, HERE)))

    @scoped("norm")
    def norm(rows, wide):
        value = normed(wide)
        a[rows] = value
        turned[:, rows] = value.T

    def turned_out(layer):
        return copy(turned, at_out.at[layer], at_sem)

    def start(t, c):
        gather.step(t)
        pl.when(t == 1)(lambda: copy(x, a, x_sem).wait())

        @pl.when(t >= 1)
        def _():
            norm(block(t - 1), a[block(t - 1)].astype(F32))

        return c

    assert gather.done(0) == tokens // TILE
    lax.fori_loop(0, gather.done(1), start, 0)
    turned_out(0).start()

    def w_tile(unit, k):
        return copy(gu.at[unit], wt.at[k], w_sem.at[k])

    def wd_tile(i, k):
        return copy(d.at[i], wdt.at[k], wd_sem.at[k])

    def x_tile(i, k):
        return copy(x.at[:, block(i)], xs.at[k], xs_sem.at[k])

    def pq_tile(layer, j, k):
        return copy(pqs.at[k], pq.at[layer * n + j], pq_sem.at[k])

    def dw_tile(j, k):
        return copy(dws.at[k], dw_out.at[block(j)], dw_sem.at[k])

    def act_tile(j):
        return copy(act.at[j], act_out.at[j], act_sem)

    base = gather.done(n + m) + 1

    def hidden(layer):
        def body(j, c):
            k = lax.rem(j, 2)
            if layer:

                extra = jnp.maximum(lax.div(j - 7, 2), 0)

                def more(i, c):
                    pl.when((i == 0) | ((j > 7) & (lax.rem(j, 2) == 0)))(lambda: gather.step(base + j + extra + i))
                    return c

                lax.fori_loop(0, 2, more, 0)
            else:
                gather.step(gather.done(1) + j)

            @pl.when(j < n - 1)
            def _():
                w_tile(layer * n + j + 1, 1 - k).start()

            if layer == 0:

                @pl.when(j == n - 1)
                def _():
                    wd_tile(0, 0).start()
                    x_tile(0, 0).start()

            w_tile(layer * n + j, k).wait()
            pl.when(j >= 2 - 2 * layer)(lambda: pq_tile(layer, j, k).wait())
            if layer:
                pl.when(j >= 2)(lambda: dw_tile(j - 2, k).wait())
            gate_w, up_w = (wt[k, :, :, :, 32 * i : 32 * i + 32, :].reshape(width, TILE) for i in range(2))

            @scoped("hidden")
            def make(fresh):
                for i in range(tokens // 512):
                    rows = pl.ds(512 * i, 512)
                    if fresh:
                        norm(rows, jnp.concatenate([h[q, rows] for q in range(m)], -1).astype(F32))
                    gate, up = dot(a[rows], gate_w), dot(a[rows], up_w)
                    s = 0.5 * jnp.tanh(0.5 * gate) + 0.5
                    silu = gate * s
                    pqs[k, 0, rows] = silu
                    pqs[k, 1, rows] = up * (s + silu * (1 - s))
                    act[j, rows] = (silu * up).astype(BF16)

            if layer:
                pl.when(j == 0)(lambda: make(True))
                pl.when(j > 0)(lambda: make(False))
                pl.when(j == 0)(lambda: turned_out(1).start())
            else:
                make(False)
            pq_tile(layer, j, k).start()
            if layer:

                @pl.when(j < n)
                @scoped("down_terms")
                def _():
                    dws[k] = dot(act[j], dyv[...], BY_ROWS).astype(BF16)

                dw_tile(j, k).start()
            else:
                act_tile(j).start()
            return c

        lax.fori_loop(0, n, body, 0)
        if layer:
            for j in (n - 2, n - 1):
                pq_tile(layer, j, j % 2).wait()
                dw_tile(j, j % 2).wait()
            turned_out(1).wait()

    w_tile(0, 0).start()
    hidden(0)

    def h_tile(i):
        return copy(h.at[i], h_out.at[:, block(i)], h_sem)

    def down(i, c):
        k = lax.rem(i, 2)
        gather.step(gather.done(n + 1) + i)

        @pl.when(i < m - 1)
        def _():
            wd_tile(i + 1, 1 - k).start()
            x_tile(i + 1, 1 - k).start()

        @pl.when(i == m - 1)
        def _():
            w_tile(n, 0).start()

        with jax.named_scope("tiles"):
            wd_tile(i, k).wait()
            x_tile(i, k).wait()
        with jax.named_scope("down"):
            for r in range(tokens // 512):
                rows = pl.ds(512 * r, 512)
                out = added(dot(act[j, rows], wdt[k, pl.ds(TILE * j, TILE)]) for j in range(n))
                h[i, rows] = xs[k, rows] + out.astype(BF16)
        h_tile(i).start()
        return c

    lax.fori_loop(0, m, down, 0)

    turned_out(0).wait()
    with jax.named_scope("between"):
        copy(act, act_out, act_sem).wait()
        copy(dy, dyv, dy_sem).wait()
    hidden(1)
    gather.steps(base + n + 3, max(0, gather.done(gather.total - 1) + 1 - (base + n + 3)))
    copy(h, h, h_sem).wait()


def forward(x, dy, weights):
    tokens, width = x.shape
    w_gate, w_up, w_down = weights
    hidden, rows = w_gate.shape[-1], w_down.shape[1]
    n, m = hidden // TILE, width // TILE
    layers, pieces = 2, (4, 4, 2, 64, TILE)
    shapes = [
        ((layers * n, *pieces), BF16),
        ((layers * m, hidden, TILE), BF16),
        ((layers * n, 2, tokens, TILE), F32),
        ((n, tokens, TILE), BF16),
        ((layers, width, tokens), BF16),
        ((tokens, width), BF16),
        ((hidden, width), BF16),
    ]

    def twice(*shape, dtype=BF16):
        return pltpu.VMEM((2, *shape), dtype)

    def sems(*shape):
        return pltpu.SemaphoreType.DMA(shape)

    scratch = [
        pltpu.VMEM((tokens, width), BF16),
        pltpu.VMEM((tokens, width), BF16),
        pltpu.VMEM((n, tokens, TILE), BF16),
        twice(*pieces),
        twice(hidden, TILE),
        twice(2, tokens, TILE, dtype=F32),
        pltpu.VMEM((m, tokens, TILE), BF16),
        pltpu.VMEM((width, tokens), BF16),
        twice(tokens, TILE),
        twice(TILE, width),
        pltpu.VMEM((layers * n, *pieces[3:]), BF16),
        pltpu.VMEM((layers * m, rows, TILE), BF16),
        sems(Gather.SLOTS, 3),
        sems(Gather.SLOTS, 8),
        sems(layers * (n + m)),
        sems(Gather.SLOTS),
    ]
    scratch += [sems() for _ in range(5)] + [sems(2) for _ in range(5)]
    return pl.pallas_call(
        forward_kernel,
        out_shape=[jax.ShapeDtypeStruct(*shape) for shape in shapes],
        in_specs=[pl.BlockSpec(memory_space=pl.ANY)] * 5,
        out_specs=[pl.BlockSpec(memory_space=pl.ANY)] * len(shapes),
        scratch_shapes=scratch,
        compiler_params=pltpu.CompilerParams(collective_id=0, has_side_effects=True, vmem_limit_bytes=VMEM_LIMIT),
        name="forward",
    )(x, dy, w_gate, w_up, w_down)


class Sum:
    @staticmethod
    def scratch(terms, slots, rows, columns):
        def many(slots, *lead, columns=columns, dtype=BF16, count=1):
            return [pltpu.VMEM((slots, *lead, rows, columns), dtype)] * count

        half, near = columns // 2, 2
        return (
            many(terms, 16, 2)
            + many(slots, 16)
            + many(slots, 4, dtype=F32)
            + many(near, 4, dtype=F32, count=2)
            + many(near, 4, count=3)
            + many(slots, 4, columns=half, count=2)
            + many(slots, 4, count=2)
            + many(slots, dtype=F32)
            + many(near, 3)
            + many(slots, 3)
            + many(slots, 4)
            + [pltpu.SemaphoreType.DMA((slots, 11))] * 2
        )

    def __init__(self, p, refs, emit, lag, delay):
        self.p, self.emit, self.lag, self.delay = p, emit, lag, delay
        self.term, self.swapped, self.ca, self.cp, self.cm, self.x1, self.x2p, self.x2m, self.r1a, self.r1b, self.r2p, self.r2m = refs[:12]
        self.db, self.y, self.ry, self.rx, self.out_sem, self.in_sem = refs[12:]
        self.half = self.term.shape[-1] // 2

    def slot(self, ref, u):
        return ref.at[lax.rem(u, ref.shape[0])]

    def copies(self, hop, u):
        p, h = self.p, self.half
        out_sem, in_sem = self.slot(self.out_sem, u), self.slot(self.in_sem, u)

        def one(i, src, dst, place):
            return send(src, dst, out_sem.at[i], in_sem.at[i], place)

        if hop == 0:
            return [one(0, self.slot(self.term, u).at[:, 1 - p.core], self.slot(self.swapped, u), p.partner())]
        if hop == 3:
            y, ry = self.slot(self.y, u), self.slot(self.ry, u)
            return [one(5 + i, y.at[i], ry.at[i], p.at(HERE, ahead)) for i, ahead in enumerate(OTHERS)]
        if hop > 3:
            mine = self.slot(self.rx, u).at[p.x]
            return [one(8 + i, mine, mine, p.along_x(d)) for i, d in enumerate(OTHERS)]
        sources, landings = ((self.x1, self.x1), (self.r1a, self.r1b)) if hop == 1 else ((self.x2p, self.x2m), (self.r2p, self.r2m))
        made = []
        for side, (src, dst, ahead) in enumerate(zip(sources, landings, (NEXT, LAST), strict=True)):
            src = self.slot(src, u)
            if hop == 1:
                src = src.at[:, :, pl.ds(side * h, h)]
            made.append(one(2 * hop - 1 + side, src, self.slot(dst, u), p.at(ahead, HERE)))
        return made

    def add(self, hop, u):
        p, h = self.p, self.half
        low, high = slice(0, h), slice(h, None)

        def of(ref, *index):
            return ref[(lax.rem(u, ref.shape[0]), *index)].astype(F32)

        def put(ref, value, *index):
            ref[(lax.rem(u, ref.shape[0]), *index)] = value.astype(ref.dtype)

        rows = slice(None)
        if hop == 1:
            for d, ref in enumerate((self.ca, self.cp, self.x1, self.cm)):
                for e in range(4):
                    chip = p.chips[d][e]
                    put(ref, of(self.term, chip, p.core) + of(self.swapped, chip), e)
        if hop == 2:
            for e in range(4):
                put(self.x2p, of(self.cp, e, rows, low) + of(self.r1a, e), e, rows, low)
                put(self.x2p, of(self.cp, e, rows, high), e, rows, high)
                put(self.x2m, of(self.cm, e, rows, low), e, rows, low)
                put(self.x2m, of(self.cm, e, rows, high) + of(self.r1b, e), e, rows, high)
        if hop == 3:
            for e in range(4):
                value = of(self.ca, e) + of(self.r2p, e) + of(self.r2m, e)
                put(self.y, value, e - 1) if e else put(self.db, value)
        if hop == 4:
            put(self.rx, (of(self.db) + of(self.ry, 0)) + (of(self.ry, 1) + of(self.ry, 2)), p.x)
        if hop == 5:
            self.emit(u, ((of(self.rx, 0) + of(self.rx, 1)) + (of(self.rx, 2) + of(self.rx, 3))).astype(BF16))

    def hop(self, hop, u):
        with jax.named_scope(f"hop{hop}"):
            self.do(hop, u)

    def do(self, hop, u):
        if hop:
            for copy in self.copies(hop - 1, u):
                copy.wait()
        self.add(hop, u)
        if hop < HOPS:
            for copy in self.copies(hop, u):
                copy.start()

    def step(self, t, first, last):
        for hop in range(HOPS, -self.delay, -1):
            u = t - self.delay - self.lag * hop
            pl.when((u >= first) & (u < last))(functools.partial(self.hop, hop, u))


def backward_kernel(dy, gu, d, pq, act, at, h, dw1, g_gate, g_up, g_down, dgu_out, dw0, dh, av, big, load_sem, dh_sem, at_sem, big_sem, wd_sem, pq_sem, dgu_sem, dw_sem, dgc_sem, h_sem, *scratch):
    tokens, width = dh.shape
    n, m, d_rows = act.shape[0], width // TILE, g_down.shape[1]
    half = len(scratch) // 2
    copy = pltpu.make_async_copy
    p = Place()

    def emit_gu(u, value):
        later = lax.div(u, n)
        for i, out in enumerate((g_gate, g_up)):
            out[1 - later, :, block(u - n * later)] = value[32 * i : 32 * i + 32]

    def emit_d(u, value):
        later = lax.div(u, m)
        g_down[1 - later, :, block(u - m * later)] = value

    sum_gu, sum_d = Sum(p, scratch[:half], emit_gu, 2, 1), Sum(p, scratch[half:], emit_d, 1, 0)
    copy(dy, dh, dh_sem).start()
    copy(at.at[1], av, at_sem).start()

    def d_start(term, s, first):
        if len(term.shape) > 2:
            copy(term.at[:, :, :, block(s)], sum_d.term.at[lax.rem(first + s, 2)], load_sem).start()
            return

        def one(i, c):
            rows = pl.ds(pl.multiple_of(d_rows * i, 8), d_rows)
            copy(term.at[rows, block(s)], sum_d.term.at[lax.rem(first + s, 2), lax.div(i, 2), lax.rem(i, 2)], load_sem).start()
            return c

        lax.fori_loop(0, 32, one, 0)

    def d_step(term, s, first, ready=None):
        sum_d.step(first + s, first, first + m)

        @pl.when(s < m)
        def _():
            whole = sum_d.term.at[lax.rem(first + s, 2)]
            copy(whole, whole, load_sem).wait()
            sum_d.hop(0, first + s)

        @pl.when(s + 1 < m)
        def _():
            if ready is not None:
                ready(s + 1)
            d_start(term, s + 1, first)

    def gradients(layer, first, begin, d_turn):
        def phase(wdt, pqt, dgu):
            def tiles(j, k):
                return [
                    copy(d.at[pl.ds(layer * m, m), block(j)], wdt.at[k], wd_sem.at[k]),
                    copy(pq.at[layer * n + j], pqt.at[k], pq_sem.at[k]),
                ]

            def dgu_tile(j, k):
                return copy(dgu.at[k], dgu_out.at[j], dgu_sem.at[k])

            def body(j, c):
                k = lax.rem(j, 2)
                sum_gu.step(first + j, first, first + n)
                d_turn(j)
                if layer:
                    copy(gu.at[n + j], big.at[j], big_sem.at[0]).start()

                @pl.when(j < n - 1)
                def _():
                    for one in tiles(j + 1, 1 - k):
                        one.start()

                with jax.named_scope("tiles"):
                    for one in tiles(j, k):
                        one.wait()
                    if layer:
                        pl.when(j >= 2)(lambda: dgu_tile(j - 2, k).wait())
                with jax.named_scope("terms"):
                    for i in range(tokens // 512):
                        rows = pl.ds(512 * i, 512)
                        by_act = added(dot(dh[rows, TILE * e : TILE * e + TILE], wdt[k, e], BY_COLUMNS) for e in range(m))
                        by_act = by_act.astype(BF16).astype(F32)
                        dgu[k, 0, rows] = (by_act * pqt[k, 1, rows]).astype(BF16)
                        dgu[k, 1, rows] = (by_act * pqt[k, 0, rows]).astype(BF16)
                    slot = lax.rem(first + j, sum_gu.term.shape[0])
                    for i in range(m):
                        for e in (0, 1):
                            value = dot(av[TILE * i : TILE * i + TILE], dgu[k, e]).astype(BF16)
                            sum_gu.term[slot, 4 * i : 4 * i + 4, :, 32 * e : 32 * e + 32, :] = value.reshape(4, 2, 32, TILE)
                if layer:
                    dgu_tile(j, k).start()
                return c

            for one in tiles(0, 0):
                one.start()
            begin()
            lax.fori_loop(0, n, body, 0)
            if layer:
                for j in (n - 2, n - 1):
                    dgu_tile(j, j % 2).wait()

        pl.run_scoped(
            phase,
            pltpu.VMEM((2, m, TILE, TILE), BF16),
            pltpu.VMEM((2, 2, tokens, TILE), F32),
            pltpu.VMEM((2, 2, tokens, TILE), BF16),
        )

    def to_states(dgc, hv):
        def rows_in(i, k):
            return [
                copy(dgu_out.at[:, :, block(i)], dgc.at[k], dgc_sem.at[k]),
                copy(h.at[block(i)], hv.at[k], h_sem.at[k]),
            ]

        def body(i, c):
            k = lax.rem(i, 2)
            sum_gu.step(n + i, 0, n)
            pl.when(k == 0)(lambda: d_step(dw1, (n + 1) // 2 + lax.div(i, 2), 0))

            @pl.when(i < tokens // TILE - 1)
            def _():
                for one in rows_in(i + 1, 1 - k):
                    one.start()

            with jax.named_scope("tiles"):
                for one in rows_in(i, k):
                    one.wait()
            with jax.named_scope("states"):
                parts = []
                for e in range(m):
                    weights = [big[j, 2 * TILE * e : 2 * TILE * (e + 1)].reshape(8, 64, TILE) for j in range(n)]
                    two = [
                        added(dot(dgc[k, j, o], weights[j][:, 32 * o : 32 * o + 32].reshape(TILE, TILE), BY_COLUMNS) for j in range(n))
                        for o in (0, 1)
                    ]
                    parts.append((two[0].astype(BF16) + two[1].astype(BF16)).astype(F32))
                by_a = jnp.concatenate(parts, -1)
                wide = hv[k].astype(F32)
                scale = lax.rsqrt(jnp.mean(wide * wide, -1, keepdims=True) + 1e-6)
                along = jnp.mean(by_a * wide, -1, keepdims=True)
                by_h = by_a * scale - wide * (scale * scale * scale * along)
                dh[block(i)] = dh[block(i)] + by_h.astype(BF16)
            return c

        for one in rows_in(0, 0):
            one.start()
        with jax.named_scope("weights"):
            copy(gu.at[pl.ds(n, n)], big, big_sem.at[0]).wait()
        lax.fori_loop(0, tokens // TILE, body, 0)

    def down(turned, made):
        def out(e):
            return copy(made.at[lax.rem(e, 2)], dw0.at[:, block(e)], dw_sem.at[lax.rem(e, 2)])

        def body(e, c):
            k = lax.rem(e, 2)
            for i in (0, 1):
                sum_gu.step(n + tokens // TILE + 2 * e + i, 0, n)

            @pl.when(e == 1)
            def _():
                out(0).wait()
                d_start(dw0, 0, m)

            pl.when(e >= 2)(lambda: d_step(dw0, e - 2, m, lambda s: out(s).wait()))
            with jax.named_scope("turn"):
                turned[...] = dh[:, block(e)].T

            pl.when(e == 0)(lambda: copy(act, big, big_sem.at[0]).wait())
            with jax.named_scope("down_terms"):
                for j in range(n):
                    made[k, TILE * j : TILE * (j + 1)] = dot(turned[...], big[j]).astype(BF16).T
            out(e).start()
            return c

        def columns():
            lax.fori_loop(0, m, body, 0)
            copy(at.at[0], av, at_sem).wait()

        copy(act, big, big_sem.at[0]).start()

        def last_turn(j):
            pl.when(lax.rem(j, 2) == 0)(lambda: d_step(dw0, 2 + lax.div(j, 2), m, lambda s: out(s).wait()))

        gradients(0, n, columns, last_turn)

    @scoped("meet")
    def begin():
        meet(p.neighbours((HERE, FAR)) + [p.along_x(d) for d in OTHERS])
        copy(dy, dh, dh_sem).wait()
        copy(at.at[1], av, at_sem).wait()

    def turn(j):
        pl.when(lax.rem(j, 2) == 0)(lambda: d_step(dw1, lax.div(j, 2), 0))

    d_start(dw1, 0, 0)
    gradients(1, 0, begin, turn)
    copy(at.at[0], av, at_sem).start()
    pl.run_scoped(
        to_states,
        pltpu.VMEM((2, n, 2, TILE, TILE), BF16),
        pltpu.VMEM((2, TILE, width), BF16),
    )
    pl.run_scoped(down, pltpu.VMEM((TILE, tokens), BF16), pltpu.VMEM((2, 32 * d_rows, TILE), BF16))

    def rest(i, c):
        sum_gu.step(2 * n + i, n, 2 * n)
        return c

    lax.fori_loop(0, 2 * HOPS + 1, rest, 0)


def backward(dy, gu, d, pq, act, at, h, dw1):
    tokens, width = dy.shape
    n, hidden = gu.shape[0] // 2, dw1.shape[0]
    rows, m = hidden // 32, width // TILE
    gu = gu.reshape(2 * n, tokens, TILE)
    assert 32 * 64 == tokens and n == 3 * m + 1 and HOPS + m == (n + 5) // 2 and 2 * HOPS + 1 <= tokens // TILE + 2 * m
    any_space, vmem = pl.BlockSpec(memory_space=pl.ANY), pl.BlockSpec(memory_space=pltpu.VMEM)
    shapes = [((2, 32, hidden), BF16)] * 2 + [((2, rows, width), BF16), ((n, 2, tokens, TILE), BF16), ((hidden, width), BF16)]
    out = pl.pallas_call(
        backward_kernel,
        out_shape=[jax.ShapeDtypeStruct(*shape) for shape in shapes],
        in_specs=[any_space] * 8,
        out_specs=[vmem] * 3 + [any_space] * 2,
        scratch_shapes=[pltpu.VMEM(shape, BF16) for shape in ((tokens, width), (width, tokens), (n, tokens, TILE))]
        + [pltpu.SemaphoreType.DMA(())] * 3
        + [pltpu.SemaphoreType.DMA((2,))] * 7
        + Sum.scratch(3, 4, 64, TILE)
        + Sum.scratch(2, 2, rows, TILE),
        compiler_params=pltpu.CompilerParams(collective_id=1, has_side_effects=True, vmem_limit_bytes=VMEM_LIMIT),
        name="backward",
    )(dy, gu, d, pq, act, at, h, dw1.reshape(16, 2, rows, width))
    return out[:3]


def solution(mesh):
    def step(x, dy, *arrays):
        weights, m, v = (arrays[i : i + 3] for i in (0, 3, 6))
        return tuple(update(weights, m, v, backward(dy[0], *forward(x[0], dy[0], weights))))

    states, cut = P(("rep", "r", "s"), None, None), P(None, "s", None)
    return jax.shard_map(
        step,
        mesh=mesh,
        in_specs=(states, states) + (cut,) * 9,
        out_specs=(P("rep", "s", None),) * 9,
        check_vma=False,
    )
```

```python
import functools

import jax
import jax.numpy as jnp
from jax import lax
from jax.experimental import pallas as pl
from jax.experimental.pallas import tpu as pltpu
from jax.sharding import PartitionSpec as P

NAMES = ("w_gate", "w_up", "w_down")
MESH = pl.DeviceIdType.MESH
F32, BF16 = jnp.float32, jnp.bfloat16
HOPS = 5
VMEM_LIMIT = 67043328
PLAIN, BY_COLUMNS, BY_ROWS = (((1,), (0,)), ((), ())), (((1,), (1,)), ((), ())), (((0,), (0,)), ((), ()))
HERE, NEXT, FAR, LAST = range(4)
TILE = 256


def adamw(w, m, v, g):
    m = 0.9 * m + 0.1 * g
    v = 0.95 * v + 0.05 * g * g
    step = m * lax.rsqrt(v + 1e-8) + 0.1 * w
    return (w - 0.02 * step).astype(jnp.bfloat16), m, v


def update_kernel(*refs):
    given, out = refs[:12], refs[12:]
    for i in range(3):
        new = adamw(*(ref[...].astype(F32) for ref in given[i::3]))
        for ref, value in zip(out[i::3], new, strict=True):
            ref[...] = value


def update(weights, m, v, gradients):
    def spec(w):
        return pl.BlockSpec((1, w.shape[1], w.shape[2] // 2), lambda layer, half: (layer, 0, half))

    return pl.pallas_call(
        update_kernel,
        grid=(2, 2),
        out_shape=[jax.ShapeDtypeStruct(w.shape, w.dtype) for w in (*weights, *m, *v)],
        in_specs=[spec(w) for w in weights] * 4,
        out_specs=[spec(w) for w in weights] * 3,
        name="update",
    )(*weights, *m, *v, *gradients)


def dot(a, b, dims=PLAIN):
    return lax.dot_general(a, b, dims, preferred_element_type=F32)


def scoped(name):
    def wrap(f):
        @functools.wraps(f)
        def inner(*args, **kwargs):
            with jax.named_scope(name):
                return f(*args, **kwargs)

        return inner

    return wrap


def block(n, size=TILE):
    return pl.ds(pl.multiple_of(n * size, size), size)


def added(values):
    total = None
    for value in values:
        total = value if total is None else total + value
    return total


OTHERS = (NEXT, FAR, LAST)


class Place:
    def __init__(self):
        self.s, self.x = lax.axis_index("s"), lax.axis_index("r")
        self.core = lax.rem(self.s, 2)
        y, z = lax.div(self.s, 8), lax.rem(lax.div(self.s, 2), 4)
        a = y * (1 - self.core) + z * self.core
        b = z * (1 - self.core) + y * self.core
        step_a, step_b = 4 - 3 * self.core, 1 + 3 * self.core
        self.a, self.b = [[lax.rem(at + d, 4) for d in range(4)] for at in (a, b)]
        self.chips = [[self.a[d] * step_a + self.b[e] * step_b for e in range(4)] for d in range(4)]
        self.devices = {(d, e): 2 * self.chips[d][e] + self.core for d in range(4) for e in range(4)}
        self.across = self.s + 1 - 2 * self.core

    def at(self, d, e):
        return {"s": self.devices[d, e]}

    def partner(self):
        return {"s": self.across}

    def along_x(self, d):
        return {"r": lax.rem(self.x + d, 4)}

    def neighbours(self, far):
        around = [self.at(*there) for there in ((NEXT, HERE), (LAST, HERE), (HERE, NEXT), (HERE, LAST), far)]
        return [self.partner()] + around


def greet(places):
    barrier = pltpu.get_barrier_semaphore()
    for place in places:
        pl.semaphore_signal(barrier, inc=1, device_id=place, device_id_type=MESH)
    return lambda: pl.semaphore_wait(barrier, len(places))


def send(src, dst, send_sem, recv_sem, place):
    return pltpu.make_async_remote_copy(src_ref=src, dst_ref=dst, send_sem=send_sem, recv_sem=recv_sem, device_id=place, device_id_type=MESH)


class Gather:
    SLOTS = 10

    def __init__(self, p, n, m, here, full, sems):
        self.p, self.n, self.m, self.here, self.full = p, n, m, here, full
        self.out_sem, self.in_sem, self.here_sem, self.own_sem = sems
        self.total = 2 * (n + m)

    def hop(self, core, kind, hop, u, later):
        p, k = self.p, lax.rem(u, self.SLOTS)
        at = u - self.m * later if kind == 0 else u - self.n * (1 + later)
        here = self.here[kind].at[at]
        rows = here.shape[0]
        f = self.full[kind].at[at]
        cut = (rows // 2 + 7) // 8 * 8
        low, high = (0, cut), (cut, rows - cut)

        def piece(d, e, half=(0, rows)):
            if kind:
                return f.at[pl.ds(pl.multiple_of(rows * p.devices[d, e], 8) + half[0], half[1])]
            whole = f.at[p.a[d], p.b[e], core] if core == 0 else f.at[p.b[e], p.a[d], core]
            return whole.at[pl.ds(*half)]

        def group(e, half=(0, rows)):
            if kind:
                return [piece(d, e, half) for d in range(4)]
            whole = f.at[:, p.b[e], core] if core == 0 else f.at[p.b[e], :, core]
            return [whole.at[:, pl.ds(*half)]]

        def of_size(lines, columns, half=(0, rows)):
            if kind:
                return f.at[pl.ds(0, lines * columns * half[1])]
            return f.at[pl.ds(0, lines), pl.ds(0, columns), 0, pl.ds(*half)]

        def go(i, ref, place, left=0, src=None):
            send(ref if src is None else src, ref, self.out_sem.at[k, left], self.in_sem.at[k, i], place).start()

        def over(e):
            for one in group(e):
                go(7, one, p.partner(), FAR)

        def came(sem, ref):
            pltpu.make_async_copy(ref, ref, sem).wait()

        def all_came(i, columns, half=(0, rows)):
            came(self.in_sem.at[k, i], of_size(1, columns, half))

        sides = ((NEXT, LAST, low), (LAST, NEXT, high))
        if hop == 0:
            came(self.here_sem.at[u], here)
            own = piece(HERE, HERE)
            for i, ahead in enumerate(OTHERS):
                go(i, own, p.at(ahead, HERE), src=here)
            pltpu.make_async_copy(here, own, self.own_sem.at[k]).start()
        if hop == 1:
            came(self.own_sem.at[k], piece(HERE, HERE))
            for i, _ in enumerate(OTHERS):
                all_came(i, 1)
            for one in group(HERE):
                for side, (ahead, _, _) in enumerate(sides):
                    go(3 + side, one, p.at(HERE, ahead), 1)
            over(HERE)
        if hop == 2:
            for side, (ahead, back, half) in enumerate(sides):
                all_came(3 + side, 4)
                for one in group(back, half):
                    go(5 + side, one, p.at(HERE, ahead), 1)
                over(back)
        if hop == 3:
            for side, (_, _, half) in enumerate(sides):
                all_came(5 + side, 4, half)
            over(FAR)
        if hop == 4:
            came(self.in_sem.at[k, 7], of_size(4, 4))
            for i, (lines, columns) in enumerate(((1, 3), (3, 4), (4, 4))):
                came(self.out_sem.at[k, i], of_size(lines, columns))

    def done(self, u):
        return u + 8

    @scoped("gather")
    def step(self, t):
        def both(core, hop, u):
            later = lax.div(u, self.n + self.m)
            is_down = u - (self.n + self.m) * later >= self.n
            pl.when(~is_down)(lambda: self.hop(core, 0, hop, u, later))
            pl.when(is_down)(lambda: self.hop(core, 1, hop, u, later))

        def run(core):
            for hop in range(4, -1, -1):
                u = t - 2 * hop
                pl.when((u >= 0) & (u < self.total))(functools.partial(both, core, hop, u))

        for core in (0, 1):
            pl.when(self.p.core == core)(functools.partial(run, core))

    def steps(self, first, count):
        lax.fori_loop(0, count, lambda i, c: (self.step(first + i), c)[1], 0)


def normed(wide):
    return (wide * lax.rsqrt(jnp.mean(wide * wide, -1, keepdims=True) + 1e-6)).astype(BF16)


def forward_kernel(x, dy, w_gate, w_up, w_down, gu, d, pq, act_out, at_out, h_out, dw_out,
                   a, dyv, act, wt, wdt, pqs, h, turned, xs, dws, here_gu, here_d, out_sem, in_sem, here_sem, own_sem,
                   x_sem, dy_sem, act_sem, h_sem, at_sem, w_sem, wd_sem, pq_sem, xs_sem, dw_sem):
    tokens, width = a.shape
    n, m = act.shape[0], h.shape[0]
    p = Place()
    gather = Gather(p, n, m, (here_gu, here_d), (gu, d), (out_sem, in_sem, here_sem, own_sem))
    met = greet(p.neighbours((FAR, HERE)))
    copy = pltpu.make_async_copy
    copy(x, a, x_sem).start()
    for layer in range(2):

        def bring(j, c, layer=layer):
            u = j + layer * (n + m)
            copy(w_gate.at[layer, :, block(j)], here_gu.at[layer * n + j, pl.ds(0, 32)], here_sem.at[u]).start()
            copy(w_up.at[layer, :, block(j)], here_gu.at[layer * n + j, pl.ds(32, 32)], here_sem.at[u]).start()
            return c

        lax.fori_loop(0, n, bring, 0)
        for i in range(m):
            u = n + i + layer * (n + m)
            copy(w_down.at[layer, :, pl.ds(i * TILE, TILE)], here_d.at[layer * m + i], here_sem.at[u]).start()
    copy(dy, dyv, dy_sem).start()
    met()

    @scoped("norm")
    def norm(rows, wide):
        value = normed(wide)
        a[rows] = value
        turned[:, rows] = value.T

    def turned_out(layer):
        return copy(turned, at_out.at[layer], at_sem)

    def start(t, c):
        gather.step(t)
        pl.when(t == 1)(lambda: copy(x, a, x_sem).wait())

        @pl.when(t >= 1)
        def _():
            norm(block(t - 1), a[block(t - 1)].astype(F32))

        return c

    assert gather.done(0) == tokens // TILE
    lax.fori_loop(0, gather.done(1), start, 0)
    turned_out(0).start()

    def w_tile(unit, k):
        return copy(gu.at[unit], wt.at[k], w_sem.at[k])

    def wd_tile(i, k):
        return copy(d.at[i], wdt.at[k], wd_sem.at[k])

    def x_tile(i, k):
        return copy(x.at[:, block(i)], xs.at[k], xs_sem.at[k])

    def pq_tile(layer, j, k):
        return copy(pqs.at[k], pq.at[layer * n + j], pq_sem.at[k])

    def dw_tile(j, k):
        return copy(dws.at[k], dw_out.at[block(j)], dw_sem.at[k])

    def act_tile(j):
        return copy(act.at[j], act_out.at[j], act_sem)

    base = gather.done(n + m) + 1

    def hidden(layer):
        def body(j, c):
            k = lax.rem(j, 2)
            if layer:

                extra = jnp.maximum(lax.div(j - 7, 2), 0)

                def more(i, c):
                    pl.when((i == 0) | ((j > 7) & (lax.rem(j, 2) == 0)))(lambda: gather.step(base + j + extra + i))
                    return c

                lax.fori_loop(0, 2, more, 0)
            else:
                gather.step(gather.done(1) + j)

            @pl.when(j < n - 1)
            def _():
                w_tile(layer * n + j + 1, 1 - k).start()

            if layer == 0:

                @pl.when(j == n - 1)
                def _():
                    wd_tile(0, 0).start()
                    x_tile(0, 0).start()

            w_tile(layer * n + j, k).wait()
            pl.when(j >= 2 - 2 * layer)(lambda: pq_tile(layer, j, k).wait())
            if layer:
                pl.when(j >= 2)(lambda: dw_tile(j - 2, k).wait())
            gate_w, up_w = (wt[k, :, :, :, 32 * i : 32 * i + 32, :].reshape(width, TILE) for i in range(2))

            @scoped("hidden")
            def make(fresh):
                for i in range(tokens // 512):
                    rows = pl.ds(512 * i, 512)
                    if fresh:
                        norm(rows, jnp.concatenate([h[q, rows] for q in range(m)], -1).astype(F32))
                    gate, up = dot(a[rows], gate_w), dot(a[rows], up_w)
                    s = 0.5 * jnp.tanh(0.5 * gate) + 0.5
                    silu = gate * s
                    pqs[k, 0, rows] = silu
                    pqs[k, 1, rows] = up * (s + silu * (1 - s))
                    act[j, rows] = (silu * up).astype(BF16)

            if layer:
                pl.when(j == 0)(lambda: make(True))
                pl.when(j > 0)(lambda: make(False))
                pl.when(j == 0)(lambda: turned_out(1).start())
            else:
                make(False)
            pq_tile(layer, j, k).start()
            if layer:

                @pl.when(j < n)
                @scoped("down_terms")
                def _():
                    dws[k] = dot(act[j], dyv[...], BY_ROWS).astype(BF16)

                dw_tile(j, k).start()
            else:
                act_tile(j).start()
            return c

        lax.fori_loop(0, n, body, 0)
        if layer:
            for j in (n - 2, n - 1):
                pq_tile(layer, j, j % 2).wait()
                dw_tile(j, j % 2).wait()
            turned_out(1).wait()

    w_tile(0, 0).start()
    hidden(0)

    def h_tile(i):
        return copy(h.at[i], h_out.at[:, block(i)], h_sem)

    def down(i, c):
        k = lax.rem(i, 2)
        gather.step(gather.done(n + 1) + i)

        @pl.when(i < m - 1)
        def _():
            wd_tile(i + 1, 1 - k).start()
            x_tile(i + 1, 1 - k).start()

        @pl.when(i == m - 1)
        def _():
            w_tile(n, 0).start()

        with jax.named_scope("tiles"):
            wd_tile(i, k).wait()
            x_tile(i, k).wait()
        with jax.named_scope("down"):
            for r in range(tokens // 512):
                rows = pl.ds(512 * r, 512)
                out = added(dot(act[j, rows], wdt[k, pl.ds(TILE * j, TILE)]) for j in range(n))
                h[i, rows] = xs[k, rows] + out.astype(BF16)
        h_tile(i).start()
        return c

    lax.fori_loop(0, m, down, 0)

    turned_out(0).wait()
    with jax.named_scope("between"):
        copy(act, act_out, act_sem).wait()
        copy(dy, dyv, dy_sem).wait()
    hidden(1)
    gather.steps(base + n + 3, max(0, gather.done(gather.total - 1) + 1 - (base + n + 3)))
    copy(h, h, h_sem).wait()


def forward(x, dy, weights):
    tokens, width = x.shape
    w_gate, w_up, w_down = weights
    hidden, rows = w_gate.shape[-1], w_down.shape[1]
    n, m = hidden // TILE, width // TILE
    layers, pieces = 2, (4, 4, 2, 64, TILE)
    shapes = [
        ((layers * n, *pieces), BF16),
        ((layers * m, hidden, TILE), BF16),
        ((layers * n, 2, tokens, TILE), F32),
        ((n, tokens, TILE), BF16),
        ((layers, width, tokens), BF16),
        ((tokens, width), BF16),
        ((hidden, width), BF16),
    ]

    def twice(*shape, dtype=BF16):
        return pltpu.VMEM((2, *shape), dtype)

    def sems(*shape):
        return pltpu.SemaphoreType.DMA(shape)

    scratch = [
        pltpu.VMEM((tokens, width), BF16),
        pltpu.VMEM((tokens, width), BF16),
        pltpu.VMEM((n, tokens, TILE), BF16),
        twice(*pieces),
        twice(hidden, TILE),
        twice(2, tokens, TILE, dtype=F32),
        pltpu.VMEM((m, tokens, TILE), BF16),
        pltpu.VMEM((width, tokens), BF16),
        twice(tokens, TILE),
        twice(TILE, width),
        pltpu.VMEM((layers * n, *pieces[3:]), BF16),
        pltpu.VMEM((layers * m, rows, TILE), BF16),
        sems(Gather.SLOTS, 3),
        sems(Gather.SLOTS, 8),
        sems(layers * (n + m)),
        sems(Gather.SLOTS),
    ]
    scratch += [sems() for _ in range(5)] + [sems(2) for _ in range(5)]
    return pl.pallas_call(
        forward_kernel,
        out_shape=[jax.ShapeDtypeStruct(*shape) for shape in shapes],
        in_specs=[pl.BlockSpec(memory_space=pl.ANY)] * 5,
        out_specs=[pl.BlockSpec(memory_space=pl.ANY)] * len(shapes),
        scratch_shapes=scratch,
        compiler_params=pltpu.CompilerParams(collective_id=0, has_side_effects=True, vmem_limit_bytes=VMEM_LIMIT),
        name="forward",
    )(x, dy, w_gate, w_up, w_down)


class Sum:
    @staticmethod
    def scratch(terms, slots, rows, columns):
        def many(slots, *lead, columns=columns, dtype=BF16, count=1):
            return [pltpu.VMEM((slots, *lead, rows, columns), dtype)] * count

        half, near = columns // 2, 2
        return (
            many(terms, 16, 2)
            + many(slots, 16)
            + many(slots, 4, dtype=F32)
            + many(near, 4, dtype=F32, count=2)
            + many(near, 4, count=3)
            + many(slots, 4, columns=half, count=2)
            + many(slots, 4, count=2)
            + many(slots, dtype=F32)
            + many(near, 3)
            + many(slots, 3)
            + many(slots, 4)
            + [pltpu.SemaphoreType.DMA((slots, 11))] * 2
        )

    def __init__(self, p, refs, emit, lag, delay):
        self.p, self.emit, self.lag, self.delay = p, emit, lag, delay
        self.term, self.swapped, self.ca, self.cp, self.cm, self.x1, self.x2p, self.x2m, self.r1a, self.r1b, self.r2p, self.r2m = refs[:12]
        self.db, self.y, self.ry, self.rx, self.out_sem, self.in_sem = refs[12:]
        self.half = self.term.shape[-1] // 2

    def slot(self, ref, u):
        return ref.at[lax.rem(u, ref.shape[0])]

    def copies(self, hop, u):
        p, h = self.p, self.half
        out_sem, in_sem = self.slot(self.out_sem, u), self.slot(self.in_sem, u)

        def one(i, src, dst, place):
            return send(src, dst, out_sem.at[i], in_sem.at[i], place)

        if hop == 0:
            return [one(0, self.slot(self.term, u).at[:, 1 - p.core], self.slot(self.swapped, u), p.partner())]
        if hop == 3:
            y, ry = self.slot(self.y, u), self.slot(self.ry, u)
            return [one(5 + i, y.at[i], ry.at[i], p.at(HERE, ahead)) for i, ahead in enumerate(OTHERS)]
        if hop > 3:
            mine = self.slot(self.rx, u).at[p.x]
            return [one(8 + i, mine, mine, p.along_x(d)) for i, d in enumerate(OTHERS)]
        sources, landings = ((self.x1, self.x1), (self.r1a, self.r1b)) if hop == 1 else ((self.x2p, self.x2m), (self.r2p, self.r2m))
        made = []
        for side, (src, dst, ahead) in enumerate(zip(sources, landings, (NEXT, LAST), strict=True)):
            src = self.slot(src, u)
            if hop == 1:
                src = src.at[:, :, pl.ds(side * h, h)]
            made.append(one(2 * hop - 1 + side, src, self.slot(dst, u), p.at(ahead, HERE)))
        return made

    def add(self, hop, u):
        p, h = self.p, self.half
        low, high = slice(0, h), slice(h, None)

        def of(ref, *index):
            return ref[(lax.rem(u, ref.shape[0]), *index)].astype(F32)

        def put(ref, value, *index):
            ref[(lax.rem(u, ref.shape[0]), *index)] = value.astype(ref.dtype)

        rows = slice(None)
        if hop == 1:
            for d, ref in enumerate((self.ca, self.cp, self.x1, self.cm)):
                for e in range(4):
                    chip = p.chips[d][e]
                    put(ref, of(self.term, chip, p.core) + of(self.swapped, chip), e)
        if hop == 2:
            for e in range(4):
                put(self.x2p, of(self.cp, e, rows, low) + of(self.r1a, e), e, rows, low)
                put(self.x2p, of(self.cp, e, rows, high), e, rows, high)
                put(self.x2m, of(self.cm, e, rows, low), e, rows, low)
                put(self.x2m, of(self.cm, e, rows, high) + of(self.r1b, e), e, rows, high)
        if hop == 3:
            for e in range(4):
                value = of(self.ca, e) + of(self.r2p, e) + of(self.r2m, e)
                put(self.y, value, e - 1) if e else put(self.db, value)
        if hop == 4:
            put(self.rx, (of(self.db) + of(self.ry, 0)) + (of(self.ry, 1) + of(self.ry, 2)), p.x)
        if hop == 5:
            self.emit(u, ((of(self.rx, 0) + of(self.rx, 1)) + (of(self.rx, 2) + of(self.rx, 3))).astype(BF16))

    def hop(self, hop, u):
        with jax.named_scope(f"hop{hop}"):
            self.do(hop, u)

    def do(self, hop, u):
        if hop:
            for copy in self.copies(hop - 1, u):
                copy.wait()
        self.add(hop, u)
        if hop < HOPS:
            for copy in self.copies(hop, u):
                copy.start()

    def step(self, t, first, last):
        for hop in range(HOPS, -self.delay, -1):
            u = t - self.delay - self.lag * hop
            pl.when((u >= first) & (u < last))(functools.partial(self.hop, hop, u))


def backward_kernel(dy, gu, d, pq, act, at, h, dw1, g_gate, g_up, g_down, dgu_out, dw0, dh, av, big, load_sem, dh_sem, at_sem, big_sem, wd_sem, pq_sem, dgu_sem, dw_sem, dgc_sem, h_sem, *scratch):
    tokens, width = dh.shape
    n, m, d_rows = act.shape[0], width // TILE, g_down.shape[1]
    half = len(scratch) // 2
    copy = pltpu.make_async_copy
    p = Place()
    met = greet(p.neighbours((HERE, FAR)) + [p.along_x(d) for d in OTHERS])

    def emit_gu(u, value):
        later = lax.div(u, n)
        for i, out in enumerate((g_gate, g_up)):
            out[1 - later, :, block(u - n * later)] = value[32 * i : 32 * i + 32]

    def emit_d(u, value):
        later = lax.div(u, m)
        g_down[1 - later, :, block(u - m * later)] = value

    sum_gu, sum_d = Sum(p, scratch[:half], emit_gu, 2, 1), Sum(p, scratch[half:], emit_d, 1, 0)
    copy(dy, dh, dh_sem).start()
    copy(at.at[1], av, at_sem).start()

    def d_start(term, s, first):
        if len(term.shape) > 2:
            copy(term.at[:, :, :, block(s)], sum_d.term.at[lax.rem(first + s, 2)], load_sem).start()
            return

        def one(i, c):
            rows = pl.ds(pl.multiple_of(d_rows * i, 8), d_rows)
            copy(term.at[rows, block(s)], sum_d.term.at[lax.rem(first + s, 2), lax.div(i, 2), lax.rem(i, 2)], load_sem).start()
            return c

        lax.fori_loop(0, 32, one, 0)

    def d_step(term, s, first, ready=None):
        sum_d.step(first + s, first, first + m)

        @pl.when(s < m)
        def _():
            whole = sum_d.term.at[lax.rem(first + s, 2)]
            copy(whole, whole, load_sem).wait()
            sum_d.hop(0, first + s)

        @pl.when(s + 1 < m)
        def _():
            if ready is not None:
                ready(s + 1)
            d_start(term, s + 1, first)

    def gradients(layer, first, begin, d_turn):
        def phase(wdt, pqt, dgu):
            def tiles(j, k):
                return [
                    copy(d.at[pl.ds(layer * m, m), block(j)], wdt.at[k], wd_sem.at[k]),
                    copy(pq.at[layer * n + j], pqt.at[k], pq_sem.at[k]),
                ]

            def dgu_tile(j, k):
                return copy(dgu.at[k], dgu_out.at[j], dgu_sem.at[k])

            def body(j, c):
                k = lax.rem(j, 2)
                if layer:
                    pl.when(j == 1)(met)
                sum_gu.step(first + j, first, first + n)
                d_turn(j)
                if layer:
                    copy(gu.at[n + j], big.at[j], big_sem.at[0]).start()

                @pl.when(j < n - 1)
                def _():
                    for one in tiles(j + 1, 1 - k):
                        one.start()

                with jax.named_scope("tiles"):
                    for one in tiles(j, k):
                        one.wait()
                    if layer:
                        pl.when(j >= 2)(lambda: dgu_tile(j - 2, k).wait())
                with jax.named_scope("terms"):
                    for i in range(tokens // 512):
                        rows = pl.ds(512 * i, 512)
                        by_act = added(dot(dh[rows, TILE * e : TILE * e + TILE], wdt[k, e], BY_COLUMNS) for e in range(m))
                        by_act = by_act.astype(BF16).astype(F32)
                        dgu[k, 0, rows] = (by_act * pqt[k, 1, rows]).astype(BF16)
                        dgu[k, 1, rows] = (by_act * pqt[k, 0, rows]).astype(BF16)
                    slot = lax.rem(first + j, sum_gu.term.shape[0])
                    for i in range(m):
                        for e in (0, 1):
                            value = dot(av[TILE * i : TILE * i + TILE], dgu[k, e]).astype(BF16)
                            sum_gu.term[slot, 4 * i : 4 * i + 4, :, 32 * e : 32 * e + 32, :] = value.reshape(4, 2, 32, TILE)
                if layer:
                    dgu_tile(j, k).start()
                return c

            for one in tiles(0, 0):
                one.start()
            begin()
            lax.fori_loop(0, n, body, 0)
            if layer:
                for j in (n - 2, n - 1):
                    dgu_tile(j, j % 2).wait()

        pl.run_scoped(
            phase,
            pltpu.VMEM((2, m, TILE, TILE), BF16),
            pltpu.VMEM((2, 2, tokens, TILE), F32),
            pltpu.VMEM((2, 2, tokens, TILE), BF16),
        )

    def to_states(dgc, hv):
        def rows_in(i, k):
            return [
                copy(dgu_out.at[:, :, block(i)], dgc.at[k], dgc_sem.at[k]),
                copy(h.at[block(i)], hv.at[k], h_sem.at[k]),
            ]

        def body(i, c):
            k = lax.rem(i, 2)
            sum_gu.step(n + i, 0, n)
            pl.when(k == 0)(lambda: d_step(dw1, n // 2 + lax.div(i, 2), 0))

            @pl.when(i < tokens // TILE - 1)
            def _():
                for one in rows_in(i + 1, 1 - k):
                    one.start()

            with jax.named_scope("tiles"):
                for one in rows_in(i, k):
                    one.wait()
            with jax.named_scope("states"):
                parts = []
                for e in range(m):
                    weights = [big[j, 2 * TILE * e : 2 * TILE * (e + 1)].reshape(8, 64, TILE) for j in range(n)]
                    two = [
                        added(dot(dgc[k, j, o], weights[j][:, 32 * o : 32 * o + 32].reshape(TILE, TILE), BY_COLUMNS) for j in range(n))
                        for o in (0, 1)
                    ]
                    parts.append((two[0].astype(BF16) + two[1].astype(BF16)).astype(F32))
                by_a = jnp.concatenate(parts, -1)
                wide = hv[k].astype(F32)
                scale = lax.rsqrt(jnp.mean(wide * wide, -1, keepdims=True) + 1e-6)
                along = jnp.mean(by_a * wide, -1, keepdims=True)
                by_h = by_a * scale - wide * (scale * scale * scale * along)
                dh[block(i)] = dh[block(i)] + by_h.astype(BF16)
            return c

        for one in rows_in(0, 0):
            one.start()
        with jax.named_scope("weights"):
            copy(gu.at[pl.ds(n, n)], big, big_sem.at[0]).wait()
        lax.fori_loop(0, tokens // TILE, body, 0)

    def down(turned, made):
        def out(e):
            return copy(made.at[lax.rem(e, 2)], dw0.at[:, block(e)], dw_sem.at[lax.rem(e, 2)])

        def body(e, c):
            k = lax.rem(e, 2)
            for i in (0, 1):
                sum_gu.step(n + tokens // TILE + 2 * e + i, 0, n)

            @pl.when(e == 1)
            def _():
                out(0).wait()
                d_start(dw0, 0, m)

            pl.when(e >= 2)(lambda: d_step(dw0, e - 2, m, lambda s: out(s).wait()))
            with jax.named_scope("turn"):
                turned[...] = dh[:, block(e)].T

            pl.when(e == 0)(lambda: copy(act, big, big_sem.at[0]).wait())
            with jax.named_scope("down_terms"):
                for j in range(n):
                    made[k, TILE * j : TILE * (j + 1)] = dot(turned[...], big[j]).astype(BF16).T
            out(e).start()
            return c

        def columns():
            lax.fori_loop(0, m, body, 0)
            copy(at.at[0], av, at_sem).wait()

        copy(act, big, big_sem.at[0]).start()

        def last_turn(j):
            pl.when(lax.rem(j, 2) == 0)(lambda: d_step(dw0, 2 + lax.div(j, 2), m, lambda s: out(s).wait()))

        gradients(0, n, columns, last_turn)

    @scoped("meet")
    def begin():
        d_start(dw1, 0, 0)
        copy(dy, dh, dh_sem).wait()
        copy(at.at[1], av, at_sem).wait()

    def turn(j):
        pl.when((lax.rem(j, 2) == 0) & (j > 0))(lambda: d_step(dw1, lax.div(j, 2) - 1, 0))

    gradients(1, 0, begin, turn)
    copy(at.at[0], av, at_sem).start()
    pl.run_scoped(
        to_states,
        pltpu.VMEM((2, n, 2, TILE, TILE), BF16),
        pltpu.VMEM((2, TILE, width), BF16),
    )
    pl.run_scoped(down, pltpu.VMEM((TILE, tokens), BF16), pltpu.VMEM((2, 32 * d_rows, TILE), BF16))

    def rest(i, c):
        sum_gu.step(2 * n + i, n, 2 * n)
        return c

    lax.fori_loop(0, 2 * HOPS + 1, rest, 0)


def backward(dy, gu, d, pq, act, at, h, dw1):
    tokens, width = dy.shape
    n, hidden = gu.shape[0] // 2, dw1.shape[0]
    rows, m = hidden // 32, width // TILE
    gu = gu.reshape(2 * n, tokens, TILE)
    assert 32 * 64 == tokens and n == 3 * m + 1 and HOPS + m == (n + 5) // 2 and 2 * HOPS + 1 <= tokens // TILE + 2 * m
    any_space, vmem = pl.BlockSpec(memory_space=pl.ANY), pl.BlockSpec(memory_space=pltpu.VMEM)
    shapes = [((2, 32, hidden), BF16)] * 2 + [((2, rows, width), BF16), ((n, 2, tokens, TILE), BF16), ((hidden, width), BF16)]
    out = pl.pallas_call(
        backward_kernel,
        out_shape=[jax.ShapeDtypeStruct(*shape) for shape in shapes],
        in_specs=[any_space] * 8,
        out_specs=[vmem] * 3 + [any_space] * 2,
        scratch_shapes=[pltpu.VMEM(shape, BF16) for shape in ((tokens, width), (width, tokens), (n, tokens, TILE))]
        + [pltpu.SemaphoreType.DMA(())] * 3
        + [pltpu.SemaphoreType.DMA((2,))] * 7
        + Sum.scratch(3, 4, 64, TILE)
        + Sum.scratch(2, 2, rows, TILE),
        compiler_params=pltpu.CompilerParams(collective_id=1, has_side_effects=True, vmem_limit_bytes=VMEM_LIMIT),
        name="backward",
    )(dy, gu, d, pq, act, at, h, dw1.reshape(16, 2, rows, width))
    return out[:3]


def solution(mesh):
    def step(x, dy, *arrays):
        weights, m, v = (arrays[i : i + 3] for i in (0, 3, 6))
        return tuple(update(weights, m, v, backward(dy[0], *forward(x[0], dy[0], weights))))

    states, cut = P(("rep", "r", "s"), None, None), P(None, "s", None)
    return jax.shard_map(
        step,
        mesh=mesh,
        in_specs=(states, states) + (cut,) * 9,
        out_specs=(P("rep", "s", None),) * 9,
        check_vma=False,
    )
```

```python
import functools

import jax
import jax.numpy as jnp
from jax import lax
from jax.experimental import pallas as pl
from jax.experimental.pallas import tpu as pltpu
from jax.sharding import PartitionSpec as P

NAMES = ("w_gate", "w_up", "w_down")
MESH = pl.DeviceIdType.MESH
F32, BF16 = jnp.float32, jnp.bfloat16
HOPS = 5
VMEM_LIMIT = 67043328
PLAIN, BY_COLUMNS, BY_ROWS = (((1,), (0,)), ((), ())), (((1,), (1,)), ((), ())), (((0,), (0,)), ((), ()))
HERE, NEXT, FAR, LAST = range(4)
TILE = 256


def adamw(w, m, v, g):
    m = 0.9 * m + 0.1 * g
    v = 0.95 * v + 0.05 * g * g
    step = m * lax.rsqrt(v + 1e-8) + 0.1 * w
    return (w - 0.02 * step).astype(jnp.bfloat16), m, v


def update_kernel(*refs):
    given, out = refs[:12], refs[12:]
    for i in range(3):
        new = adamw(*(ref[...].astype(F32) for ref in given[i::3]))
        for ref, value in zip(out[i::3], new, strict=True):
            ref[...] = value


def update(weights, m, v, gradients):
    def spec(w):
        return pl.BlockSpec((1, w.shape[1], w.shape[2] // 2), lambda layer, half: (layer, 0, half))

    return pl.pallas_call(
        update_kernel,
        grid=(2, 2),
        out_shape=[jax.ShapeDtypeStruct(w.shape, w.dtype) for w in (*weights, *m, *v)],
        in_specs=[spec(w) for w in weights] * 4,
        out_specs=[spec(w) for w in weights] * 3,
        name="update",
    )(*weights, *m, *v, *gradients)


def dot(a, b, dims=PLAIN):
    return lax.dot_general(a, b, dims, preferred_element_type=F32)


def scoped(name):
    def wrap(f):
        @functools.wraps(f)
        def inner(*args, **kwargs):
            with jax.named_scope(name):
                return f(*args, **kwargs)

        return inner

    return wrap


def block(n, size=TILE):
    return pl.ds(pl.multiple_of(n * size, size), size)


def added(values):
    total = None
    for value in values:
        total = value if total is None else total + value
    return total


OTHERS = (NEXT, FAR, LAST)


class Place:
    def __init__(self):
        self.s, self.x = lax.axis_index("s"), lax.axis_index("r")
        self.core = lax.rem(self.s, 2)
        y, z = lax.div(self.s, 8), lax.rem(lax.div(self.s, 2), 4)
        a = y * (1 - self.core) + z * self.core
        b = z * (1 - self.core) + y * self.core
        step_a, step_b = 4 - 3 * self.core, 1 + 3 * self.core
        self.a, self.b = [[lax.rem(at + d, 4) for d in range(4)] for at in (a, b)]
        self.chips = [[self.a[d] * step_a + self.b[e] * step_b for e in range(4)] for d in range(4)]
        self.devices = {(d, e): 2 * self.chips[d][e] + self.core for d in range(4) for e in range(4)}
        self.across = self.s + 1 - 2 * self.core

    def at(self, d, e):
        return {"s": self.devices[d, e]}

    def partner(self):
        return {"s": self.across}

    def along_x(self, d):
        return {"r": lax.rem(self.x + d, 4)}

    def neighbours(self, far):
        around = [self.at(*there) for there in ((NEXT, HERE), (LAST, HERE), (HERE, NEXT), (HERE, LAST), far)]
        return [self.partner()] + around


def meet(places):
    barrier = pltpu.get_barrier_semaphore()
    for place in places:
        pl.semaphore_signal(barrier, inc=1, device_id=place, device_id_type=MESH)
    pl.semaphore_wait(barrier, len(places))


def send(src, dst, send_sem, recv_sem, place):
    return pltpu.make_async_remote_copy(src_ref=src, dst_ref=dst, send_sem=send_sem, recv_sem=recv_sem, device_id=place, device_id_type=MESH)


class Gather:
    SLOTS = 10

    def __init__(self, p, n, m, here, full, sems):
        self.p, self.n, self.m, self.here, self.full = p, n, m, here, full
        self.out_sem, self.in_sem, self.here_sem, self.own_sem = sems
        self.total = 2 * (n + m)

    def hop(self, core, kind, hop, u, later):
        p, k = self.p, lax.rem(u, self.SLOTS)
        at = u - self.m * later if kind == 0 else u - self.n * (1 + later)
        here = self.here[kind].at[at]
        rows = here.shape[0]
        f = self.full[kind].at[at]
        cut = (rows // 2 + 7) // 8 * 8
        low, high = (0, cut), (cut, rows - cut)

        def piece(d, e, half=(0, rows)):
            if kind:
                return f.at[pl.ds(pl.multiple_of(rows * p.devices[d, e], 8) + half[0], half[1])]
            whole = f.at[p.a[d], p.b[e], core] if core == 0 else f.at[p.b[e], p.a[d], core]
            return whole.at[pl.ds(*half)]

        def group(e, half=(0, rows)):
            if kind:
                return [piece(d, e, half) for d in range(4)]
            whole = f.at[:, p.b[e], core] if core == 0 else f.at[p.b[e], :, core]
            return [whole.at[:, pl.ds(*half)]]

        def of_size(lines, columns, half=(0, rows)):
            if kind:
                return f.at[pl.ds(0, lines * columns * half[1])]
            return f.at[pl.ds(0, lines), pl.ds(0, columns), 0, pl.ds(*half)]

        def go(i, ref, place, left=0, src=None):
            send(ref if src is None else src, ref, self.out_sem.at[k, left], self.in_sem.at[k, i], place).start()

        def over(e):
            for one in group(e):
                go(7, one, p.partner(), FAR)

        def came(sem, ref):
            pltpu.make_async_copy(ref, ref, sem).wait()

        def all_came(i, columns, half=(0, rows)):
            came(self.in_sem.at[k, i], of_size(1, columns, half))

        sides = ((NEXT, LAST, low), (LAST, NEXT, high))
        if hop == 0:
            came(self.here_sem.at[u], here)
            own = piece(HERE, HERE)
            for i, ahead in enumerate(OTHERS):
                go(i, own, p.at(ahead, HERE), src=here)
            pltpu.make_async_copy(here, own, self.own_sem.at[k]).start()
        if hop == 1:
            came(self.own_sem.at[k], piece(HERE, HERE))
            for i, _ in enumerate(OTHERS):
                all_came(i, 1)
            for one in group(HERE):
                for side, (ahead, _, _) in enumerate(sides):
                    go(3 + side, one, p.at(HERE, ahead), 1)
            over(HERE)
        if hop == 2:
            for side, (ahead, back, half) in enumerate(sides):
                all_came(3 + side, 4)
                for one in group(back, half):
                    go(5 + side, one, p.at(HERE, ahead), 1)
                over(back)
        if hop == 3:
            for side, (_, _, half) in enumerate(sides):
                all_came(5 + side, 4, half)
            over(FAR)
        if hop == 4:
            came(self.in_sem.at[k, 7], of_size(4, 4))
            for i, (lines, columns) in enumerate(((1, 3), (3, 4), (4, 4))):
                came(self.out_sem.at[k, i], of_size(lines, columns))

    def done(self, u):
        return u + 8

    @scoped("gather")
    def step(self, t):
        def both(core, hop, u):
            later = lax.div(u, self.n + self.m)
            is_down = u - (self.n + self.m) * later >= self.n
            pl.when(~is_down)(lambda: self.hop(core, 0, hop, u, later))
            pl.when(is_down)(lambda: self.hop(core, 1, hop, u, later))

        def run(core):
            for hop in range(4, -1, -1):
                u = t - 2 * hop
                pl.when((u >= 0) & (u < self.total))(functools.partial(both, core, hop, u))

        for core in (0, 1):
            pl.when(self.p.core == core)(functools.partial(run, core))

    def steps(self, first, count):
        lax.fori_loop(0, count, lambda i, c: (self.step(first + i), c)[1], 0)


def normed(wide):
    return (wide * lax.rsqrt(jnp.mean(wide * wide, -1, keepdims=True) + 1e-6)).astype(BF16)


def forward_kernel(x, dy, w_gate, w_up, w_down, gu, d, pq, act_out, at_out, h_out, dw_out,
                   a, dyv, act, wt, wdt, pqs, h, turned, xs, dws, here_gu, here_d, out_sem, in_sem, here_sem, own_sem,
                   x_sem, dy_sem, act_sem, h_sem, at_sem, w_sem, wd_sem, pq_sem, xs_sem, dw_sem):
    tokens, width = a.shape
    n, m = act.shape[0], h.shape[0]
    p = Place()
    gather = Gather(p, n, m, (here_gu, here_d), (gu, d), (out_sem, in_sem, here_sem, own_sem))
    copy = pltpu.make_async_copy
    copy(x, a, x_sem).start()
    for layer in range(2):

        def bring(j, c, layer=layer):
            u = j + layer * (n + m)
            copy(w_gate.at[layer, :, block(j)], here_gu.at[layer * n + j, pl.ds(0, 32)], here_sem.at[u]).start()
            copy(w_up.at[layer, :, block(j)], here_gu.at[layer * n + j, pl.ds(32, 32)], here_sem.at[u]).start()
            return c

        lax.fori_loop(0, n, bring, 0)
        for i in range(m):
            u = n + i + layer * (n + m)
            copy(w_down.at[layer, :, pl.ds(i * TILE, TILE)], here_d.at[layer * m + i], here_sem.at[u]).start()
    copy(dy, dyv, dy_sem).start()
    meet(p.neighbours((FAR, HERE)))

    @scoped("norm")
    def norm(rows, wide):
        value = normed(wide)
        a[rows] = value
        turned[:, rows] = value.T

    def turned_out(layer):
        return copy(turned, at_out.at[layer], at_sem)

    def start(t, c):
        gather.step(t)
        pl.when(t == 1)(lambda: copy(x, a, x_sem).wait())

        @pl.when(t >= 1)
        def _():
            norm(block(t - 1), a[block(t - 1)].astype(F32))

        return c

    assert gather.done(0) == tokens // TILE
    lax.fori_loop(0, gather.done(1), start, 0)
    turned_out(0).start()

    def w_tile(unit, k):
        return copy(gu.at[unit], wt.at[k], w_sem.at[k])

    def wd_tile(i, k):
        return copy(d.at[i], wdt.at[k], wd_sem.at[k])

    def x_tile(i, k):
        return copy(x.at[:, block(i)], xs.at[k], xs_sem.at[k])

    def pq_tile(layer, j, k):
        return copy(pqs.at[k], pq.at[layer * n + j], pq_sem.at[k])

    def dw_tile(j, k):
        return copy(dws.at[k], dw_out.at[block(j)], dw_sem.at[k])

    def act_tile(j):
        return copy(act.at[j], act_out.at[j], act_sem)

    base = gather.done(n + m) + 1

    def hidden(layer):
        def body(j, c):
            k = lax.rem(j, 2)
            if layer:

                extra = jnp.maximum(lax.div(j - 7, 2), 0)

                def more(i, c):
                    pl.when((i == 0) | ((j > 7) & (lax.rem(j, 2) == 0)))(lambda: gather.step(base + j + extra + i))
                    return c

                lax.fori_loop(0, 2, more, 0)
            else:
                gather.step(gather.done(1) + j)

            @pl.when(j < n - 1)
            def _():
                w_tile(layer * n + j + 1, 1 - k).start()

            if layer == 0:

                @pl.when(j == n - 1)
                def _():
                    wd_tile(0, 0).start()
                    x_tile(0, 0).start()

            w_tile(layer * n + j, k).wait()
            pl.when(j >= 2 - 2 * layer)(lambda: pq_tile(layer, j, k).wait())
            if layer:
                pl.when(j >= 2)(lambda: dw_tile(j - 2, k).wait())
            gate_w, up_w = (wt[k, :, :, :, 32 * i : 32 * i + 32, :].reshape(width, TILE) for i in range(2))

            @scoped("hidden")
            def make(fresh):
                for i in range(tokens // 512):
                    rows = pl.ds(512 * i, 512)
                    if fresh:
                        norm(rows, jnp.concatenate([h[q, rows] for q in range(m)], -1).astype(F32))
                    gate, up = dot(a[rows], gate_w), dot(a[rows], up_w)
                    s = 0.5 * jnp.tanh(0.5 * gate) + 0.5
                    silu = gate * s
                    pqs[k, 0, rows] = silu
                    pqs[k, 1, rows] = up * (s + silu * (1 - s))
                    act[j, rows] = (silu * up).astype(BF16)

            if layer:
                pl.when(j == 0)(lambda: make(True))
                pl.when(j > 0)(lambda: make(False))
                pl.when(j == 0)(lambda: turned_out(1).start())
            else:
                make(False)
            pq_tile(layer, j, k).start()
            if layer:

                @pl.when(j < n)
                @scoped("down_terms")
                def _():
                    dws[k] = dot(act[j], dyv[...], BY_ROWS).astype(BF16)

                dw_tile(j, k).start()
            else:
                act_tile(j).start()
            return c

        lax.fori_loop(0, n, body, 0)
        if layer:
            for j in (n - 2, n - 1):
                pq_tile(layer, j, j % 2).wait()
                dw_tile(j, j % 2).wait()
            turned_out(1).wait()

    w_tile(0, 0).start()
    hidden(0)

    def h_tile(i):
        return copy(h.at[i], h_out.at[:, block(i)], h_sem)

    def down(i, c):
        k = lax.rem(i, 2)
        gather.step(gather.done(n + 1) + i)

        @pl.when(i < m - 1)
        def _():
            wd_tile(i + 1, 1 - k).start()
            x_tile(i + 1, 1 - k).start()

        @pl.when(i == m - 1)
        def _():
            w_tile(n, 0).start()

        with jax.named_scope("tiles"):
            wd_tile(i, k).wait()
            x_tile(i, k).wait()
        with jax.named_scope("down"):
            for r in range(tokens // 512):
                rows = pl.ds(512 * r, 512)
                out = added(dot(act[j, rows], wdt[k, pl.ds(TILE * j, TILE)]) for j in range(n))
                h[i, rows] = xs[k, rows] + out.astype(BF16)
        h_tile(i).start()
        return c

    lax.fori_loop(0, m, down, 0)

    turned_out(0).wait()
    with jax.named_scope("between"):
        copy(act, act_out, act_sem).wait()
        copy(dy, dyv, dy_sem).wait()
    hidden(1)
    gather.steps(base + n + 3, max(0, gather.done(gather.total - 1) + 1 - (base + n + 3)))
    copy(h, h, h_sem).wait()


def forward(x, dy, weights):
    tokens, width = x.shape
    w_gate, w_up, w_down = weights
    hidden, rows = w_gate.shape[-1], w_down.shape[1]
    n, m = hidden // TILE, width // TILE
    layers, pieces = 2, (4, 4, 2, 64, TILE)
    shapes = [
        ((layers * n, *pieces), BF16),
        ((layers * m, hidden, TILE), BF16),
        ((layers * n, 2, tokens, TILE), F32),
        ((n, tokens, TILE), BF16),
        ((layers, width, tokens), BF16),
        ((tokens, width), BF16),
        ((hidden, width), BF16),
    ]

    def twice(*shape, dtype=BF16):
        return pltpu.VMEM((2, *shape), dtype)

    def sems(*shape):
        return pltpu.SemaphoreType.DMA(shape)

    scratch = [
        pltpu.VMEM((tokens, width), BF16),
        pltpu.VMEM((tokens, width), BF16),
        pltpu.VMEM((n, tokens, TILE), BF16),
        twice(*pieces),
        twice(hidden, TILE),
        twice(2, tokens, TILE, dtype=F32),
        pltpu.VMEM((m, tokens, TILE), BF16),
        pltpu.VMEM((width, tokens), BF16),
        twice(tokens, TILE),
        twice(TILE, width),
        pltpu.VMEM((layers * n, *pieces[3:]), BF16),
        pltpu.VMEM((layers * m, rows, TILE), BF16),
        sems(Gather.SLOTS, 3),
        sems(Gather.SLOTS, 8),
        sems(layers * (n + m)),
        sems(Gather.SLOTS),
    ]
    scratch += [sems() for _ in range(5)] + [sems(2) for _ in range(5)]
    return pl.pallas_call(
        forward_kernel,
        out_shape=[jax.ShapeDtypeStruct(*shape) for shape in shapes],
        in_specs=[pl.BlockSpec(memory_space=pl.ANY)] * 5,
        out_specs=[pl.BlockSpec(memory_space=pl.ANY)] * len(shapes),
        scratch_shapes=scratch,
        compiler_params=pltpu.CompilerParams(collective_id=0, has_side_effects=True, vmem_limit_bytes=VMEM_LIMIT),
        name="forward",
    )(x, dy, w_gate, w_up, w_down)


class Sum:
    @staticmethod
    def scratch(terms, slots, rows, columns):
        def many(slots, *lead, columns=columns, dtype=BF16, count=1):
            return [pltpu.VMEM((slots, *lead, rows, columns), dtype)] * count

        half, near = columns // 2, 2
        return (
            many(terms, 16, 2)
            + many(slots, 16)
            + many(slots, 4, dtype=F32)
            + many(near, 4, dtype=F32, count=2)
            + many(near, 4, count=3)
            + many(slots, 4, columns=half, count=2)
            + many(slots, 4, count=2)
            + many(slots, dtype=F32)
            + many(near, 3)
            + many(slots, 3)
            + many(slots, 4)
            + [pltpu.SemaphoreType.DMA((slots, 11))] * 2
        )

    def __init__(self, p, refs, emit, lag, delay):
        self.p, self.emit, self.lag, self.delay = p, emit, lag, delay
        self.term, self.swapped, self.ca, self.cp, self.cm, self.x1, self.x2p, self.x2m, self.r1a, self.r1b, self.r2p, self.r2m = refs[:12]
        self.db, self.y, self.ry, self.rx, self.out_sem, self.in_sem = refs[12:]
        self.half = self.term.shape[-1] // 2

    def slot(self, ref, u):
        return ref.at[lax.rem(u, ref.shape[0])]

    def copies(self, hop, u):
        p, h = self.p, self.half
        out_sem, in_sem = self.slot(self.out_sem, u), self.slot(self.in_sem, u)

        def one(i, src, dst, place):
            return send(src, dst, out_sem.at[i], in_sem.at[i], place)

        if hop == 0:
            return [one(0, self.slot(self.term, u).at[:, 1 - p.core], self.slot(self.swapped, u), p.partner())]
        if hop == 3:
            y, ry = self.slot(self.y, u), self.slot(self.ry, u)
            return [one(5 + i, y.at[i], ry.at[i], p.at(HERE, ahead)) for i, ahead in enumerate(OTHERS)]
        if hop > 3:
            mine = self.slot(self.rx, u).at[p.x]
            return [one(8 + i, mine, mine, p.along_x(d)) for i, d in enumerate(OTHERS)]
        sources, landings = ((self.x1, self.x1), (self.r1a, self.r1b)) if hop == 1 else ((self.x2p, self.x2m), (self.r2p, self.r2m))
        made = []
        for side, (src, dst, ahead) in enumerate(zip(sources, landings, (NEXT, LAST), strict=True)):
            src = self.slot(src, u)
            if hop == 1:
                src = src.at[:, :, pl.ds(side * h, h)]
            made.append(one(2 * hop - 1 + side, src, self.slot(dst, u), p.at(ahead, HERE)))
        return made

    def add(self, hop, u):
        p, h = self.p, self.half
        low, high = slice(0, h), slice(h, None)

        def of(ref, *index):
            return ref[(lax.rem(u, ref.shape[0]), *index)].astype(F32)

        def put(ref, value, *index):
            ref[(lax.rem(u, ref.shape[0]), *index)] = value.astype(ref.dtype)

        rows = slice(None)
        if hop == 1:
            for d, ref in enumerate((self.ca, self.cp, self.x1, self.cm)):
                for e in range(4):
                    chip = p.chips[d][e]
                    put(ref, of(self.term, chip, p.core) + of(self.swapped, chip), e)
        if hop == 2:
            for e in range(4):
                put(self.x2p, of(self.cp, e, rows, low) + of(self.r1a, e), e, rows, low)
                put(self.x2p, of(self.cp, e, rows, high), e, rows, high)
                put(self.x2m, of(self.cm, e, rows, low), e, rows, low)
                put(self.x2m, of(self.cm, e, rows, high) + of(self.r1b, e), e, rows, high)
        if hop == 3:
            for e in range(4):
                value = of(self.ca, e) + of(self.r2p, e) + of(self.r2m, e)
                put(self.y, value, e - 1) if e else put(self.db, value)
        if hop == 4:
            put(self.rx, (of(self.db) + of(self.ry, 0)) + (of(self.ry, 1) + of(self.ry, 2)), p.x)
        if hop == 5:
            self.emit(u, ((of(self.rx, 0) + of(self.rx, 1)) + (of(self.rx, 2) + of(self.rx, 3))).astype(BF16))

    def hop(self, hop, u):
        with jax.named_scope(f"hop{hop}"):
            self.do(hop, u)

    def do(self, hop, u):
        if hop:
            for copy in self.copies(hop - 1, u):
                copy.wait()
        self.add(hop, u)
        if hop < HOPS:
            for copy in self.copies(hop, u):
                copy.start()

    def step(self, t, first, last):
        for hop in range(HOPS, -self.delay, -1):
            u = t - self.delay - self.lag * hop
            pl.when((u >= first) & (u < last))(functools.partial(self.hop, hop, u))


def backward_kernel(dy, gu, d, pq, act, at, h, dw1, g_gate, g_up, g_down, dgu_out, dw0, dh, av, big, load_sem, dh_sem, at_sem, big_sem, wd_sem, pq_sem, dgu_sem, dw_sem, dgc_sem, h_sem, *scratch):
    tokens, width = dh.shape
    n, m, d_rows = act.shape[0], width // TILE, g_down.shape[1]
    half = len(scratch) // 2
    copy = pltpu.make_async_copy
    p = Place()

    def emit_gu(u, value):
        later = lax.div(u, n)
        for i, out in enumerate((g_gate, g_up)):
            out[1 - later, :, block(u - n * later)] = value[32 * i : 32 * i + 32]

    def emit_d(u, value):
        later = lax.div(u, m)
        g_down[1 - later, :, block(u - m * later)] = value

    sum_gu, sum_d = Sum(p, scratch[:half], emit_gu, 2, 0), Sum(p, scratch[half:], emit_d, 1, 0)
    copy(dy, dh, dh_sem).start()
    copy(at.at[1], av, at_sem).start()

    def d_start(term, s, first):
        if len(term.shape) > 2:
            copy(term.at[:, :, :, block(s)], sum_d.term.at[lax.rem(first + s, 2)], load_sem).start()
            return

        def one(i, c):
            rows = pl.ds(pl.multiple_of(d_rows * i, 8), d_rows)
            copy(term.at[rows, block(s)], sum_d.term.at[lax.rem(first + s, 2), lax.div(i, 2), lax.rem(i, 2)], load_sem).start()
            return c

        lax.fori_loop(0, 32, one, 0)

    def d_step(term, s, first, ready=None):
        sum_d.step(first + s, first, first + m)

        @pl.when(s < m)
        def _():
            whole = sum_d.term.at[lax.rem(first + s, 2)]
            copy(whole, whole, load_sem).wait()
            sum_d.hop(0, first + s)

        @pl.when(s + 1 < m)
        def _():
            if ready is not None:
                ready(s + 1)
            d_start(term, s + 1, first)

    def gradients(layer, first, begin, d_turn):
        def phase(wdt, pqt, dgu):
            def tiles(j, k):
                return [
                    copy(d.at[pl.ds(layer * m, m), block(j)], wdt.at[k], wd_sem.at[k]),
                    copy(pq.at[layer * n + j], pqt.at[k], pq_sem.at[k]),
                ]

            def dgu_tile(j, k):
                return copy(dgu.at[k], dgu_out.at[j], dgu_sem.at[k])

            def body(j, c):
                k = lax.rem(j, 2)
                sum_gu.step(first + j, first, first + n)
                d_turn(j)
                if layer:
                    copy(gu.at[n + j], big.at[j], big_sem.at[0]).start()

                @pl.when(j < n - 1)
                def _():
                    for one in tiles(j + 1, 1 - k):
                        one.start()

                with jax.named_scope("tiles"):
                    for one in tiles(j, k):
                        one.wait()
                    if layer:
                        pl.when(j >= 2)(lambda: dgu_tile(j - 2, k).wait())
                with jax.named_scope("terms"):
                    for i in range(tokens // 512):
                        rows = pl.ds(512 * i, 512)
                        by_act = added(dot(dh[rows, TILE * e : TILE * e + TILE], wdt[k, e], BY_COLUMNS) for e in range(m))
                        by_act = by_act.astype(BF16).astype(F32)
                        dgu[k, 0, rows] = (by_act * pqt[k, 1, rows]).astype(BF16)
                        dgu[k, 1, rows] = (by_act * pqt[k, 0, rows]).astype(BF16)
                    slot = lax.rem(first + j, sum_gu.term.shape[0])
                    for i in range(m):
                        for e in (0, 1):
                            value = dot(av[TILE * i : TILE * i + TILE], dgu[k, e]).astype(BF16)
                            sum_gu.term[slot, 4 * i : 4 * i + 4, :, 32 * e : 32 * e + 32, :] = value.reshape(4, 2, 32, TILE)
                if layer:
                    dgu_tile(j, k).start()
                sum_gu.hop(0, first + j)
                return c

            for one in tiles(0, 0):
                one.start()
            begin()
            lax.fori_loop(0, n, body, 0)
            if layer:
                for j in (n - 2, n - 1):
                    dgu_tile(j, j % 2).wait()

        pl.run_scoped(
            phase,
            pltpu.VMEM((2, m, TILE, TILE), BF16),
            pltpu.VMEM((2, 2, tokens, TILE), F32),
            pltpu.VMEM((2, 2, tokens, TILE), BF16),
        )

    def to_states(dgc, hv):
        def rows_in(i, k):
            return [
                copy(dgu_out.at[:, :, block(i)], dgc.at[k], dgc_sem.at[k]),
                copy(h.at[block(i)], hv.at[k], h_sem.at[k]),
            ]

        def body(i, c):
            k = lax.rem(i, 2)
            sum_gu.step(n + i, 0, n)
            pl.when(k == 0)(lambda: d_step(dw1, (n + 1) // 2 + lax.div(i, 2), 0))

            @pl.when(i < tokens // TILE - 1)
            def _():
                for one in rows_in(i + 1, 1 - k):
                    one.start()

            with jax.named_scope("tiles"):
                for one in rows_in(i, k):
                    one.wait()
            with jax.named_scope("states"):
                parts = []
                for e in range(m):
                    weights = [big[j, 2 * TILE * e : 2 * TILE * (e + 1)].reshape(8, 64, TILE) for j in range(n)]
                    two = [
                        added(dot(dgc[k, j, o], weights[j][:, 32 * o : 32 * o + 32].reshape(TILE, TILE), BY_COLUMNS) for j in range(n))
                        for o in (0, 1)
                    ]
                    parts.append((two[0].astype(BF16) + two[1].astype(BF16)).astype(F32))
                by_a = jnp.concatenate(parts, -1)
                wide = hv[k].astype(F32)
                scale = lax.rsqrt(jnp.mean(wide * wide, -1, keepdims=True) + 1e-6)
                along = jnp.mean(by_a * wide, -1, keepdims=True)
                by_h = by_a * scale - wide * (scale * scale * scale * along)
                dh[block(i)] = dh[block(i)] + by_h.astype(BF16)
            return c

        for one in rows_in(0, 0):
            one.start()
        with jax.named_scope("weights"):
            copy(gu.at[pl.ds(n, n)], big, big_sem.at[0]).wait()
        lax.fori_loop(0, tokens // TILE, body, 0)

    def down(turned, made):
        def out(e):
            return copy(made.at[lax.rem(e, 2)], dw0.at[:, block(e)], dw_sem.at[lax.rem(e, 2)])

        def body(e, c):
            k = lax.rem(e, 2)
            for i in (0, 1):
                sum_gu.step(n + tokens // TILE + 2 * e + i, 0, n)

            @pl.when(e == 1)
            def _():
                out(0).wait()
                d_start(dw0, 0, m)

            pl.when(e >= 2)(lambda: d_step(dw0, e - 2, m, lambda s: out(s).wait()))
            with jax.named_scope("turn"):
                turned[...] = dh[:, block(e)].T

            pl.when(e == 0)(lambda: copy(act, big, big_sem.at[0]).wait())
            with jax.named_scope("down_terms"):
                for j in range(n):
                    made[k, TILE * j : TILE * (j + 1)] = dot(turned[...], big[j]).astype(BF16).T
            out(e).start()
            return c

        def columns():
            lax.fori_loop(0, m, body, 0)
            copy(at.at[0], av, at_sem).wait()

        copy(act, big, big_sem.at[0]).start()

        def last_turn(j):
            pl.when(lax.rem(j, 2) == 0)(lambda: d_step(dw0, 2 + lax.div(j, 2), m, lambda s: out(s).wait()))

        gradients(0, n, columns, last_turn)

    @scoped("meet")
    def begin():
        meet(p.neighbours((HERE, FAR)) + [p.along_x(d) for d in OTHERS])
        copy(dy, dh, dh_sem).wait()
        copy(at.at[1], av, at_sem).wait()

    def turn(j):
        pl.when(lax.rem(j, 2) == 0)(lambda: d_step(dw1, lax.div(j, 2), 0))

    d_start(dw1, 0, 0)
    gradients(1, 0, begin, turn)
    copy(at.at[0], av, at_sem).start()
    pl.run_scoped(
        to_states,
        pltpu.VMEM((2, n, 2, TILE, TILE), BF16),
        pltpu.VMEM((2, TILE, width), BF16),
    )
    pl.run_scoped(down, pltpu.VMEM((TILE, tokens), BF16), pltpu.VMEM((2, 32 * d_rows, TILE), BF16))

    def rest(i, c):
        sum_gu.step(2 * n + i, n, 2 * n)
        return c

    lax.fori_loop(0, 2 * HOPS, rest, 0)


def backward(dy, gu, d, pq, act, at, h, dw1):
    tokens, width = dy.shape
    n, hidden = gu.shape[0] // 2, dw1.shape[0]
    rows, m = hidden // 32, width // TILE
    gu = gu.reshape(2 * n, tokens, TILE)
    assert 32 * 64 == tokens and n == 3 * m + 1 and HOPS + m == (n + 5) // 2 and 2 * HOPS + 1 <= tokens // TILE + 2 * m
    any_space, vmem = pl.BlockSpec(memory_space=pl.ANY), pl.BlockSpec(memory_space=pltpu.VMEM)
    shapes = [((2, 32, hidden), BF16)] * 2 + [((2, rows, width), BF16), ((n, 2, tokens, TILE), BF16), ((hidden, width), BF16)]
    out = pl.pallas_call(
        backward_kernel,
        out_shape=[jax.ShapeDtypeStruct(*shape) for shape in shapes],
        in_specs=[any_space] * 8,
        out_specs=[vmem] * 3 + [any_space] * 2,
        scratch_shapes=[pltpu.VMEM(shape, BF16) for shape in ((tokens, width), (width, tokens), (n, tokens, TILE))]
        + [pltpu.SemaphoreType.DMA(())] * 3
        + [pltpu.SemaphoreType.DMA((2,))] * 7
        + Sum.scratch(3, 4, 64, TILE)
        + Sum.scratch(2, 2, rows, TILE),
        compiler_params=pltpu.CompilerParams(collective_id=1, has_side_effects=True, vmem_limit_bytes=VMEM_LIMIT),
        name="backward",
    )(dy, gu, d, pq, act, at, h, dw1.reshape(16, 2, rows, width))
    return out[:3]


def solution(mesh):
    def step(x, dy, *arrays):
        weights, m, v = (arrays[i : i + 3] for i in (0, 3, 6))
        return tuple(update(weights, m, v, backward(dy[0], *forward(x[0], dy[0], weights))))

    states, cut = P(("rep", "r", "s"), None, None), P(None, "s", None)
    return jax.shard_map(
        step,
        mesh=mesh,
        in_specs=(states, states) + (cut,) * 9,
        out_specs=(P("rep", "s", None),) * 9,
        check_vma=False,
    )
```
